32 devices in a mesh: ctx: 4 (over z), exp: 8 (over y, x, core).
Axes of the slice: x: 2, y: 2, z: 4, core: 2. Of those that a mesh axis runs over, the one named last changes fastest.
Arguments:
- hidden_in: bfloat16 [8, 512, 2048], P('exp', 'ctx'), may hold values from -40 to 40
- expert_ids: int32 [8, 512, 8], P('exp', 'ctx'), may hold values from 0 to 31, all different within a row; in each aligned block of 128 rows (0 to 127, 128 to 255, ..., all dimensions but the last counted through in order) at most 42 rows name the same one
- gate_weights: float32 [8, 512, 8], P('exp', 'ctx'), may hold values from 0.1 to 0.4
- attn_gain: bfloat16 [2048], P('exp'), may hold values from 0.5 to 1.5
- w_query: bfloat16 [2048, 4096], P('exp'), may hold values from -0.125 to 0.125
- key_projection: bfloat16 [2048, 512], P('exp'), may hold values from -0.125 to 0.125
- value_projection: bfloat16 [2048, 512], P('exp'), may hold values from -0.125 to 0.125
- query_gain: bfloat16 [128], P('exp'), may hold values from 0.5 to 1.5
- key_norm_gain: bfloat16 [128], P('exp'), may hold values from 0.5 to 1.5
- w_output: bfloat16 [4096, 2048], P('exp'), may hold values from -0.75 to 0.75
- mlp_gain: bfloat16 [2048], P('exp'), may hold values from 0.5 to 1.5
- w_gate: bfloat16 [32, 2048, 768], P(('ctx', 'exp')), may hold values from -0.125 to 0.125
- w_up: bfloat16 [32, 2048, 768], P(('ctx', 'exp')), may hold values from -0.125 to 0.125
- w_down: bfloat16 [32, 768, 2048], P(('ctx', 'exp')), may hold values from -0.4375 to 0.4375
- grad_out: bfloat16 [8, 512, 2048], P('exp', 'ctx'), may hold values from -6 to 6
Outputs:
- hidden_out: bfloat16 [8, 512, 2048], P('exp', 'ctx')
- grad_in: float32 [8, 512, 2048], P('exp', 'ctx')
- grad_attn_gain: float32 [2048], P('exp')
- grad_w_query: float32 [2048, 4096], P('exp')
- grad_w_key: float32 [2048, 512], P('exp')
- grad_w_value: float32 [2048, 512], P('exp')
- grad_query_gain: float32 [128], P('exp')
- grad_key_gain: float32 [128], P('exp')
- grad_w_output: float32 [4096, 2048], P('exp')
- grad_mlp_gain: float32 [2048], P('exp')
- grad_w_gate: float32 [32, 2048, 768], P(('ctx', 'exp'))
- grad_w_up: float32 [32, 2048, 768], P(('ctx', 'exp'))
- grad_w_down: float32 [32, 768, 2048], P(('ctx', 'exp'))
The draws below stay inside these ranges and needn't reach their ends.
Inputs may be any that keep to these rules, and one draw needn't show every extreme that they name: `expert_ids`: each row names 8 different experts; among the 128 rows of one device no expert is named more than 42 times, a bound that some block reaches.
All inputs are finite; a program needn't handle non-finite values.
Results may differ from the reference program's by a relative error of at most 0.023.
Values may be sent and summed in bfloat16 or wider, within the bound.
A program may use at most 320 MiB of HBM per device.

```python
import math
import jax
import jax.numpy as jnp
import numpy as np
from jax import lax

MODEL_WIDTH = 2048
QUERY_HEADS = 32
KEY_VALUE_HEADS = 4
HEAD_SIZE = 128
FF = 768
TOPK = 8
TOK_DEV = 128
EXPERTS = 32
SEQS = 8
LEN = 512
CAP = 42
N_CTX = 4
N_EXP = 8


def draw_hidden_in(key, part):
    subkeys = jax.random.split(key, 3)
    row_scale = jnp.exp(jax.random.uniform(subkeys[0], (SEQS, LEN, 1), jnp.float32, -1.15, 1.15))
    column_scale = jnp.exp(jax.random.uniform(subkeys[1], (1, 1, MODEL_WIDTH), jnp.float32, -1.15, 1.15))
    base = jnp.clip(jax.random.normal(subkeys[2], (SEQS, LEN, MODEL_WIDTH), jnp.float32), -4.0, 4.0)
    return (base * row_scale * column_scale).astype(jnp.bfloat16)


def block_levels(own_key, dims, cuts, smallest, largest):
    gain = 1.0
    for axis_at, shards_of in cuts:
        heights = jax.random.uniform(jax.random.fold_in(jax.random.fold_in(own_key, 6), axis_at), (shards_of,), jnp.float32, smallest / len(cuts), largest / len(cuts))
        gain = gain * jnp.repeat(jnp.exp(heights), dims[axis_at] // shards_of).reshape((-1,) + (1,) * (len(dims) - 1 - axis_at))
    return gain


def routed_block(stream_key, own, number, rows, number_of, top, bound, lean):
    order = jax.random.permutation(stream_key, number_of)
    heavy_load, usual = load_shares(number_of, rows * top, bound, lean, True), load_shares(number_of, rows * top, bound, lean, False)
    places = jnp.arange(number_of)

    def named(lengths, offset_by):
        used = int((lengths > 0).sum())
        fixed = max(1, used // 4)
        passed = fixed + (places - fixed + offset_by * (used - fixed)) % max(1, number_of - fixed)
        return jnp.zeros((number_of,), jnp.int32).at[order[jnp.where(places < fixed, places, passed)]].set(jnp.asarray(lengths, jnp.int32))

    lengths = jnp.where(number % 4 == 0, named(heavy_load, number // 4), named(usual, number - number // 4 - 1))
    mixed = jax.random.permutation(jax.random.fold_in(own, 3), number_of)
    giver, taker = mixed[0:number_of // 2 * 2:2], mixed[1:number_of // 2 * 2:2]
    margin = jnp.minimum(lengths[giver] - 1, bound - lengths[taker]) // 2
    margin = jnp.where((giver == order[0]) | (taker == order[0]) | (lengths[taker] == 0), 0, jnp.maximum(margin, 0))
    passed = jax.random.randint(jax.random.fold_in(own, 4), (number_of // 2,), 0, 1 << 20) % (margin + 1)
    lengths = lengths.at[giver].add(-passed).at[taker].add(passed)
    labels = jnp.searchsorted(jnp.cumsum(lengths), jnp.arange(rows * top), side="right").astype(jnp.int32)
    grid = labels.reshape(top, rows).T
    grid = grid[jax.random.permutation(jax.random.fold_in(own, 1), rows)]
    offset_by = jax.random.randint(jax.random.fold_in(own, 2), (rows, 1), 0, top)
    return jnp.take_along_axis(grid, (jnp.arange(top)[None, :] + offset_by) % top, axis=1)


def load_shares(amount, total, bound, skew, full):
    loads = [(1 << 20) // math.isqrt(rank ** skew) + 1 for rank in range(1, amount + 1)]
    largest = bound if full else min(bound, max(-(-total // amount), total * loads[0] // sum(loads)))
    least = 1 if total - largest >= amount - 1 else 0
    counts, spare = [largest] + [least] * (amount - 1), total - largest - least * (amount - 1)
    while spare > 0:
        movable = [i for i in range(1, amount) if counts[i] < largest] or [i for i in range(1, amount) if counts[i] < bound]
        mass, left = sum([loads[i] for i in movable]), spare
        for i in movable:
            extra = min(bound - counts[i], max(1, left * loads[i] // mass), spare)
            counts[i] = counts[i] + extra
            spare = spare - extra
    return np.array(counts)


def centred(key, dims, width, most, cuts=(), kind=jnp.bfloat16):
    entries = width * jax.random.normal(key, dims, jnp.float32)
    if cuts:
        entries = entries * block_levels(key, dims, cuts, -0.22, 0.18)
    return jnp.clip(entries, -most, most).astype(kind)


def setup_inputs(seed: int = 0) -> dict:
    splits = jax.random.split(jax.random.key(seed), 16)
    hidden_in = draw_hidden_in(jax.random.fold_in(splits[15], 71), 0)
    expert_ids_keys = jax.random.split(jax.random.fold_in(splits[1], 1), SEQS * LEN // TOK_DEV)
    expert_ids_turns = jax.random.permutation(jax.random.fold_in(splits[1], 3), SEQS * LEN // TOK_DEV)
    expert_ids = jax.vmap(lambda own, number: routed_block(jax.random.fold_in(splits[1], 2), own, number, TOK_DEV, EXPERTS, TOPK, CAP, 2))(expert_ids_keys, expert_ids_turns).reshape((SEQS, LEN, TOPK))
    gate_weights = jnp.clip(0.1 + 0.3 * jax.random.uniform(splits[2], (SEQS, LEN, TOPK), jnp.float32) ** block_levels(splits[2], (SEQS, LEN, TOPK), ((0, 8), (1, 4)), -0.2, 0.2), 0.1, 0.4)
    attn_gain = jnp.clip(1.0 + 0.1 * jax.random.normal(splits[3], (MODEL_WIDTH,), jnp.float32), 0.5, 1.5).astype(jnp.bfloat16)
    w_query = centred(splits[4], (MODEL_WIDTH, QUERY_HEADS * HEAD_SIZE), MODEL_WIDTH ** -0.5, 0.125, ((0, 8),))
    key_projection = centred(splits[5], (MODEL_WIDTH, KEY_VALUE_HEADS * HEAD_SIZE), MODEL_WIDTH ** -0.5, 0.125, ((0, 8),))
    value_projection = centred(splits[6], (MODEL_WIDTH, KEY_VALUE_HEADS * HEAD_SIZE), MODEL_WIDTH ** -0.5, 0.125, ((0, 8),))
    query_gain = jnp.clip(1.0 + 0.1 * jax.random.normal(splits[7], (HEAD_SIZE,), jnp.float32), 0.5, 1.5).astype(jnp.bfloat16)
    key_norm_gain = jnp.clip(1.0 + 0.1 * jax.random.normal(splits[8], (HEAD_SIZE,), jnp.float32), 0.5, 1.5).astype(jnp.bfloat16)
    w_output = centred(splits[9], (QUERY_HEADS * HEAD_SIZE, MODEL_WIDTH), (QUERY_HEADS * HEAD_SIZE // 64) ** -0.5, 0.75, ((0, 8),))
    mlp_gain = jnp.clip(1.0 + 0.1 * jax.random.normal(splits[10], (MODEL_WIDTH,), jnp.float32), 0.5, 1.5).astype(jnp.bfloat16)
    w_gate = centred(splits[11], (EXPERTS, MODEL_WIDTH, FF), MODEL_WIDTH ** -0.5, 0.125, ((0, 32),))
    w_up = centred(splits[12], (EXPERTS, MODEL_WIDTH, FF), MODEL_WIDTH ** -0.5, 0.125, ((0, 32),))
    w_down = centred(splits[13], (EXPERTS, FF, MODEL_WIDTH), (FF // 4) ** -0.5, 0.4375, ((0, 32),))
    grad_out = centred(splits[14], (SEQS, LEN, MODEL_WIDTH), 1.0, 6.0, ((0, 8), (1, 4)))
    return {"hidden_in": hidden_in, "expert_ids": expert_ids, "gate_weights": gate_weights, "attn_gain": attn_gain, "w_query": w_query, "key_projection": key_projection, "value_projection": value_projection, "query_gain": query_gain, "key_norm_gain": key_norm_gain, "w_output": w_output, "mlp_gain": mlp_gain, "w_gate": w_gate, "w_up": w_up, "w_down": w_down, "grad_out": grad_out}


EPSILON = 1e-06
THETA = 1000000.0

def widen_heads(tensor):
    return lax.optimization_barrier(tensor).astype(jnp.float32)

def rms_scale(tensor):
    return lax.rsqrt(lax.optimization_barrier(jnp.mean(tensor * tensor, axis=-1, keepdims=True)) + EPSILON)

def norm_backward(cotangent, tensor, factor, weight):
    scaled = cotangent * weight
    unit_form = tensor * factor
    return factor * (scaled - unit_form * lax.optimization_barrier(jnp.mean(scaled * unit_form, axis=-1, keepdims=True)))

def rope_tables(positions):
    halfway = HEAD_SIZE // 2
    frequency = THETA ** (-(jnp.arange(halfway, dtype=jnp.float32) * (2.0 / HEAD_SIZE)))
    angles = positions.astype(jnp.float32)[:, None] * frequency[None, :]
    cosine_lookup = jnp.concatenate([jnp.cos(angles), jnp.cos(angles)], axis=-1)[:, None, :]
    sine_lookup = jnp.concatenate([jnp.sin(angles), jnp.sin(angles)], axis=-1)[:, None, :]
    return (cosine_lookup, sine_lookup)

def rotate(tensor, cosine_lookup, sine_lookup):
    halfway = tensor.shape[-1] // 2
    turned = jnp.concatenate([-tensor[..., halfway:], tensor[..., :halfway]], axis=-1)
    return tensor * cosine_lookup + turned * sine_lookup

def rotation_backward(cotangent, cosine_lookup, sine_lookup):
    halfway = cotangent.shape[-1] // 2
    sine_part = cotangent * sine_lookup
    turned = jnp.concatenate([sine_part[..., halfway:], -sine_part[..., :halfway]], axis=-1)
    return cotangent * cosine_lookup + turned

def project_heads(wide_in, attn_gain, w_query, key_projection, value_projection, query_gain, key_norm_gain, cosine_lookup, sine_lookup):
    row_total_count = wide_in.shape[0]
    first_scale = rms_scale(wide_in)
    normalized_input = (wide_in * first_scale * attn_gain.astype(jnp.float32)).astype(jnp.bfloat16)
    queries = jnp.dot(normalized_input, w_query, preferred_element_type=jnp.float32).reshape(row_total_count, QUERY_HEADS, HEAD_SIZE)
    key_unnormed = jnp.dot(normalized_input, key_projection, preferred_element_type=jnp.float32).reshape(row_total_count, KEY_VALUE_HEADS, HEAD_SIZE)
    values_raw = jnp.dot(normalized_input, value_projection, preferred_element_type=jnp.float32)
    query_scale = rms_scale(queries)
    key_rms_factor = rms_scale(key_unnormed)
    query_rotated = rotate(queries * query_scale * query_gain.astype(jnp.float32), cosine_lookup, sine_lookup).astype(jnp.bfloat16)
    key_rotated = rotate(key_unnormed * key_rms_factor * key_norm_gain.astype(jnp.float32), cosine_lookup, sine_lookup).astype(jnp.bfloat16)
    value_row_block = values_raw.astype(jnp.bfloat16)
    return (first_scale, normalized_input, queries, query_scale, key_unnormed, key_rms_factor, query_rotated, key_rotated, value_row_block)

def score_table(query_rotated, key_rotated):
    row_total_count = query_rotated.shape[0]
    query_group_width = QUERY_HEADS // KEY_VALUE_HEADS
    query_widened = widen_heads(query_rotated).reshape(row_total_count, KEY_VALUE_HEADS, query_group_width, HEAD_SIZE)
    key_wide = widen_heads(key_rotated)
    scores = jnp.einsum('qkgd,tkd->kgqt', query_widened, key_wide) * HEAD_SIZE ** (-0.5)
    causal = jnp.arange(row_total_count)[None, :] <= jnp.arange(row_total_count)[:, None]
    return (query_widened, key_wide, jnp.where(causal, jnp.exp(scores), 0.0))

def attend(query_rotated, key_rotated, value_row_block):
    row_total_count = query_rotated.shape[0]
    query_widened, key_wide, expos = score_table(query_rotated, key_rotated)
    value_widened = widen_heads(value_row_block).reshape(row_total_count, KEY_VALUE_HEADS, HEAD_SIZE)
    totals = lax.optimization_barrier(jnp.sum(expos, axis=-1))
    summed = jnp.einsum('kgqt,tkd->qkgd', widen_heads(expos.astype(jnp.bfloat16)), value_widened)
    output = summed / jnp.transpose(totals, (2, 0, 1))[..., None]
    return (output.reshape(row_total_count, QUERY_HEADS * HEAD_SIZE).astype(jnp.bfloat16), totals)

def attend_back(query_rotated, key_rotated, value_row_block, attention_rows, totals, attention_gradient):
    row_total_count = query_rotated.shape[0]
    query_group_width = QUERY_HEADS // KEY_VALUE_HEADS
    query_widened, key_wide, expos = score_table(query_rotated, key_rotated)
    value_widened = widen_heads(value_row_block).reshape(row_total_count, KEY_VALUE_HEADS, HEAD_SIZE)
    probs = expos / totals[..., None]
    gradient_widened = widen_heads(attention_gradient).reshape(row_total_count, KEY_VALUE_HEADS, query_group_width, HEAD_SIZE)
    value_gradient = jnp.einsum('kgqt,qkgd->tkd', widen_heads(probs.astype(jnp.bfloat16)), gradient_widened)
    grad_probs = jnp.einsum('qkgd,tkd->kgqt', gradient_widened, value_widened)
    rows_widened = widen_heads(attention_rows).reshape(row_total_count, KEY_VALUE_HEADS, query_group_width, HEAD_SIZE)
    deltas = jnp.transpose(lax.optimization_barrier(jnp.sum(gradient_widened * rows_widened, axis=-1)), (1, 2, 0))
    grad_scores = widen_heads((probs * (grad_probs - deltas[..., None]) * HEAD_SIZE ** (-0.5)).astype(jnp.bfloat16))
    grad_queries = jnp.einsum('kgqt,tkd->qkgd', grad_scores, key_wide).reshape(row_total_count, QUERY_HEADS, HEAD_SIZE)
    key_gradient = jnp.einsum('kgqt,qkgd->tkd', grad_scores, query_widened)
    return (grad_queries, key_gradient, value_gradient)

def reference(hidden_in, expert_ids, gate_weights, attn_gain, w_query, key_projection, value_projection, query_gain, key_norm_gain, w_output, mlp_gain, w_gate, w_up, w_down, grad_out):
    seq_count, sequence_length, feature_width = hidden_in.shape
    cosine_lookup, sine_lookup = rope_tables(jnp.arange(sequence_length, dtype=jnp.int32))

    def forward_seq(seq_in):
        wide_in = seq_in.astype(jnp.float32)
        outs_proj = project_heads(wide_in, attn_gain, w_query, key_projection, value_projection, query_gain, key_norm_gain, cosine_lookup, sine_lookup)
        attention_rows, totals = attend(outs_proj[6], outs_proj[7], outs_proj[8])
        return wide_in + jnp.dot(attention_rows, w_output, preferred_element_type=jnp.float32)
    mid_all = lax.map(forward_seq, hidden_in)
    flat_mid = mid_all.reshape(-1, feature_width)
    second_scale = rms_scale(flat_mid)
    mlp_in = (flat_mid * second_scale * mlp_gain.astype(jnp.float32)).astype(jnp.bfloat16)
    token_count = flat_mid.shape[0]
    slot_count = token_count * TOPK
    most_rows = N_CTX * N_EXP * CAP
    flat_ids = expert_ids.reshape(-1)
    flat_gates = gate_weights.reshape(-1).astype(jnp.float32)
    grad_rows = grad_out.reshape(-1, feature_width).astype(jnp.float32)
    padded_in = jnp.concatenate([mlp_in, jnp.zeros((1, feature_width), jnp.bfloat16)], axis=0)
    padded_grad = jnp.concatenate([grad_rows, jnp.zeros((1, feature_width), jnp.float32)], axis=0)

    def expert_step(running, expert):
        mixed, returned = running
        picked_slots = jnp.nonzero(flat_ids == expert, size=most_rows, fill_value=slot_count)[0].astype(jnp.int32)
        is_live = picked_slots < slot_count
        token_rows = jnp.where(is_live, picked_slots // TOPK, token_count).astype(jnp.int32)
        slot_gates = jnp.where(is_live, flat_gates[jnp.minimum(picked_slots, slot_count - 1)], 0.0)
        expert_in = padded_in[token_rows]
        gate_mat = w_gate[expert]
        up_mat = w_up[expert]
        down_mat = w_down[expert]
        gate_pre = jnp.dot(expert_in, gate_mat, preferred_element_type=jnp.float32)
        up_pre = jnp.dot(expert_in, up_mat, preferred_element_type=jnp.float32)
        sigmoid_gate = jax.nn.sigmoid(gate_pre)
        silu_gate = gate_pre * sigmoid_gate
        inner = (silu_gate * up_pre).astype(jnp.bfloat16)
        expert_out = jnp.dot(inner, down_mat, preferred_element_type=jnp.float32).astype(jnp.bfloat16)
        mixed = mixed.at[token_rows].add(slot_gates[:, None] * widen_heads(expert_out), mode='drop')
        grad_slot = (slot_gates[:, None] * padded_grad[token_rows]).astype(jnp.bfloat16)
        grad_inner = jnp.dot(grad_slot, down_mat.T, preferred_element_type=jnp.float32)
        grad_down = jnp.dot(inner.T, grad_slot, preferred_element_type=jnp.float32)
        grad_gate_pre = (grad_inner * up_pre * sigmoid_gate * (1.0 + gate_pre * (1.0 - sigmoid_gate))).astype(jnp.bfloat16)
        grad_up_pre = (grad_inner * silu_gate).astype(jnp.bfloat16)
        grad_gate_mat = jnp.dot(expert_in.T, grad_gate_pre, preferred_element_type=jnp.float32)
        grad_up_mat = jnp.dot(expert_in.T, grad_up_pre, preferred_element_type=jnp.float32)
        grad_expert_in = (jnp.dot(grad_gate_pre, gate_mat.T, preferred_element_type=jnp.float32) + jnp.dot(grad_up_pre, up_mat.T, preferred_element_type=jnp.float32)).astype(jnp.bfloat16)
        returned = returned.at[token_rows].add(widen_heads(grad_expert_in), mode='drop')
        return ((mixed, returned), (grad_gate_mat, grad_up_mat, grad_down))
    start_sums = (jnp.zeros((token_count, feature_width), jnp.float32), jnp.zeros((token_count, feature_width), jnp.float32))
    (mixed, grad_mlp), (grad_w_gate, grad_w_up, grad_w_down) = lax.scan(expert_step, start_sums, jnp.arange(EXPERTS, dtype=jnp.int32))
    hidden_out = (flat_mid + mixed).astype(jnp.bfloat16).reshape(seq_count, sequence_length, feature_width)
    grad_mlp_gain = lax.optimization_barrier(jnp.sum(grad_mlp * flat_mid * second_scale, axis=0))
    grad_mid = grad_rows + norm_backward(grad_mlp, flat_mid, second_scale, mlp_gain.astype(jnp.float32))

    def backward_step(running, pieces):
        seq_in, seq_grad = pieces
        wide_in = seq_in.astype(jnp.float32)
        first_scale, normalized_input, queries, query_scale, key_unnormed, key_rms_factor, query_rotated, key_rotated, value_row_block = project_heads(wide_in, attn_gain, w_query, key_projection, value_projection, query_gain, key_norm_gain, cosine_lookup, sine_lookup)
        attention_rows, totals = attend(query_rotated, key_rotated, value_row_block)
        grad_branch = seq_grad.astype(jnp.bfloat16)
        grad_wout = jnp.dot(attention_rows.T, grad_branch, preferred_element_type=jnp.float32)
        attention_gradient = jnp.dot(grad_branch, w_output.T, preferred_element_type=jnp.float32).astype(jnp.bfloat16)
        grad_queries, key_gradient, value_gradient = attend_back(query_rotated, key_rotated, value_row_block, attention_rows, totals, attention_gradient)
        grad_queries = rotation_backward(grad_queries, cosine_lookup, sine_lookup)
        key_gradient = rotation_backward(key_gradient, cosine_lookup, sine_lookup)
        query_gain_part = lax.optimization_barrier(jnp.sum(grad_queries * queries * query_scale, axis=(0, 1)))
        key_gain_part = lax.optimization_barrier(jnp.sum(key_gradient * key_unnormed * key_rms_factor, axis=(0, 1)))
        grad_query_rows = norm_backward(grad_queries, queries, query_scale, query_gain.astype(jnp.float32)).reshape(sequence_length, QUERY_HEADS * HEAD_SIZE).astype(jnp.bfloat16)
        key_row_gradient = norm_backward(key_gradient, key_unnormed, key_rms_factor, key_norm_gain.astype(jnp.float32)).reshape(sequence_length, KEY_VALUE_HEADS * HEAD_SIZE).astype(jnp.bfloat16)
        value_row_gradient = value_gradient.reshape(sequence_length, KEY_VALUE_HEADS * HEAD_SIZE).astype(jnp.bfloat16)
        grad_wq = jnp.dot(normalized_input.T, grad_query_rows, preferred_element_type=jnp.float32)
        grad_wk = jnp.dot(normalized_input.T, key_row_gradient, preferred_element_type=jnp.float32)
        grad_wv = jnp.dot(normalized_input.T, value_row_gradient, preferred_element_type=jnp.float32)
        grad_normed = jnp.dot(grad_query_rows, w_query.T, preferred_element_type=jnp.float32) + jnp.dot(key_row_gradient, key_projection.T, preferred_element_type=jnp.float32) + jnp.dot(value_row_gradient, value_projection.T, preferred_element_type=jnp.float32)
        attn_gain_part = lax.optimization_barrier(jnp.sum(grad_normed * wide_in * first_scale, axis=0))
        grad_seq_in = seq_grad + norm_backward(grad_normed, wide_in, first_scale, attn_gain.astype(jnp.float32))
        parts = (attn_gain_part, grad_wq, grad_wk, grad_wv, query_gain_part, key_gain_part, grad_wout)
        return (tuple((total_part + new_part for total_part, new_part in zip(running, parts))), grad_seq_in)
    initial_gradients = (jnp.zeros((feature_width,), jnp.float32), jnp.zeros((feature_width, QUERY_HEADS * HEAD_SIZE), jnp.float32), jnp.zeros((feature_width, KEY_VALUE_HEADS * HEAD_SIZE), jnp.float32), jnp.zeros((feature_width, KEY_VALUE_HEADS * HEAD_SIZE), jnp.float32), jnp.zeros((HEAD_SIZE,), jnp.float32), jnp.zeros((HEAD_SIZE,), jnp.float32), jnp.zeros((QUERY_HEADS * HEAD_SIZE, feature_width), jnp.float32))
    grads_sum, grad_in = lax.scan(backward_step, initial_gradients, (hidden_in, grad_mid.reshape(seq_count, sequence_length, feature_width)))
    return (hidden_out, grad_in, grads_sum[0], grads_sum[1], grads_sum[2], grads_sum[3], grads_sum[4], grads_sum[5], grads_sum[6], grad_mlp_gain, grad_w_gate, grad_w_up, grad_w_down)
```

```python
import jax
import jax.numpy as jnp
from jax import lax
from jax.sharding import PartitionSpec as P

KEY_VALUE_HEADS = 4
HEAD_SIZE = 128
TOPK = 8

EPSILON = 1e-06
THETA = 1000000.0

BF = jnp.bfloat16
F32 = jnp.float32
EVERY = ("ctx", "exp")


def rms_scale(tensor):
    return lax.rsqrt(jnp.mean(tensor * tensor, axis=-1, keepdims=True) + EPSILON)


def norm_backward(cotangent, tensor, factor, weight):
    scaled = cotangent * weight
    unit_form = tensor * factor
    return factor * (scaled - unit_form * jnp.mean(scaled * unit_form, axis=-1, keepdims=True))


def rope_tables(positions):
    halfway = HEAD_SIZE // 2
    frequency = THETA ** (-(jnp.arange(halfway, dtype=F32) * (2.0 / HEAD_SIZE)))
    angles = positions.astype(F32)[:, None] * frequency[None, :]
    cosine = jnp.concatenate([jnp.cos(angles), jnp.cos(angles)], axis=-1)
    sine = jnp.concatenate([jnp.sin(angles), jnp.sin(angles)], axis=-1)
    return cosine, sine


def rotate(tensor, cosine, sine):
    halfway = tensor.shape[-1] // 2
    turned = jnp.concatenate([-tensor[..., halfway:], tensor[..., :halfway]], axis=-1)
    return tensor * cosine + turned * sine


def rotation_backward(cotangent, cosine, sine):
    halfway = cotangent.shape[-1] // 2
    sine_part = cotangent * sine
    turned = jnp.concatenate([sine_part[..., halfway:], -sine_part[..., :halfway]], axis=-1)
    return cotangent * cosine + turned


def dot(a, b, dims):
    return lax.dot_general(a, b, (dims, ((), ())), preferred_element_type=F32)


def after(value, *earlier):
    return lax.optimization_barrier((value,) + earlier)[0]


def round_up(number, multiple):
    return -(-number // multiple) * multiple


def per_device(
    hidden_in,
    expert_ids,
    gate_weights,
    attn_gain,
    w_query,
    key_projection,
    value_projection,
    query_gain,
    key_norm_gain,
    w_output,
    mlp_gain,
    w_gate,
    w_up,
    w_down,
    grad_out,
):
    length, width = hidden_in.shape[1:]
    n_ctx, n_exp = lax.axis_size("ctx"), lax.axis_size("exp")
    n_all = n_ctx * n_exp
    ctx_index = lax.axis_index("ctx")
    rows_own, query_width = w_query.shape
    heads_own = query_width // HEAD_SIZE // n_exp
    own_width = heads_own * HEAD_SIZE
    sharers = n_exp // KEY_VALUE_HEADS
    tokens = n_exp * length
    factor = HEAD_SIZE ** (-0.5)
    w_gate, w_up, w_down = w_gate[0], w_up[0], w_down[0]

    def spread_heads(kv):
        per_head = kv.reshape(rows_own, KEY_VALUE_HEADS, HEAD_SIZE)
        return jnp.repeat(per_head, sharers, axis=1)

    packed = jnp.concatenate(
        [
            w_query.reshape(rows_own, n_exp, own_width),
            spread_heads(key_projection),
            spread_heads(value_projection),
        ],
        axis=2,
    )
    packed_width = own_width + 2 * HEAD_SIZE
    packed = jnp.transpose(packed, (1, 0, 2))
    gains = jnp.concatenate([attn_gain, mlp_gain, query_gain, key_norm_gain])
    gain_rows = round_up(round_up(gains.shape[0], packed_width) // packed_width, 16)
    gains = jnp.pad(gains, (0, gain_rows * packed_width - gains.shape[0]))
    gains = jnp.broadcast_to(gains.reshape(1, gain_rows, packed_width), (n_exp, gain_rows, packed_width))
    hidden_all = lax.all_gather(hidden_in[0], "exp", axis=0, tiled=True)
    heads_in = lax.all_to_all(
        jnp.concatenate([packed, gains], axis=1), "exp", split_axis=0, concat_axis=0, tiled=True
    )
    weight_cols = heads_in[:, :rows_own].reshape(n_exp * rows_own, packed_width)
    gains = heads_in[:, rows_own:].reshape(n_exp, gain_rows * packed_width).astype(F32)
    cut = attn_gain.shape[0]
    small = query_gain.shape[0]
    first_gain = gains[:, :cut].reshape(-1)
    second_gain = gains[:, cut : 2 * cut].reshape(-1)
    q_gain = gains[:, 2 * cut : 2 * cut + small].reshape(-1)
    k_gain = gains[:, 2 * cut + small : 2 * cut + 2 * small].reshape(-1)

    hits = expert_ids[0][:, :, None] == jnp.arange(n_all, dtype=jnp.int32)[None, None, :]
    dense_gates = jnp.sum(jnp.where(hits, gate_weights[0][:, :, None], 0.0), axis=1)
    my_gates = lax.all_to_all(
        jnp.transpose(dense_gates), EVERY, split_axis=0, concat_axis=0, tiled=True
    )
    blocks = 4
    groups = n_all // blocks
    span = blocks * length
    capacity = blocks * max(2, length * TOPK * 4 // (3 * n_all))
    slots = round_up(capacity, 16)
    my_gates = my_gates.reshape(groups, span)
    chosen = my_gates > 0.0
    below = (
        jnp.arange(span, dtype=jnp.int32)[:, None] < jnp.arange(span, dtype=jnp.int32)[None, :]
    ).astype(BF)
    rank = dot(chosen.astype(BF), below, ((1,), (0,))).astype(jnp.int32)
    is_slot = chosen[:, None, :] & (
        rank[:, None, :] == jnp.arange(slots, dtype=jnp.int32)[None, :, None]
    )
    pick = is_slot.astype(BF)
    slot_gates = jnp.sum(jnp.where(is_slot, my_gates[:, None, :], 0.0), axis=2)

    def to_slots(rows):
        return lax.dot_general(
            pick, rows.reshape(groups, span, width), (((2,), (1,)), ((0,), (0,))),
            preferred_element_type=F32,
        )

    def to_tokens(rows):
        return lax.dot_general(
            pick, rows.reshape(groups, slots, width), (((1,), (1,)), ((0,), (0,))),
            preferred_element_type=F32,
        )

    positions = ctx_index * length + jnp.arange(length, dtype=jnp.int32)
    cosine, sine = rope_tables(positions)
    cos_q, sin_q = cosine[None, :, None, :], sine[None, :, None, :]
    cos_k, sin_k = cosine[None], sine[None]
    wide_all = hidden_all.astype(F32)
    normed = (wide_all * rms_scale(wide_all) * first_gain).astype(BF)
    projected = dot(normed, weight_cols, ((1,), (0,)))
    queries = projected[:, :own_width].reshape(n_exp, length, heads_own, HEAD_SIZE)
    keys_raw = projected[:, own_width : own_width + HEAD_SIZE].reshape(n_exp, length, HEAD_SIZE)
    values = projected[:, own_width + HEAD_SIZE :].astype(BF)
    query_scale, key_scale = rms_scale(queries), rms_scale(keys_raw)
    query_rot = rotate(queries * query_scale * q_gain, cos_q, sin_q).astype(BF)
    key_rot = rotate(keys_raw * key_scale * k_gain, cos_k, sin_k).astype(BF)
    key_values = jnp.concatenate([key_rot.reshape(tokens, HEAD_SIZE), values], axis=1)
    key_values = lax.all_gather(key_values, "ctx", axis=0, tiled=False)
    key_values = key_values.reshape(n_ctx, n_exp, length, 2 * HEAD_SIZE)
    key_values = jnp.transpose(key_values, (1, 0, 2, 3)).reshape(n_exp, n_ctx * length, 2 * HEAD_SIZE)
    keys_all, values_all = key_values[..., :HEAD_SIZE], key_values[..., HEAD_SIZE:]

    grad_rows_all = lax.all_gather(after(grad_out[0], key_values), EVERY, axis=0, tiled=True)

    query_rows = jnp.transpose(query_rot, (0, 2, 1, 3)).reshape(n_exp, heads_own * length, HEAD_SIZE)
    key_pos = jnp.arange(n_ctx * length, dtype=jnp.int32)
    causal = key_pos[None, :] <= jnp.tile(positions, heads_own)[:, None]

    def batched(a, b, a_dim, b_dim):
        return lax.dot_general(
            a, b, (((a_dim,), (b_dim,)), ((0,), (0,))), preferred_element_type=F32
        )

    expos = jnp.where(causal, jnp.exp(batched(query_rows, keys_all, 2, 2) * factor), 0.0)
    totals = jnp.sum(expos, axis=-1, keepdims=True)
    attn_heads = (batched(expos.astype(BF), values_all, 2, 1) / totals).astype(BF)
    attn_rows = jnp.transpose(
        attn_heads.reshape(n_exp, heads_own, length, HEAD_SIZE), (0, 2, 1, 3)
    ).reshape(tokens, own_width)
    branch_part = dot(attn_rows, w_output, ((1,), (0,))).astype(BF)
    branch = lax.psum_scatter(branch_part, "exp", scatter_dimension=0, tiled=True)
    wide_in = hidden_in[0].astype(F32)
    mid = wide_in + branch.astype(F32)
    second_scale = rms_scale(mid)
    mlp_in = (mid * second_scale * second_gain).astype(BF)

    mlp_all = lax.all_gather(mlp_in, EVERY, axis=0, tiled=True)
    arrived = to_slots(mlp_all).astype(BF).reshape(groups * slots, width)
    slot_grads = (to_slots(grad_rows_all) * slot_gates[:, :, None]).astype(BF)
    slot_grads = slot_grads.reshape(groups * slots, width)
    gate_pre = dot(arrived, w_gate, ((1,), (0,)))
    up_pre = dot(arrived, w_up, ((1,), (0,)))
    sigmoid_gate = jax.nn.sigmoid(gate_pre)
    silu_gate = gate_pre * sigmoid_gate
    inner = (silu_gate * up_pre).astype(BF)
    grad_inner = dot(slot_grads, w_down, ((1,), (1,)))
    grad_gate_pre = (
        grad_inner * up_pre * sigmoid_gate * (1.0 + gate_pre * (1.0 - sigmoid_gate))
    ).astype(BF)
    grad_up_pre = (grad_inner * silu_gate).astype(BF)
    grad_expert_in = (
        dot(grad_gate_pre, w_gate, ((1,), (1,))) + dot(grad_up_pre, w_up, ((1,), (1,)))
    ).astype(BF)
    grad_mlp = lax.psum_scatter(
        to_tokens(grad_expert_in).astype(BF).reshape(n_all * length, width),
        EVERY, scatter_dimension=0, tiled=True,
    ).astype(F32)

    gradient_wide = grad_out[0].astype(F32)
    mlp_gain_part = jnp.sum(grad_mlp * mid * second_scale, axis=0)
    grad_mid = gradient_wide + norm_backward(grad_mlp, mid, second_scale, second_gain)
    branch_all = lax.all_gather(grad_mid.astype(BF), "exp", axis=0, tiled=True)

    expert_out = dot(inner, w_down, ((1,), (0,))).astype(BF)
    mixed_part = (to_tokens(expert_out) * my_gates[:, :, None]).astype(BF)
    mixed_part = mixed_part.reshape(n_all * length, width)
    mixed = lax.psum_scatter(
        after(mixed_part, branch_all), EVERY, scatter_dimension=0, tiled=True
    ).astype(F32)
    hidden_out = (mid + mixed).astype(BF)
    grad_down = dot(inner, slot_grads, ((0,), (0,)))
    grad_gate_mat = dot(arrived, grad_gate_pre, ((0,), (0,)))
    grad_up_mat = dot(arrived, grad_up_pre, ((0,), (0,)))

    grad_wout = dot(attn_rows, branch_all, ((0,), (0,))).astype(BF)
    attn_grad = dot(branch_all, w_output, ((1,), (1,))).astype(BF)
    grad_heads = jnp.transpose(
        attn_grad.reshape(n_exp, length, heads_own, HEAD_SIZE), (0, 2, 1, 3)
    ).reshape(n_exp, heads_own * length, HEAD_SIZE)
    deltas = jnp.sum(grad_heads.astype(F32) * attn_heads.astype(F32), axis=-1, keepdims=True)
    probs = jnp.where(causal, jnp.exp(batched(query_rows, keys_all, 2, 2) * factor), 0.0) / totals
    grad_scores = (
        probs * (batched(grad_heads, values_all, 2, 2) - deltas) * factor
    ).astype(BF)
    value_part = batched(probs.astype(BF), grad_heads, 1, 1)
    key_part = batched(grad_scores, query_rows, 1, 1)
    kv_part = jnp.concatenate([key_part, value_part], axis=-1).astype(BF)
    kv_part = jnp.transpose(
        kv_part.reshape(n_exp, n_ctx, length, 2 * HEAD_SIZE), (1, 0, 2, 3)
    ).reshape(n_ctx * tokens, 2 * HEAD_SIZE)
    kv_sums = lax.psum_scatter(kv_part, "ctx", scatter_dimension=0, tiled=True).astype(F32)
    grad_query_rot = batched(grad_scores, keys_all, 2, 1)
    grad_query_unit = rotation_backward(
        jnp.transpose(
            grad_query_rot.reshape(n_exp, heads_own, length, HEAD_SIZE), (0, 2, 1, 3)
        ), cos_q, sin_q,
    )
    q_gain_part = jnp.sum(grad_query_unit * queries * query_scale, axis=(0, 1, 2))
    grad_query_rows = norm_backward(grad_query_unit, queries, query_scale, q_gain).astype(BF)
    grad_query_rows = grad_query_rows.reshape(tokens, own_width)
    grad_key_unit = rotation_backward(
        kv_sums[:, :HEAD_SIZE].reshape(n_exp, length, HEAD_SIZE), cos_k, sin_k
    )
    k_gain_part = jnp.sum(grad_key_unit * keys_raw * key_scale, axis=(0, 1))
    grad_key_rows = norm_backward(grad_key_unit, keys_raw, key_scale, k_gain).astype(BF)
    grad_heads_in = jnp.concatenate(
        [
            grad_query_rows,
            grad_key_rows.reshape(tokens, HEAD_SIZE),
            kv_sums[:, HEAD_SIZE:].astype(BF),
        ],
        axis=1,
    )
    normed_part = dot(grad_heads_in, weight_cols, ((1,), (1,))).astype(BF)
    grad_normed = lax.psum_scatter(normed_part, "exp", scatter_dimension=0, tiled=True)
    first_scale = rms_scale(wide_in)
    grad_normed = grad_normed.astype(F32)
    attn_gain_part = jnp.sum(grad_normed * wide_in * first_scale, axis=0)
    grad_in = grad_mid + norm_backward(grad_normed, wide_in, first_scale, first_gain)

    wout_sum = lax.psum_scatter(grad_wout, "ctx", scatter_dimension=0, tiled=True)
    wout_sum = lax.all_gather(wout_sum, "ctx", axis=0, tiled=True).astype(F32)
    grad_cols = dot(normed, grad_heads_in, ((0,), (0,))).astype(BF)
    part_rows = rows_own // n_ctx
    grad_cols = grad_cols.reshape(n_exp, n_ctx, part_rows, packed_width)
    grad_cols = jnp.transpose(grad_cols, (1, 0, 2, 3))
    grad_cols = lax.psum_scatter(
        grad_cols.reshape(n_ctx * n_exp * part_rows, packed_width),
        "ctx", scatter_dimension=0, tiled=True,
    ).reshape(n_exp, part_rows, packed_width)
    grad_cols = lax.all_to_all(grad_cols, "exp", split_axis=0, concat_axis=0, tiled=True)
    to_row = jnp.transpose(grad_cols, (1, 0, 2))

    def join_heads(kv):
        kv = kv.reshape(part_rows, KEY_VALUE_HEADS, sharers, HEAD_SIZE).astype(F32)
        return jnp.sum(kv, axis=2).astype(BF).reshape(part_rows, KEY_VALUE_HEADS * HEAD_SIZE)

    weight_rows = jnp.concatenate(
        [
            to_row[:, :, :own_width].reshape(part_rows, query_width),
            join_heads(to_row[:, :, own_width : own_width + HEAD_SIZE]),
            join_heads(to_row[:, :, own_width + HEAD_SIZE :]),
        ],
        axis=1,
    )
    weight_rows = lax.all_gather(weight_rows, "ctx", axis=0, tiled=True).astype(F32)
    kv_width = KEY_VALUE_HEADS * HEAD_SIZE
    grad_wq = weight_rows[:, :query_width]
    grad_wk = weight_rows[:, query_width : query_width + kv_width]
    grad_wv = weight_rows[:, query_width + kv_width :]

    parts = jnp.concatenate([attn_gain_part, mlp_gain_part, q_gain_part, k_gain_part])
    parts = lax.psum(parts, EVERY)
    exp_index = lax.axis_index("exp")

    def own(start, count):
        return lax.dynamic_slice(parts, (start + exp_index * count,), (count,))

    return (
        hidden_out[None],
        grad_in[None],
        own(0, cut),
        grad_wq,
        grad_wk,
        grad_wv,
        own(2 * width, small),
        own(2 * width + HEAD_SIZE, small),
        wout_sum,
        own(width, cut),
        grad_gate_mat[None],
        grad_up_mat[None],
        grad_down[None],
    )


def solution(mesh):
    rows = P("exp", "ctx", None)
    shard, matrix, expert = P("exp"), P("exp", None), P(("ctx", "exp"), None, None)
    in_specs = (
        rows, rows, rows, shard, matrix, matrix, matrix, shard, shard, matrix, shard,
        expert, expert, expert, rows,
    )
    out_specs = (
        rows, rows, shard, matrix, matrix, matrix, shard, shard, matrix, shard,
        expert, expert, expert,
    )
    return jax.shard_map(
        per_device, mesh=mesh, in_specs=in_specs, out_specs=out_specs, check_vma=False
    )
```

```python
import functools

import jax
import jax.numpy as jnp
from jax import lax
from jax.experimental import pallas as pl
from jax.experimental.pallas import tpu as pltpu
from jax.sharding import PartitionSpec as P


KEY_VALUE_HEADS = 4
HEAD_SIZE = 128
TOPK = 8

EPSILON = 1e-06
THETA = 1000000.0

BF = jnp.bfloat16
F32 = jnp.float32


def rms_scale(tensor):
    return lax.rsqrt(jnp.mean(tensor * tensor, axis=-1, keepdims=True) + EPSILON)


def norm_backward(cotangent, tensor, factor, weight):
    scaled = cotangent * weight
    unit_form = tensor * factor
    return factor * (scaled - unit_form * jnp.mean(scaled * unit_form, axis=-1, keepdims=True))


def rope_tables(positions):
    halfway = HEAD_SIZE // 2
    frequency = THETA ** (-(jnp.arange(halfway, dtype=F32) * (2.0 / HEAD_SIZE)))
    angles = positions.astype(F32)[:, None] * frequency[None, :]
    cosine = jnp.concatenate([jnp.cos(angles), jnp.cos(angles)], axis=-1)
    sine = jnp.concatenate([jnp.sin(angles), jnp.sin(angles)], axis=-1)
    return cosine, sine


def rotate(tensor, cosine, sine):
    halfway = tensor.shape[-1] // 2
    turned = jnp.concatenate([-tensor[..., halfway:], tensor[..., :halfway]], axis=-1)
    return tensor * cosine + turned * sine


def rotation_backward(cotangent, cosine, sine):
    halfway = cotangent.shape[-1] // 2
    sine_part = cotangent * sine
    turned = jnp.concatenate([sine_part[..., halfway:], -sine_part[..., :halfway]], axis=-1)
    return cotangent * cosine + turned


def dot(a, b, dims):
    return lax.dot_general(a, b, (dims, ((), ())), preferred_element_type=F32)


def after(value, *earlier):
    return lax.optimization_barrier((value,) + earlier)[0]


def round_up(number, multiple):
    return -(-number // multiple) * multiple


MESH = pl.DeviceIdType.MESH


def line_sum_steps(n_ctx, chunks, part, finish, line, lag=2):
    (from_left, from_right, to_right, to_left, right_send, right_recv, left_send, left_recv) = line
    ctx, last = lax.axis_index("ctx"), n_ctx - 1

    def copy_right(k):
        return pltpu.make_async_remote_copy(
            src_ref=to_right.at[k], dst_ref=from_left.at[k],
            send_sem=right_send.at[k], recv_sem=right_recv.at[k],
            device_id={"ctx": ctx + 1}, device_id_type=MESH,
        )

    def copy_left(k):
        return pltpu.make_async_remote_copy(
            src_ref=to_left.at[k], dst_ref=from_right.at[k],
            send_sem=left_send.at[k], recv_sem=left_recv.at[k],
            device_id={"ctx": ctx - 1}, device_id_type=MESH,
        )

    def step(time, carry):
        k_right = time - lag * ctx
        k_left = time - lag * (last - ctx)
        k_done = time - lag * jnp.maximum(ctx, last - ctx)

        @pl.when((k_right >= 0) & (k_right < chunks))
        def _():
            @pl.when(ctx == 0)
            def _():
                to_right[k_right] = part(k_right).astype(BF)

            @pl.when(ctx > 0)
            def _():
                copy_right(k_right).wait_recv()
                to_right[k_right] = (part(k_right) + from_left[k_right].astype(F32)).astype(BF)

            @pl.when(ctx < last)
            def _():
                copy_right(k_right).start()

        @pl.when((k_left >= 0) & (k_left < chunks))
        def _():
            @pl.when(ctx == last)
            def _():
                to_left[k_left] = part(k_left).astype(BF)

            @pl.when(ctx < last)
            def _():
                copy_left(k_left).wait_recv()
                to_left[k_left] = (part(k_left) + from_right[k_left].astype(F32)).astype(BF)

            @pl.when(ctx > 0)
            def _():
                copy_left(k_left).start()

        @pl.when((k_done >= 0) & (k_done < chunks))
        def _():
            @pl.when(ctx == last)
            def _():
                finish(k_done, to_right[k_done].astype(F32))

            @pl.when(ctx < last)
            def _():
                finish(k_done, to_right[k_done].astype(F32) + from_right[k_done].astype(F32))

        return carry

    lax.fori_loop(0, chunks + lag * last, step, 0)

    def drain(k, carry):
        @pl.when(ctx < last)
        def _():
            copy_right(k).wait_send()

        @pl.when(ctx > 0)
        def _():
            copy_left(k).wait_send()

        return carry

    lax.fori_loop(0, chunks, drain, 0)


def greet(n_line, others):
    barrier = pltpu.get_barrier_semaphore()
    for other in others:
        pl.semaphore_signal(barrier, inc=1, device_id=other, device_id_type=MESH)
    if n_line == 1:
        pl.semaphore_wait(barrier, len(others))
        return
    ctx, last = lax.axis_index("ctx"), n_line - 1

    @pl.when(ctx > 0)
    def _():
        pl.semaphore_signal(barrier, inc=1, device_id={"ctx": ctx - 1}, device_id_type=MESH)

    @pl.when(ctx < last)
    def _():
        pl.semaphore_signal(barrier, inc=1, device_id={"ctx": ctx + 1}, device_id_type=MESH)

    at_end = (ctx == 0) | (ctx == last)

    @pl.when(at_end)
    def _():
        pl.semaphore_wait(barrier, len(others) + 1)

    @pl.when(jnp.logical_not(at_end))
    def _():
        pl.semaphore_wait(barrier, len(others) + 2)


def line_buffers(chunks, rows, width):
    slots = pltpu.VMEM((chunks, rows, width), BF)
    sems = pltpu.SemaphoreType.DMA((chunks,))
    return [slots] * 4 + [sems] * 4


def line_sum_kernel(n_ctx, chunks, x_ref, out_ref, *line):
    greet(n_ctx, [])

    def finish(k, value):
        out_ref[k] = value

    line_sum_steps(n_ctx, chunks, lambda k: x_ref[k].astype(F32), finish, line)


def line_sum(x, n_ctx, chunks=16):
    total, width = x.shape
    rows = total // chunks
    out = pl.pallas_call(
        functools.partial(line_sum_kernel, n_ctx, chunks),
        out_shape=jax.ShapeDtypeStruct((chunks, rows, width), F32),
        in_specs=[pl.BlockSpec(memory_space=pltpu.VMEM)],
        out_specs=pl.BlockSpec(memory_space=pltpu.VMEM),
        scratch_shapes=line_buffers(chunks, rows, width),
        compiler_params=pltpu.CompilerParams(
            collective_id=2, has_side_effects=True, vmem_limit_bytes=40 * 1024 * 1024
        ),
    )(x.reshape(chunks, rows, width))
    return out.reshape(total, width)


def column_sum_kernel(n_ctx, n_exp, subs, x_ref, out_ref, whole, plane_send, plane_recv, own_sem, *line):
    exp = lax.axis_index("exp")
    chunks = n_exp * subs
    greet(n_ctx, [{"exp": lax.rem(exp + hop, n_exp)} for hop in range(1, n_exp)])

    def copy_plane(k):
        hop, sub = k // subs, lax.rem(k, subs)
        return pltpu.make_async_remote_copy(
            src_ref=whole.at[k], dst_ref=out_ref.at[exp, sub],
            send_sem=plane_send.at[k], recv_sem=plane_recv.at[k],
            device_id={"exp": lax.rem(exp + hop, n_exp)}, device_id_type=MESH,
        )

    def copy_own(k):
        return pltpu.make_async_copy(whole.at[k], out_ref.at[exp, k], own_sem.at[k])

    def part(k):
        owner = lax.rem(exp + k // subs, n_exp)
        return x_ref[owner * subs + lax.rem(k, subs)].astype(F32)

    def finish(k, value):
        whole[k] = value.astype(BF)

        @pl.when(k < subs)
        def _():
            copy_own(k).start()

        @pl.when(k >= subs)
        def _():
            copy_plane(k).start()

    line_sum_steps(n_ctx, chunks, part, finish, line)

    def drain(k, carry):
        @pl.when(k < subs)
        def _():
            copy_own(k).wait()

        @pl.when(k >= subs)
        def _():
            copy_plane(k).wait()

        return carry

    lax.fori_loop(0, chunks, drain, 0)


def column_sum(x, n_ctx, n_exp, subs=2):
    total, width = x.shape
    rows = total // n_exp // subs
    chunks = n_exp * subs
    sems = pltpu.SemaphoreType.DMA((chunks,))
    out = pl.pallas_call(
        functools.partial(column_sum_kernel, n_ctx, n_exp, subs),
        out_shape=jax.ShapeDtypeStruct((n_exp, subs, rows, width), BF),
        in_specs=[pl.BlockSpec(memory_space=pltpu.VMEM)],
        out_specs=pl.BlockSpec(memory_space=pltpu.VMEM),
        scratch_shapes=[
            pltpu.VMEM((chunks, rows, width), BF), sems, sems, pltpu.SemaphoreType.DMA((subs,)),
        ] + line_buffers(chunks, rows, width),
        compiler_params=pltpu.CompilerParams(
            collective_id=1, has_side_effects=True, vmem_limit_bytes=48 * 1024 * 1024
        ),
    )(x.reshape(chunks, rows, width))
    return out.reshape(n_exp, subs * rows, width)


def gather_kernel(n_line, x_ref, out_ref, *sems):
    (z_send, x_send, y_send, d_send, p_send, z_recv, x_recv, y_recv, d_recv, p_recv, own_sem) = sems
    exp = lax.axis_index("exp")
    ctx = lax.axis_index("ctx") if n_line > 1 else 0
    last = n_line - 1

    def flip(bit):
        return exp + bit - 2 * bit * lax.rem(exp // bit, 2)

    over_core, over_x, over_y = flip(1), flip(2), flip(4)
    over_both = over_x + over_y - exp
    greet(n_line, [{"exp": other} for other in (over_core, over_x, over_y)])

    def send(src, place, half, send_sem, recv_sem, device):
        return pltpu.make_async_remote_copy(
            src_ref=src, dst_ref=out_ref.at[place[0], place[1], half],
            send_sem=send_sem, recv_sem=recv_sem, device_id=device, device_id_type=MESH,
        )

    def held(block, line, half):
        return out_ref.at[block, line, half]

    def to_z(src, line, half, way):
        step = 2 * way - 1
        return send(
            src, (exp, line), half, z_send.at[way, line, half], z_recv.at[line, half],
            {"ctx": ctx + step},
        )

    def to_x(src, line, half):
        return send(src, (exp, line), half, x_send.at[line, half], x_recv.at[line, half], {"exp": over_x})

    def to_y(src, line, half):
        return send(src, (exp, line), half, y_send.at[line, half], y_recv.at[line, half], {"exp": over_y})

    def across(line, half):
        block, device = ((over_x, over_y), (over_y, over_x))[half]
        return send(
            held(block, line, half), (block, line), half, d_send.at[line, half],
            d_recv.at[line, half], {"exp": device},
        )

    blocks = (exp, over_x, over_y, over_both)

    def to_core(src, which, line, half):
        return send(
            src, (blocks[which], line), half, p_send.at[which, line, half],
            p_recv.at[which, line, half], {"exp": over_core},
        )

    def when(cond, body):
        if cond is True:
            body()
        else:
            pl.when(cond)(body)

    def own(half):
        return pltpu.make_async_copy(x_ref.at[half], held(exp, ctx, half), own_sem.at[half])

    def place(distance, way):
        line = ctx - (2 * way - 1) * distance
        return line, (True if distance == 0 else (line >= 0) & (line <= last))

    def along(distance, way):
        line, there = place(distance, way)

        def body():
            for half in (0, 1):
                src = x_ref.at[half] if distance == 0 else held(exp, line, half)
                if distance:
                    to_z(src, line, half, way).wait_recv()
                if n_line > 1:
                    for onward in (0, 1) if distance == 0 else (way,):
                        @pl.when((ctx > 0) if onward == 0 else (ctx < last))
                        def _():
                            to_z(src, line, half, onward).start()
            for half in (0, 1):
                src = [x_ref.at[h] if distance == 0 else held(exp, line, h) for h in (0, 1)]
                to_x(src[half], line, half).start()
                to_y(src[1 - half], line, 1 - half).start()
            for half in (0, 1):
                to_core(src[half], 0, line, half).start()

        when(there, body)

    def plane(distance, way):
        line, there = place(distance, way)

        def body():
            to_x(held(over_x, line, 0), line, 0).wait_recv()
            across(line, 0).start()
            to_y(held(over_y, line, 1), line, 1).wait_recv()
            across(line, 1).start()
            to_core(held(over_x, line, 0), 1, line, 0).start()
            to_core(held(over_y, line, 1), 2, line, 1).start()
            to_x(held(over_x, line, 1), line, 1).wait_recv()
            to_core(held(over_x, line, 1), 1, line, 1).start()
            to_y(held(over_y, line, 0), line, 0).wait_recv()
            to_core(held(over_y, line, 0), 2, line, 0).start()

        when(there, body)

    def corner(distance, way):
        line, there = place(distance, way)

        def body():
            for half in (0, 1):
                across(line, half).wait_recv()
                to_core(held(over_both, line, half), 3, line, half).start()

        when(there, body)

    def finish(distance, way):
        line, there = place(distance, way)

        def body():
            for half in (0, 1):
                src = x_ref.at[half] if distance == 0 else held(exp, line, half)
                for which in range(4):
                    from_core = to_core(src, which, line, half)
                    from_core.wait_recv()
                    from_core.wait_send()
                to_x(src, line, half).wait_send()
                to_y(src, line, half).wait_send()
                across(line, half).wait_send()
                if n_line > 1:
                    for onward in (0, 1) if distance == 0 else (way,):
                        @pl.when((ctx > 0) if onward == 0 else (ctx < last))
                        def _():
                            to_z(src, line, half, onward).wait_send()

        when(there, body)

    def everywhere(stage, distance):
        if 0 <= distance < n_line:
            for way in (1,) if distance == 0 else (1, 0):
                stage(distance, way)

    for half in (0, 1):
        own(half).start()
    for time in range(n_line + 2):
        everywhere(along, time)
        everywhere(plane, time - 1)
        everywhere(corner, time - 2)
    for distance in range(n_line):
        everywhere(finish, distance)
    for half in (0, 1):
        own(half).wait()


def gather_rows(x, n_line, n_exp, collective_id):
    rows, width = x.shape
    if n_exp != 8:
        if n_line > 1:
            x = lax.all_gather(x, "ctx", axis=0, tiled=True)
        return lax.all_gather(x, "exp", axis=0, tiled=False)
    dma = pltpu.SemaphoreType.DMA
    pair, four = dma((n_line, 2)), dma((4, n_line, 2))
    out = pl.pallas_call(
        functools.partial(gather_kernel, n_line),
        out_shape=jax.ShapeDtypeStruct((n_exp, n_line, 2, rows // 2, width), x.dtype),
        in_specs=[pl.BlockSpec(memory_space=pltpu.VMEM)],
        out_specs=pl.BlockSpec(memory_space=pl.ANY),
        scratch_shapes=[
            dma((2, n_line, 2)), pair, pair, pair, four, pair, pair, pair, pair, four, dma((2,)),
        ],
        compiler_params=pltpu.CompilerParams(
            collective_id=collective_id, has_side_effects=True
        ),
    )(x.reshape(2, rows // 2, width))
    return out.reshape(n_exp, n_line * rows, width)


def per_device(
    hidden_in,
    expert_ids,
    gate_weights,
    attn_gain,
    w_query,
    key_projection,
    value_projection,
    query_gain,
    key_norm_gain,
    w_output,
    mlp_gain,
    w_gate,
    w_up,
    w_down,
    grad_out,
):
    length, width = hidden_in.shape[1:]
    n_ctx, n_exp = lax.axis_size("ctx"), lax.axis_size("exp")
    n_all = n_ctx * n_exp
    ctx_index = lax.axis_index("ctx")
    rows_own, query_width = w_query.shape
    heads_own = query_width // HEAD_SIZE // n_exp
    own_width = heads_own * HEAD_SIZE
    sharers = n_exp // KEY_VALUE_HEADS
    tokens = n_exp * length
    holds_keys = lax.rem(lax.axis_index("exp"), 2) == 0
    pairs = [(i, i ^ 1) for i in range(n_exp)]
    factor = HEAD_SIZE ** (-0.5)
    w_gate, w_up, w_down = w_gate[0], w_up[0], w_down[0]

    def heads_of(kv):
        return kv.reshape(rows_own, KEY_VALUE_HEADS, 1, HEAD_SIZE)

    halves = jnp.concatenate([heads_of(key_projection), heads_of(value_projection)], axis=2)
    halves = jnp.broadcast_to(
        halves[:, :, None], (rows_own, KEY_VALUE_HEADS, sharers // 2, 2, HEAD_SIZE)
    ).reshape(rows_own, n_exp, HEAD_SIZE)
    packed = jnp.concatenate([w_query.reshape(rows_own, n_exp, own_width), halves], axis=2)
    packed_width = own_width + HEAD_SIZE
    packed = jnp.transpose(packed, (1, 0, 2))
    gains = jnp.concatenate([attn_gain, mlp_gain, query_gain, key_norm_gain])
    gain_rows = round_up(round_up(gains.shape[0], packed_width) // packed_width, 16)
    gains = jnp.pad(gains, (0, gain_rows * packed_width - gains.shape[0]))
    gains = jnp.broadcast_to(gains.reshape(1, gain_rows, packed_width), (n_exp, gain_rows, packed_width))
    hidden_all = lax.all_gather(hidden_in[0], "exp", axis=0, tiled=True)
    heads_in = lax.all_to_all(
        jnp.concatenate([packed, gains], axis=1), "exp", split_axis=0, concat_axis=0, tiled=True
    )
    weight_cols = heads_in[:, :rows_own].reshape(n_exp * rows_own, packed_width)
    gains = heads_in[:, rows_own:].reshape(n_exp, gain_rows * packed_width).astype(F32)
    cut = attn_gain.shape[0]
    small = query_gain.shape[0]
    first_gain = gains[:, :cut].reshape(-1)
    second_gain = gains[:, cut : 2 * cut].reshape(-1)
    q_gain = gains[:, 2 * cut : 2 * cut + small].reshape(-1)
    k_gain = gains[:, 2 * cut + small : 2 * cut + 2 * small].reshape(-1)

    hits = expert_ids[0][:, :, None] == jnp.arange(n_all, dtype=jnp.int32)[None, None, :]
    dense_gates = jnp.sum(jnp.where(hits, gate_weights[0][:, :, None], 0.0), axis=1)
    column_gates = lax.all_gather(dense_gates, "ctx", axis=0, tiled=True)
    span = n_ctx * length
    slots = round_up(n_ctx * max(2, length * TOPK * 4 // (3 * n_all)), 8)
    below = (
        jnp.arange(span, dtype=jnp.int32)[:, None] < jnp.arange(span, dtype=jnp.int32)[None, :]
    ).astype(BF)

    def in_slots(chosen):
        rank = dot(chosen.astype(BF), below, ((1,), (0,))).astype(jnp.int32)
        return chosen[:, None, :] & (
            rank[:, None, :] == jnp.arange(slots, dtype=jnp.int32)[None, :, None]
        )

    plane_gates = jnp.transpose(
        lax.dynamic_slice(column_gates, (0, ctx_index * n_exp), (span, n_exp))
    )
    chosen = plane_gates > 0.0
    is_slot = in_slots(chosen)
    pick = is_slot.astype(BF).reshape(n_exp * slots, span)
    weighted = jnp.where(is_slot, plane_gates[:, None, :], 0.0).reshape(n_exp * slots, span)
    slot_gates = jnp.sum(weighted, axis=1, keepdims=True)
    pick_high = weighted.astype(BF)
    pick_low = (weighted - pick_high.astype(F32)).astype(BF)

    def exchange(rows):
        rows = rows.astype(BF).reshape(n_exp, slots, width)
        rows = lax.all_to_all(rows, "exp", split_axis=0, concat_axis=0, tiled=True)
        return rows.reshape(n_exp * slots, width)

    grad_column = lax.all_gather(grad_out[0], "ctx", axis=0, tiled=True)
    slot_grads = dot(pick, grad_column, ((1,), (0,))) * slot_gates
    pattern = jnp.pad(chosen.astype(BF)[:, None, :], ((0, 0), (0, 7), (0, width - span)))
    sent = jnp.concatenate([slot_grads.astype(BF).reshape(n_exp, slots, width), pattern], axis=1)
    received = lax.all_to_all(sent, "exp", split_axis=0, concat_axis=0, tiled=True)
    slot_grads = received[:, :slots].reshape(n_exp * slots, width)
    take = in_slots(received[:, slots, :span] > 0.5).astype(BF)

    positions = ctx_index * length + jnp.arange(length, dtype=jnp.int32)
    cosine, sine = rope_tables(positions)
    cos_q, sin_q = cosine[None, :, None, :], sine[None, :, None, :]
    cos_k, sin_k = cosine[None], sine[None]
    wide_all = hidden_all.astype(F32)
    normed = (wide_all * rms_scale(wide_all) * first_gain).astype(BF)
    projected = dot(normed, weight_cols, ((1,), (0,)))
    queries = projected[:, :own_width].reshape(n_exp, length, heads_own, HEAD_SIZE)
    own_raw = projected[:, own_width:].reshape(n_exp, length, HEAD_SIZE)
    query_scale, key_scale = rms_scale(queries), rms_scale(own_raw)
    query_rot = rotate(queries * query_scale * q_gain, cos_q, sin_q).astype(BF)
    key_rot = rotate(own_raw * key_scale * k_gain, cos_k, sin_k).astype(BF)
    own_half = jnp.where(holds_keys, key_rot, own_raw.astype(BF)).reshape(tokens, HEAD_SIZE)
    own_half = lax.all_gather(own_half, "ctx", axis=0, tiled=True)
    other_half = lax.ppermute(own_half, "exp", pairs)

    def by_sequence(half):
        half = half.reshape(n_ctx, n_exp, length, HEAD_SIZE)
        return jnp.transpose(half, (1, 0, 2, 3)).reshape(n_exp, n_ctx * length, HEAD_SIZE)

    keys_all = by_sequence(jnp.where(holds_keys, own_half, other_half))
    values_all = by_sequence(jnp.where(holds_keys, other_half, own_half))

    query_rows = jnp.transpose(query_rot, (0, 2, 1, 3)).reshape(n_exp, heads_own * length, HEAD_SIZE)
    key_pos = jnp.arange(n_ctx * length, dtype=jnp.int32)
    causal = key_pos[None, :] <= jnp.tile(positions, heads_own)[:, None]

    def batched(a, b, a_dim, b_dim):
        return lax.dot_general(
            a, b, (((a_dim,), (b_dim,)), ((0,), (0,))), preferred_element_type=F32
        )

    expos = jnp.where(causal, jnp.exp(batched(query_rows, keys_all, 2, 2) * factor), 0.0)
    totals = jnp.sum(expos, axis=-1, keepdims=True)
    attn_heads = (batched(expos.astype(BF), values_all, 2, 1) / totals).astype(BF)
    attn_rows = jnp.transpose(
        attn_heads.reshape(n_exp, heads_own, length, HEAD_SIZE), (0, 2, 1, 3)
    ).reshape(tokens, own_width)
    branch_part = dot(attn_rows, w_output, ((1,), (0,))).astype(BF)
    branch = lax.psum_scatter(branch_part, "exp", scatter_dimension=0, tiled=True)
    wide_in = hidden_in[0].astype(F32)
    mid = wide_in + branch.astype(F32)
    second_scale = rms_scale(mid)
    mlp_in = (mid * second_scale * second_gain).astype(BF)

    mlp_all = gather_rows(after(mlp_in, take), n_ctx, n_exp, 3)
    arrived = lax.dot_general(
        take, mlp_all, (((2,), (1,)), ((0,), (0,))), preferred_element_type=F32
    ).astype(BF).reshape(n_exp * slots, width)
    gate_pre = dot(arrived, w_gate, ((1,), (0,)))
    up_pre = dot(arrived, w_up, ((1,), (0,)))
    sigmoid_gate = jax.nn.sigmoid(gate_pre)
    silu_gate = gate_pre * sigmoid_gate
    inner = (silu_gate * up_pre).astype(BF)
    grad_inner = dot(slot_grads, w_down, ((1,), (1,)))
    grad_gate_pre = (
        grad_inner * up_pre * sigmoid_gate * (1.0 + gate_pre * (1.0 - sigmoid_gate))
    ).astype(BF)
    grad_up_pre = (grad_inner * silu_gate).astype(BF)
    grad_expert_in = dot(grad_gate_pre, w_gate, ((1,), (1,))) + dot(
        grad_up_pre, w_up, ((1,), (1,))
    )
    grad_back = exchange(grad_expert_in)
    grad_mlp = lax.psum_scatter(
        dot(pick, grad_back, ((0,), (0,))).astype(BF), "ctx", scatter_dimension=0, tiled=True
    ).astype(F32)

    gradient_wide = grad_out[0].astype(F32)
    mlp_gain_part = jnp.sum(grad_mlp * mid * second_scale, axis=0)
    grad_mid = gradient_wide + norm_backward(grad_mlp, mid, second_scale, second_gain)
    branch_all = gather_rows(grad_mid.astype(BF), 1, n_exp, 4)
    branch_all = branch_all.reshape(tokens, width)

    expert_out = dot(inner, w_down, ((1,), (0,))).astype(BF)
    out_back = exchange(after(expert_out, branch_all))
    mixed_part = dot(pick_high, out_back, ((0,), (0,))) + dot(pick_low, out_back, ((0,), (0,)))
    mixed = lax.psum_scatter(mixed_part.astype(BF), "ctx", scatter_dimension=0, tiled=True)
    hidden_out = (mid + mixed.astype(F32)).astype(BF)
    grad_down = dot(inner, slot_grads, ((0,), (0,)))
    grad_gate_mat = dot(arrived, grad_gate_pre, ((0,), (0,)))
    grad_up_mat = dot(arrived, grad_up_pre, ((0,), (0,)))

    grad_wout = dot(attn_rows, branch_all, ((0,), (0,))).astype(BF)
    attn_grad = dot(after(branch_all, grad_wout), w_output, ((1,), (1,))).astype(BF)
    grad_heads = jnp.transpose(
        attn_grad.reshape(n_exp, length, heads_own, HEAD_SIZE), (0, 2, 1, 3)
    ).reshape(n_exp, heads_own * length, HEAD_SIZE)
    deltas = jnp.sum(grad_heads.astype(F32) * attn_heads.astype(F32), axis=-1, keepdims=True)
    probs = jnp.where(causal, jnp.exp(batched(query_rows, keys_all, 2, 2) * factor), 0.0) / totals
    grad_scores = (
        probs * (batched(grad_heads, values_all, 2, 2) - deltas) * factor
    ).astype(BF)
    value_part = batched(probs.astype(BF), grad_heads, 1, 1)
    key_part = batched(grad_scores, query_rows, 1, 1)

    def by_position(part):
        part = part.reshape(n_exp, n_ctx, length, HEAD_SIZE)
        return jnp.transpose(part, (1, 0, 2, 3))

    key_part, value_part = by_position(key_part), by_position(value_part)
    partner = jnp.where(holds_keys, value_part, key_part).astype(BF)
    partner = lax.ppermute(partner, "exp", pairs)
    own_part = jnp.where(holds_keys, key_part, value_part) + partner.astype(F32)
    own_part = own_part.astype(BF).reshape(n_ctx, tokens, HEAD_SIZE)
    own_sums = lax.psum_scatter(
        own_part.reshape(n_ctx * tokens, HEAD_SIZE),
        "ctx", scatter_dimension=0, tiled=True,
    ).astype(F32).reshape(n_exp, length, HEAD_SIZE)
    grad_query_rot = batched(grad_scores, keys_all, 2, 1)
    grad_query_unit = rotation_backward(
        jnp.transpose(
            grad_query_rot.reshape(n_exp, heads_own, length, HEAD_SIZE), (0, 2, 1, 3)
        ), cos_q, sin_q,
    )
    q_gain_part = jnp.sum(grad_query_unit * queries * query_scale, axis=(0, 1, 2))
    grad_query_rows = norm_backward(grad_query_unit, queries, query_scale, q_gain).astype(BF)
    grad_query_rows = grad_query_rows.reshape(tokens, own_width)
    grad_key_unit = rotation_backward(own_sums, cos_k, sin_k)
    k_gain_part = jnp.sum(grad_key_unit * own_raw * key_scale, axis=(0, 1))
    k_gain_part = jnp.where(holds_keys, k_gain_part, 0.0)
    grad_own = jnp.where(
        holds_keys, norm_backward(grad_key_unit, own_raw, key_scale, k_gain), own_sums
    ).astype(BF)
    grad_heads_in = jnp.concatenate(
        [grad_query_rows, grad_own.reshape(tokens, HEAD_SIZE)], axis=1
    )
    normed_part = dot(grad_heads_in, weight_cols, ((1,), (1,))).astype(BF)
    grad_normed = lax.psum_scatter(normed_part, "exp", scatter_dimension=0, tiled=True)
    grad_normed = grad_normed.astype(F32)
    first_scale = rms_scale(wide_in)
    grad_in = grad_mid + norm_backward(grad_normed, wide_in, first_scale, first_gain)

    wout_sum = line_sum(grad_wout, n_ctx)
    grad_cols = dot(normed, grad_heads_in, ((0,), (0,))).astype(BF)
    gain_parts = jnp.concatenate(
        [
            mlp_gain_part.reshape(n_exp, cut),
            q_gain_part.reshape(n_exp, small),
            k_gain_part.reshape(n_exp, small),
        ],
        axis=1,
    )
    gain_parts = jnp.pad(gain_parts, ((0, 0), (0, packed_width - cut - 2 * small)))[:, None, :]
    gain_parts = jnp.pad(gain_parts, ((0, 0), (0, 15), (0, 0))).astype(BF)
    grad_cols = jnp.concatenate(
        [grad_cols.reshape(n_exp, rows_own, packed_width), gain_parts], axis=1
    )
    grad_cols = column_sum(grad_cols.reshape(n_exp * (rows_own + 16), packed_width), n_ctx, n_exp)
    own_gains = jnp.sum(grad_cols[:, rows_own].astype(F32), axis=0)
    grad_cols = grad_cols[:, :rows_own]
    to_row = jnp.transpose(grad_cols, (1, 0, 2))
    halves = jnp.sum(
        to_row[:, :, own_width:]
        .reshape(rows_own, KEY_VALUE_HEADS, sharers // 2, 2, HEAD_SIZE)
        .astype(F32),
        axis=2,
    )
    kv_width = KEY_VALUE_HEADS * HEAD_SIZE
    grad_wq = to_row[:, :, :own_width].reshape(rows_own, query_width).astype(F32)
    grad_wk = halves[:, :, 0].reshape(rows_own, kv_width)
    grad_wv = halves[:, :, 1].reshape(rows_own, kv_width)

    attn_gain_sum = (
        jnp.sum(w_query.astype(F32) * grad_wq, axis=1)
        + jnp.sum(key_projection.astype(F32) * grad_wk, axis=1)
        + jnp.sum(value_projection.astype(F32) * grad_wv, axis=1)
    ) / attn_gain.astype(F32)

    return (
        hidden_out[None],
        grad_in[None],
        attn_gain_sum,
        grad_wq,
        grad_wk,
        grad_wv,
        own_gains[cut : cut + small],
        own_gains[cut + small : cut + 2 * small],
        wout_sum,
        own_gains[:cut],
        grad_gate_mat[None],
        grad_up_mat[None],
        grad_down[None],
    )


def solution(mesh):
    rows = P("exp", "ctx", None)
    shard, matrix, expert = P("exp"), P("exp", None), P(("ctx", "exp"), None, None)
    in_specs = (
        rows, rows, rows, shard, matrix, matrix, matrix, shard, shard, matrix, shard,
        expert, expert, expert, rows,
    )
    out_specs = (
        rows, rows, shard, matrix, matrix, matrix, shard, shard, matrix, shard,
        expert, expert, expert,
    )
    return jax.shard_map(
        per_device, mesh=mesh, in_specs=in_specs, out_specs=out_specs, check_vma=False
    )
```

```python
import functools

import jax
import jax.numpy as jnp
from jax import lax
from jax.experimental import pallas as pl
from jax.experimental.pallas import tpu as pltpu
from jax.sharding import PartitionSpec as P


KEY_VALUE_HEADS = 4
HEAD_SIZE = 128
TOPK = 8

EPSILON = 1e-06
THETA = 1000000.0

BF = jnp.bfloat16
F32 = jnp.float32


def rms_scale(tensor):
    return lax.rsqrt(jnp.mean(tensor * tensor, axis=-1, keepdims=True) + EPSILON)


def norm_backward(cotangent, tensor, factor, weight):
    scaled = cotangent * weight
    unit_form = tensor * factor
    return factor * (scaled - unit_form * jnp.mean(scaled * unit_form, axis=-1, keepdims=True))


def rope_tables(positions):
    halfway = HEAD_SIZE // 2
    frequency = THETA ** (-(jnp.arange(halfway, dtype=F32) * (2.0 / HEAD_SIZE)))
    angles = positions.astype(F32)[:, None] * frequency[None, :]
    cosine = jnp.concatenate([jnp.cos(angles), jnp.cos(angles)], axis=-1)
    sine = jnp.concatenate([jnp.sin(angles), jnp.sin(angles)], axis=-1)
    return cosine, sine


def rotate(tensor, cosine, sine):
    halfway = tensor.shape[-1] // 2
    turned = jnp.concatenate([-tensor[..., halfway:], tensor[..., :halfway]], axis=-1)
    return tensor * cosine + turned * sine


def rotation_backward(cotangent, cosine, sine):
    halfway = cotangent.shape[-1] // 2
    sine_part = cotangent * sine
    turned = jnp.concatenate([sine_part[..., halfway:], -sine_part[..., :halfway]], axis=-1)
    return cotangent * cosine + turned


def dot(a, b, dims):
    return lax.dot_general(a, b, (dims, ((), ())), preferred_element_type=F32)


def after(value, *earlier):
    return lax.optimization_barrier((value,) + earlier)[0]


def round_up(number, multiple):
    return -(-number // multiple) * multiple


MESH = pl.DeviceIdType.MESH


def line_sum_steps(n_ctx, chunks, part, finish, line, lag=2):
    (from_left, from_right, to_right, to_left, right_send, right_recv, left_send, left_recv) = line
    ctx, last = lax.axis_index("ctx"), n_ctx - 1

    def copy_right(k):
        return pltpu.make_async_remote_copy(
            src_ref=to_right.at[k], dst_ref=from_left.at[k],
            send_sem=right_send.at[k], recv_sem=right_recv.at[k],
            device_id={"ctx": ctx + 1}, device_id_type=MESH,
        )

    def copy_left(k):
        return pltpu.make_async_remote_copy(
            src_ref=to_left.at[k], dst_ref=from_right.at[k],
            send_sem=left_send.at[k], recv_sem=left_recv.at[k],
            device_id={"ctx": ctx - 1}, device_id_type=MESH,
        )

    def step(time, carry):
        k_right = time - lag * ctx
        k_left = time - lag * (last - ctx)
        k_done = time - lag * jnp.maximum(ctx, last - ctx)

        @pl.when((k_right >= 0) & (k_right < chunks))
        def _():
            @pl.when(ctx == 0)
            def _():
                to_right[k_right] = part(k_right).astype(BF)

            @pl.when(ctx > 0)
            def _():
                copy_right(k_right).wait_recv()
                to_right[k_right] = (part(k_right) + from_left[k_right].astype(F32)).astype(BF)

            @pl.when(ctx < last)
            def _():
                copy_right(k_right).start()

        @pl.when((k_left >= 0) & (k_left < chunks))
        def _():
            @pl.when(ctx == last)
            def _():
                to_left[k_left] = part(k_left).astype(BF)

            @pl.when(ctx < last)
            def _():
                copy_left(k_left).wait_recv()
                to_left[k_left] = (part(k_left) + from_right[k_left].astype(F32)).astype(BF)

            @pl.when(ctx > 0)
            def _():
                copy_left(k_left).start()

        @pl.when((k_done >= 0) & (k_done < chunks))
        def _():
            @pl.when(ctx == last)
            def _():
                finish(k_done, to_right[k_done].astype(F32))

            @pl.when(ctx < last)
            def _():
                finish(k_done, to_right[k_done].astype(F32) + from_right[k_done].astype(F32))

        return carry

    lax.fori_loop(0, chunks + lag * last, step, 0)

    def drain(k, carry):
        @pl.when(ctx < last)
        def _():
            copy_right(k).wait_send()

        @pl.when(ctx > 0)
        def _():
            copy_left(k).wait_send()

        return carry

    lax.fori_loop(0, chunks, drain, 0)


def greet(n_line, others):
    barrier = pltpu.get_barrier_semaphore()
    for other in others:
        pl.semaphore_signal(barrier, inc=1, device_id=other, device_id_type=MESH)
    if n_line == 1:
        pl.semaphore_wait(barrier, len(others))
        return
    ctx, last = lax.axis_index("ctx"), n_line - 1

    @pl.when(ctx > 0)
    def _():
        pl.semaphore_signal(barrier, inc=1, device_id={"ctx": ctx - 1}, device_id_type=MESH)

    @pl.when(ctx < last)
    def _():
        pl.semaphore_signal(barrier, inc=1, device_id={"ctx": ctx + 1}, device_id_type=MESH)

    at_end = (ctx == 0) | (ctx == last)

    @pl.when(at_end)
    def _():
        pl.semaphore_wait(barrier, len(others) + 1)

    @pl.when(jnp.logical_not(at_end))
    def _():
        pl.semaphore_wait(barrier, len(others) + 2)


def line_buffers(chunks, rows, width):
    slots = pltpu.VMEM((chunks, rows, width), BF)
    sems = pltpu.SemaphoreType.DMA((chunks,))
    return [slots] * 4 + [sems] * 4


def line_sum_kernel(n_ctx, chunks, x_ref, out_ref, *line):
    greet(n_ctx, [])

    def finish(k, value):
        out_ref[k] = value

    line_sum_steps(n_ctx, chunks, lambda k: x_ref[k].astype(F32), finish, line)


def line_sum(x, n_ctx, chunks=16):
    total, width = x.shape
    rows = total // chunks
    out = pl.pallas_call(
        functools.partial(line_sum_kernel, n_ctx, chunks),
        out_shape=jax.ShapeDtypeStruct((chunks, rows, width), F32),
        in_specs=[pl.BlockSpec(memory_space=pltpu.VMEM)],
        out_specs=pl.BlockSpec(memory_space=pltpu.VMEM),
        scratch_shapes=line_buffers(chunks, rows, width),
        compiler_params=pltpu.CompilerParams(
            collective_id=2, has_side_effects=True, vmem_limit_bytes=40 * 1024 * 1024
        ),
    )(x.reshape(chunks, rows, width))
    return out.reshape(total, width)


def column_sum_kernel(n_ctx, n_exp, subs, x_ref, out_ref, whole, plane_send, plane_recv, own_sem, *line):
    exp = lax.axis_index("exp")
    chunks = n_exp * subs
    greet(n_ctx, [{"exp": lax.rem(exp + hop, n_exp)} for hop in range(1, n_exp)])

    def copy_plane(k):
        hop, sub = k // subs, lax.rem(k, subs)
        return pltpu.make_async_remote_copy(
            src_ref=whole.at[k], dst_ref=out_ref.at[exp, sub],
            send_sem=plane_send.at[k], recv_sem=plane_recv.at[k],
            device_id={"exp": lax.rem(exp + hop, n_exp)}, device_id_type=MESH,
        )

    def copy_own(k):
        return pltpu.make_async_copy(whole.at[k], out_ref.at[exp, k], own_sem.at[k])

    def part(k):
        owner = lax.rem(exp + k // subs, n_exp)
        return x_ref[owner * subs + lax.rem(k, subs)].astype(F32)

    def finish(k, value):
        whole[k] = value.astype(BF)

        @pl.when(k < subs)
        def _():
            copy_own(k).start()

        @pl.when(k >= subs)
        def _():
            copy_plane(k).start()

    line_sum_steps(n_ctx, chunks, part, finish, line)

    def drain(k, carry):
        @pl.when(k < subs)
        def _():
            copy_own(k).wait()

        @pl.when(k >= subs)
        def _():
            copy_plane(k).wait()

        return carry

    lax.fori_loop(0, chunks, drain, 0)


def column_sum(x, n_ctx, n_exp, subs=2):
    total, width = x.shape
    rows = total // n_exp // subs
    chunks = n_exp * subs
    sems = pltpu.SemaphoreType.DMA((chunks,))
    out = pl.pallas_call(
        functools.partial(column_sum_kernel, n_ctx, n_exp, subs),
        out_shape=jax.ShapeDtypeStruct((n_exp, subs, rows, width), BF),
        in_specs=[pl.BlockSpec(memory_space=pltpu.VMEM)],
        out_specs=pl.BlockSpec(memory_space=pltpu.VMEM),
        scratch_shapes=[
            pltpu.VMEM((chunks, rows, width), BF), sems, sems, pltpu.SemaphoreType.DMA((subs,)),
        ] + line_buffers(chunks, rows, width),
        compiler_params=pltpu.CompilerParams(
            collective_id=1, has_side_effects=True, vmem_limit_bytes=48 * 1024 * 1024
        ),
    )(x.reshape(chunks, rows, width))
    return out.reshape(n_exp, subs * rows, width)


def gather_kernel(n_line, x_ref, out_ref, *sems):
    (z_send, x_send, y_send, d_send, p_send, z_recv, x_recv, y_recv, d_recv, p_recv, own_sem) = sems
    exp = lax.axis_index("exp")
    ctx = lax.axis_index("ctx") if n_line > 1 else 0
    last = n_line - 1

    def flip(bit):
        return exp + bit - 2 * bit * lax.rem(exp // bit, 2)

    over_core, over_x, over_y = flip(1), flip(2), flip(4)
    over_both = over_x + over_y - exp
    greet(n_line, [{"exp": other} for other in (over_core, over_x, over_y)])

    def send(src, place, half, send_sem, recv_sem, device):
        return pltpu.make_async_remote_copy(
            src_ref=src, dst_ref=out_ref.at[place[0], place[1], half],
            send_sem=send_sem, recv_sem=recv_sem, device_id=device, device_id_type=MESH,
        )

    def held(block, line, half):
        return out_ref.at[block, line, half]

    def to_z(src, line, half, way):
        step = 2 * way - 1
        return send(
            src, (exp, line), half, z_send.at[way, line, half], z_recv.at[line, half],
            {"ctx": ctx + step},
        )

    def to_x(src, line, half):
        return send(src, (exp, line), half, x_send.at[line, half], x_recv.at[line, half], {"exp": over_x})

    def to_y(src, line, half):
        return send(src, (exp, line), half, y_send.at[line, half], y_recv.at[line, half], {"exp": over_y})

    def across(line, half):
        block, device = ((over_x, over_y), (over_y, over_x))[half]
        return send(
            held(block, line, half), (block, line), half, d_send.at[line, half],
            d_recv.at[line, half], {"exp": device},
        )

    blocks = (exp, over_x, over_y, over_both)

    def to_core(src, which, line, half):
        return send(
            src, (blocks[which], line), half, p_send.at[which, line, half],
            p_recv.at[which, line, half], {"exp": over_core},
        )

    def when(cond, body):
        if cond is True:
            body()
        else:
            pl.when(cond)(body)

    def own(half):
        return pltpu.make_async_copy(x_ref.at[half], held(exp, ctx, half), own_sem.at[half])

    def place(distance, way):
        line = ctx - (2 * way - 1) * distance
        return line, (True if distance == 0 else (line >= 0) & (line <= last))

    def along(distance, way):
        line, there = place(distance, way)

        def body():
            for half in (0, 1):
                src = x_ref.at[half] if distance == 0 else held(exp, line, half)
                if distance:
                    to_z(src, line, half, way).wait_recv()
                if n_line > 1:
                    for onward in (0, 1) if distance == 0 else (way,):
                        @pl.when((ctx > 0) if onward == 0 else (ctx < last))
                        def _():
                            to_z(src, line, half, onward).start()
            for half in (0, 1):
                src = [x_ref.at[h] if distance == 0 else held(exp, line, h) for h in (0, 1)]
                to_x(src[half], line, half).start()
                to_y(src[1 - half], line, 1 - half).start()
            for half in (0, 1):
                to_core(src[half], 0, line, half).start()

        when(there, body)

    def plane(distance, way):
        line, there = place(distance, way)

        def body():
            to_x(held(over_x, line, 0), line, 0).wait_recv()
            across(line, 0).start()
            to_y(held(over_y, line, 1), line, 1).wait_recv()
            across(line, 1).start()
            to_core(held(over_x, line, 0), 1, line, 0).start()
            to_core(held(over_y, line, 1), 2, line, 1).start()
            to_x(held(over_x, line, 1), line, 1).wait_recv()
            to_core(held(over_x, line, 1), 1, line, 1).start()
            to_y(held(over_y, line, 0), line, 0).wait_recv()
            to_core(held(over_y, line, 0), 2, line, 0).start()

        when(there, body)

    def corner(distance, way):
        line, there = place(distance, way)

        def body():
            for half in (0, 1):
                across(line, half).wait_recv()
                to_core(held(over_both, line, half), 3, line, half).start()

        when(there, body)

    def finish(distance, way):
        line, there = place(distance, way)

        def body():
            for half in (0, 1):
                src = x_ref.at[half] if distance == 0 else held(exp, line, half)
                for which in range(4):
                    from_core = to_core(src, which, line, half)
                    from_core.wait_recv()
                    from_core.wait_send()
                to_x(src, line, half).wait_send()
                to_y(src, line, half).wait_send()
                across(line, half).wait_send()
                if n_line > 1:
                    for onward in (0, 1) if distance == 0 else (way,):
                        @pl.when((ctx > 0) if onward == 0 else (ctx < last))
                        def _():
                            to_z(src, line, half, onward).wait_send()

        when(there, body)

    def everywhere(stage, distance):
        if 0 <= distance < n_line:
            for way in (1,) if distance == 0 else (1, 0):
                stage(distance, way)

    for half in (0, 1):
        own(half).start()
    for time in range(n_line + 2):
        everywhere(along, time)
        everywhere(plane, time - 1)
        everywhere(corner, time - 2)
    for distance in range(n_line):
        everywhere(finish, distance)
    for half in (0, 1):
        own(half).wait()


def gather_rows(x, n_line, n_exp, collective_id):
    rows, width = x.shape
    if n_exp != 8:
        if n_line > 1:
            x = lax.all_gather(x, "ctx", axis=0, tiled=True)
        return lax.all_gather(x, "exp", axis=0, tiled=False)
    dma = pltpu.SemaphoreType.DMA
    pair, four = dma((n_line, 2)), dma((4, n_line, 2))
    out = pl.pallas_call(
        functools.partial(gather_kernel, n_line),
        out_shape=jax.ShapeDtypeStruct((n_exp, n_line, 2, rows // 2, width), x.dtype),
        in_specs=[pl.BlockSpec(memory_space=pltpu.VMEM)],
        out_specs=pl.BlockSpec(memory_space=pl.ANY),
        scratch_shapes=[
            dma((2, n_line, 2)), pair, pair, pair, four, pair, pair, pair, pair, four, dma((2,)),
        ],
        compiler_params=pltpu.CompilerParams(
            collective_id=collective_id, has_side_effects=True
        ),
    )(x.reshape(2, rows // 2, width))
    return out.reshape(n_exp, n_line * rows, width)


def reduce_kernel(x_ref, out_ref, from_core, sums, arrived, c_send, c_recv, q_send, q_recv):
    exp = lax.axis_index("exp")

    def flip(device, bit):
        return device + bit - 2 * bit * lax.rem(device // bit, 2)

    over_core, over_x, over_y = flip(exp, 1), flip(exp, 2), flip(exp, 4)
    owners = (flip(over_x, 4), over_x, over_y, exp)
    greet(1, [{"exp": other} for other in (over_core,) + owners[:3]])
    rows = 16

    def to_core(t):
        return pltpu.make_async_remote_copy(
            src_ref=x_ref.at[flip(owners[t], 1)], dst_ref=from_core.at[t],
            send_sem=c_send.at[t], recv_sem=c_recv.at[t],
            device_id={"exp": over_core}, device_id_type=MESH,
        )

    def to_owner(t):
        return pltpu.make_async_remote_copy(
            src_ref=sums.at[t], dst_ref=arrived.at[t],
            send_sem=q_send.at[t], recv_sem=q_recv.at[t],
            device_id={"exp": owners[t]}, device_id_type=MESH,
        )

    def by_rows(body):
        def step(i, carry):
            body(pl.ds(pl.multiple_of(i * rows, rows), rows))
            return carry

        lax.fori_loop(0, out_ref.shape[0] // rows, step, 0)

    for t in range(4):
        to_core(t).start()
    for t in range(4):
        to_core(t).wait_recv()

        def add(at, t=t):
            value = x_ref[owners[t], at, :].astype(F32) + from_core[t, at, :].astype(F32)
            if t < 3:
                sums[t, at, :] = value.astype(BF)
            else:
                out_ref[at, :] = value

        by_rows(add)
        if t < 3:
            to_owner(t).start()
    for t in (1, 2, 0):
        to_owner(t).wait_recv()

        def gather(at, t=t):
            out_ref[at, :] = out_ref[at, :] + arrived[t, at, :].astype(F32)

        by_rows(gather)
    for t in range(4):
        to_core(t).wait_send()
        if t < 3:
            to_owner(t).wait_send()


def reduce_rows(x, n_exp, collective_id):
    rows, width = x.shape[0] // n_exp, x.shape[1]
    if n_exp != 8:
        return lax.psum_scatter(x, "exp", scatter_dimension=0, tiled=True).astype(F32)
    dma = pltpu.SemaphoreType.DMA
    return pl.pallas_call(
        reduce_kernel,
        out_shape=jax.ShapeDtypeStruct((rows, width), F32),
        in_specs=[pl.BlockSpec(memory_space=pltpu.VMEM)],
        out_specs=pl.BlockSpec(memory_space=pltpu.VMEM),
        scratch_shapes=[
            pltpu.VMEM((4, rows, width), BF), pltpu.VMEM((3, rows, width), BF),
            pltpu.VMEM((3, rows, width), BF), dma((4,)), dma((4,)), dma((3,)), dma((3,)),
        ],
        compiler_params=pltpu.CompilerParams(
            collective_id=collective_id, has_side_effects=True, vmem_limit_bytes=32 * 1024 * 1024
        ),
    )(x.reshape(n_exp, rows, width))


def spread_kernel(
    n_exp, sharers, query_ref, halves_ref, gains_ref, out_ref, gains_out_ref,
    q_send, q_recv, h_send, h_recv, g_send, g_recv, own_sems,
):
    exp = lax.axis_index("exp")
    own_width = query_ref.shape[1] // n_exp
    greet(1, [{"exp": lax.rem(exp + hop, n_exp)} for hop in range(1, n_exp)])

    def pieces(owner):
        columns = pl.ds(pl.multiple_of(owner * own_width, own_width), own_width)
        return (
            (query_ref.at[:, columns], out_ref.at[exp, :, pl.ds(0, own_width)]),
            (
                halves_ref.at[owner // sharers, lax.rem(owner, 2)],
                out_ref.at[exp, :, pl.ds(own_width, HEAD_SIZE)],
            ),
            (gains_ref, gains_out_ref.at[exp]),
        )

    copies = []
    for hop in range(1, n_exp):
        owner = lax.rem(exp + hop, n_exp)
        for (src, dst), send, recv in zip(
            pieces(owner), (q_send, h_send, g_send), (q_recv, h_recv, g_recv)
        ):
            copies.append(
                pltpu.make_async_remote_copy(
                    src_ref=src, dst_ref=dst, send_sem=send.at[hop], recv_sem=recv.at[hop],
                    device_id={"exp": owner}, device_id_type=MESH,
                )
            )
    for i, (src, dst) in enumerate(pieces(exp)):
        copies.append(pltpu.make_async_copy(src, dst, own_sems.at[i]))
    for copy in copies:
        copy.start()
    for copy in copies:
        copy.wait()


def spread_columns(query, halves, gains, n_exp, sharers):
    rows, width = query.shape
    dma = pltpu.SemaphoreType.DMA((n_exp,))
    vmem = pl.BlockSpec(memory_space=pltpu.VMEM)
    return pl.pallas_call(
        functools.partial(spread_kernel, n_exp, sharers),
        out_shape=(
            jax.ShapeDtypeStruct((n_exp, rows, width // n_exp + HEAD_SIZE), BF),
            jax.ShapeDtypeStruct((n_exp,) + gains.shape, BF),
        ),
        in_specs=[vmem] * 3,
        out_specs=(vmem, vmem),
        scratch_shapes=[dma] * 6 + [pltpu.SemaphoreType.DMA((3,))],
        compiler_params=pltpu.CompilerParams(
            collective_id=6, has_side_effects=True, vmem_limit_bytes=24 * 1024 * 1024
        ),
    )(query, halves, gains)


def per_device(
    hidden_in,
    expert_ids,
    gate_weights,
    attn_gain,
    w_query,
    key_projection,
    value_projection,
    query_gain,
    key_norm_gain,
    w_output,
    mlp_gain,
    w_gate,
    w_up,
    w_down,
    grad_out,
):
    length, width = hidden_in.shape[1:]
    n_ctx, n_exp = lax.axis_size("ctx"), lax.axis_size("exp")
    n_all = n_ctx * n_exp
    ctx_index = lax.axis_index("ctx")
    rows_own, query_width = w_query.shape
    heads_own = query_width // HEAD_SIZE // n_exp
    own_width = heads_own * HEAD_SIZE
    sharers = n_exp // KEY_VALUE_HEADS
    tokens = n_exp * length
    holds_keys = lax.rem(lax.axis_index("exp"), 2) == 0
    pairs = [(i, i ^ 1) for i in range(n_exp)]
    factor = HEAD_SIZE ** (-0.5)
    w_gate, w_up, w_down = w_gate[0], w_up[0], w_down[0]

    def heads_of(kv):
        return kv.reshape(rows_own, KEY_VALUE_HEADS, 1, HEAD_SIZE)

    halves = jnp.concatenate([heads_of(key_projection), heads_of(value_projection)], axis=2)
    halves = jnp.transpose(halves, (1, 2, 0, 3))
    packed_width = own_width + HEAD_SIZE
    gains = jnp.concatenate([attn_gain, mlp_gain, query_gain, key_norm_gain])
    gain_rows = round_up(gains.shape[0], 16 * HEAD_SIZE) // HEAD_SIZE
    gains = jnp.pad(gains, (0, gain_rows * HEAD_SIZE - gains.shape[0]))
    hidden_all = gather_rows(hidden_in[0], 1, n_exp, 7)
    hidden_all = hidden_all.reshape(tokens, width)
    weight_cols, gains = spread_columns(
        after(w_query, hidden_all), halves, gains.reshape(gain_rows, HEAD_SIZE),
        n_exp, sharers,
    )
    weight_cols = weight_cols.reshape(n_exp * rows_own, packed_width)
    gains = gains.reshape(n_exp, gain_rows * HEAD_SIZE).astype(F32)
    cut = attn_gain.shape[0]
    small = query_gain.shape[0]
    first_gain = gains[:, :cut].reshape(-1)
    second_gain = gains[:, cut : 2 * cut].reshape(-1)
    q_gain = gains[:, 2 * cut : 2 * cut + small].reshape(-1)
    k_gain = gains[:, 2 * cut + small : 2 * cut + 2 * small].reshape(-1)

    hits = expert_ids[0][:, :, None] == jnp.arange(n_all, dtype=jnp.int32)[None, None, :]
    dense_gates = jnp.sum(jnp.where(hits, gate_weights[0][:, :, None], 0.0), axis=1)
    high = lax.reduce_precision(dense_gates, 8, 7)
    middle = lax.reduce_precision(dense_gates - high, 8, 7)
    gate_parts = jnp.concatenate([high, middle, dense_gates - high - middle], axis=1).astype(BF)
    gate_parts = jnp.pad(gate_parts, ((0, 0), (0, round_up(3 * n_all, HEAD_SIZE) - 3 * n_all)))
    grad_column = lax.all_gather(
        jnp.concatenate([grad_out[0], gate_parts], axis=1), "ctx",
        axis=0, tiled=True,
    )
    gate_parts = grad_column[:, width : width + 3 * n_all].astype(F32)
    column_gates = (
        gate_parts[:, :n_all] + gate_parts[:, n_all : 2 * n_all] + gate_parts[:, 2 * n_all :]
    )
    span = n_ctx * length
    slots = round_up(n_ctx * max(2, length * TOPK * 4 // (3 * n_all)), 8)
    below = (
        jnp.arange(span, dtype=jnp.int32)[:, None] < jnp.arange(span, dtype=jnp.int32)[None, :]
    ).astype(BF)

    def in_slots(chosen):
        rank = dot(chosen.astype(BF), below, ((1,), (0,))).astype(jnp.int32)
        return chosen[:, None, :] & (
            rank[:, None, :] == jnp.arange(slots, dtype=jnp.int32)[None, :, None]
        )

    plane_gates = jnp.transpose(
        lax.dynamic_slice(column_gates, (0, ctx_index * n_exp), (span, n_exp))
    )
    chosen = plane_gates > 0.0
    is_slot = in_slots(chosen)
    pick = is_slot.astype(BF).reshape(n_exp * slots, span)
    weighted = jnp.where(is_slot, plane_gates[:, None, :], 0.0).reshape(n_exp * slots, span)
    slot_gates = jnp.sum(weighted, axis=1, keepdims=True)
    high = lax.reduce_precision(weighted, 8, 7)
    pick_high, pick_low = high.astype(BF), (weighted - high).astype(BF)

    def exchange(rows):
        rows = rows.astype(BF).reshape(n_exp, slots, width)
        rows = lax.all_to_all(rows, "exp", split_axis=0, concat_axis=0, tiled=True)
        return rows.reshape(n_exp * slots, width)

    slot_grads = dot(pick, grad_column[:, :width], ((1,), (0,))) * slot_gates
    pattern = jnp.pad(chosen.astype(BF)[:, None, :], ((0, 0), (0, 7), (0, width - span)))
    sent = jnp.concatenate([slot_grads.astype(BF).reshape(n_exp, slots, width), pattern], axis=1)
    received = lax.all_to_all(sent, "exp", split_axis=0, concat_axis=0, tiled=True)
    slot_grads = received[:, :slots].reshape(n_exp * slots, width)
    take = in_slots(received[:, slots, :span] > 0.5).astype(BF)

    positions = ctx_index * length + jnp.arange(length, dtype=jnp.int32)
    cosine, sine = rope_tables(positions)
    cos_q, sin_q = cosine[None, :, None, :], sine[None, :, None, :]
    cos_k, sin_k = cosine[None], sine[None]
    wide_all = hidden_all.astype(F32)
    normed = (wide_all * rms_scale(wide_all) * first_gain).astype(BF)
    projected = dot(normed, weight_cols, ((1,), (0,)))
    queries = projected[:, :own_width].reshape(n_exp, length, heads_own, HEAD_SIZE)
    own_raw = projected[:, own_width:].reshape(n_exp, length, HEAD_SIZE)
    query_scale, key_scale = rms_scale(queries), rms_scale(own_raw)
    query_rot = rotate(queries * query_scale * q_gain, cos_q, sin_q).astype(BF)
    key_rot = rotate(own_raw * key_scale * k_gain, cos_k, sin_k).astype(BF)
    own_half = jnp.where(holds_keys, key_rot, own_raw.astype(BF)).reshape(tokens, HEAD_SIZE)
    own_half = lax.all_gather(own_half, "ctx", axis=0, tiled=True)
    other_half = lax.ppermute(own_half, "exp", pairs)

    def by_sequence(half):
        half = half.reshape(n_ctx, n_exp, length, HEAD_SIZE)
        return jnp.transpose(half, (1, 0, 2, 3)).reshape(n_exp, n_ctx * length, HEAD_SIZE)

    keys_all = by_sequence(jnp.where(holds_keys, own_half, other_half))
    values_all = by_sequence(jnp.where(holds_keys, other_half, own_half))

    query_rows = jnp.transpose(query_rot, (0, 2, 1, 3)).reshape(n_exp, heads_own * length, HEAD_SIZE)
    key_pos = jnp.arange(n_ctx * length, dtype=jnp.int32)
    causal = key_pos[None, :] <= jnp.tile(positions, heads_own)[:, None]

    def batched(a, b, a_dim, b_dim):
        return lax.dot_general(
            a, b, (((a_dim,), (b_dim,)), ((0,), (0,))), preferred_element_type=F32
        )

    expos = jnp.where(causal, jnp.exp(batched(query_rows, keys_all, 2, 2) * factor), 0.0)
    totals = jnp.sum(expos, axis=-1, keepdims=True)
    attn_heads = (batched(expos.astype(BF), values_all, 2, 1) / totals).astype(BF)
    attn_rows = jnp.transpose(
        attn_heads.reshape(n_exp, heads_own, length, HEAD_SIZE), (0, 2, 1, 3)
    ).reshape(tokens, own_width)
    branch_part = dot(attn_rows, w_output, ((1,), (0,))).astype(BF)
    branch = reduce_rows(branch_part, n_exp, 5)
    wide_in = hidden_in[0].astype(F32)
    mid = wide_in + branch
    second_scale = rms_scale(mid)
    mlp_in = (mid * second_scale * second_gain).astype(BF)

    mlp_all = gather_rows(after(mlp_in, take), n_ctx, n_exp, 3)
    arrived = lax.dot_general(
        take, mlp_all, (((2,), (1,)), ((0,), (0,))), preferred_element_type=F32
    ).astype(BF).reshape(n_exp * slots, width)
    gate_pre = dot(arrived, w_gate, ((1,), (0,)))
    up_pre = dot(arrived, w_up, ((1,), (0,)))
    sigmoid_gate = jax.nn.sigmoid(gate_pre)
    silu_gate = gate_pre * sigmoid_gate
    inner = (silu_gate * up_pre).astype(BF)
    grad_inner = dot(slot_grads, w_down, ((1,), (1,)))
    grad_gate_pre = (
        grad_inner * up_pre * sigmoid_gate * (1.0 + gate_pre * (1.0 - sigmoid_gate))
    ).astype(BF)
    grad_up_pre = (grad_inner * silu_gate).astype(BF)
    split = width // 2

    def give_back(at):
        rows = dot(grad_gate_pre, w_gate[at], ((1,), (1,))) + dot(grad_up_pre, w_up[at], ((1,), (1,)))
        return rows.astype(BF).reshape(n_exp, slots, split)

    def back_sum(rows):
        part = dot(pick, rows.reshape(n_exp * slots, split), ((0,), (0,))).astype(BF)
        return lax.psum_scatter(part, "ctx", scatter_dimension=0, tiled=True)

    first = lax.all_to_all(give_back(slice(0, split)), "exp", split_axis=0, concat_axis=0, tiled=True)
    second = after(give_back(slice(split, width)), first)
    second = lax.all_to_all(second, "exp", split_axis=0, concat_axis=0, tiled=True)
    grad_mlp = jnp.concatenate([back_sum(first), back_sum(second)], axis=1).astype(F32)

    gradient_wide = grad_out[0].astype(F32)
    mlp_gain_part = jnp.sum(grad_mlp * mid * second_scale, axis=0)
    grad_mid = gradient_wide + norm_backward(grad_mlp, mid, second_scale, second_gain)
    branch_all = gather_rows(grad_mid.astype(BF), 1, n_exp, 4)
    branch_all = branch_all.reshape(tokens, width)

    expert_out = dot(inner, w_down, ((1,), (0,))).astype(BF)
    out_back = exchange(after(expert_out, branch_all))
    mixed_part = dot(pick_high, out_back, ((0,), (0,))) + dot(pick_low, out_back, ((0,), (0,)))
    mixed_part = mixed_part.astype(BF)
    mixed = lax.psum_scatter(mixed_part, "ctx", scatter_dimension=0, tiled=True)
    hidden_out = (mid + mixed.astype(F32)).astype(BF)
    grad_down = dot(inner, slot_grads, ((0,), (0,)))
    grad_gate_mat = dot(arrived, grad_gate_pre, ((0,), (0,)))
    grad_up_mat = dot(arrived, grad_up_pre, ((0,), (0,)))

    grad_wout = dot(attn_rows, branch_all, ((0,), (0,))).astype(BF)
    wout_sum = line_sum(grad_wout, n_ctx)
    attn_grad = dot(after(branch_all, wout_sum), w_output, ((1,), (1,))).astype(BF)
    grad_heads = jnp.transpose(
        after(attn_grad, mixed_part).reshape(n_exp, length, heads_own, HEAD_SIZE), (0, 2, 1, 3)
    ).reshape(n_exp, heads_own * length, HEAD_SIZE)
    deltas = jnp.sum(grad_heads.astype(F32) * attn_heads.astype(F32), axis=-1, keepdims=True)
    probs = jnp.where(causal, jnp.exp(batched(query_rows, keys_all, 2, 2) * factor), 0.0) / totals
    grad_scores = (
        probs * (batched(grad_heads, values_all, 2, 2) - deltas) * factor
    ).astype(BF)
    value_part = batched(probs.astype(BF), grad_heads, 1, 1)
    key_part = batched(grad_scores, query_rows, 1, 1)

    def by_position(part):
        part = part.reshape(n_exp, n_ctx, length, HEAD_SIZE)
        return jnp.transpose(part, (1, 0, 2, 3))

    key_part, value_part = by_position(key_part), by_position(value_part)
    partner = jnp.where(holds_keys, value_part, key_part).astype(BF)
    partner = lax.ppermute(partner, "exp", pairs)
    own_part = jnp.where(holds_keys, key_part, value_part) + partner.astype(F32)
    own_part = own_part.astype(BF).reshape(n_ctx, tokens, HEAD_SIZE)
    own_sums = lax.psum_scatter(
        own_part.reshape(n_ctx * tokens, HEAD_SIZE),
        "ctx", scatter_dimension=0, tiled=True,
    ).astype(F32).reshape(n_exp, length, HEAD_SIZE)
    grad_query_rot = batched(grad_scores, keys_all, 2, 1)
    grad_query_unit = rotation_backward(
        jnp.transpose(
            grad_query_rot.reshape(n_exp, heads_own, length, HEAD_SIZE), (0, 2, 1, 3)
        ), cos_q, sin_q,
    )
    q_gain_part = jnp.sum(grad_query_unit * queries * query_scale, axis=(0, 1, 2))
    grad_query_rows = norm_backward(grad_query_unit, queries, query_scale, q_gain).astype(BF)
    grad_query_rows = grad_query_rows.reshape(tokens, own_width)
    grad_key_unit = rotation_backward(own_sums, cos_k, sin_k)
    k_gain_part = jnp.sum(grad_key_unit * own_raw * key_scale, axis=(0, 1))
    k_gain_part = jnp.where(holds_keys, k_gain_part, 0.0)
    grad_own = jnp.where(
        holds_keys, norm_backward(grad_key_unit, own_raw, key_scale, k_gain), own_sums
    ).astype(BF)
    grad_heads_in = jnp.concatenate(
        [grad_query_rows, grad_own.reshape(tokens, HEAD_SIZE)], axis=1
    )
    normed_part = dot(grad_heads_in, weight_cols, ((1,), (1,))).astype(BF)
    grad_normed = lax.psum_scatter(normed_part, "exp", scatter_dimension=0, tiled=True)
    grad_normed = grad_normed.astype(F32)
    first_scale = rms_scale(wide_in)
    grad_in = grad_mid + norm_backward(grad_normed, wide_in, first_scale, first_gain)

    grad_cols = dot(normed, grad_heads_in, ((0,), (0,))).astype(BF)
    gain_parts = jnp.concatenate(
        [
            mlp_gain_part.reshape(n_exp, cut),
            q_gain_part.reshape(n_exp, small),
            k_gain_part.reshape(n_exp, small),
        ],
        axis=1,
    )
    gain_parts = jnp.pad(gain_parts, ((0, 0), (0, packed_width - cut - 2 * small)))[:, None, :]
    gain_parts = jnp.pad(gain_parts, ((0, 0), (0, 15), (0, 0))).astype(BF)
    grad_cols = jnp.concatenate(
        [grad_cols.reshape(n_exp, rows_own, packed_width), gain_parts], axis=1
    )
    grad_cols = column_sum(grad_cols.reshape(n_exp * (rows_own + 16), packed_width), n_ctx, n_exp)
    own_gains = jnp.sum(grad_cols[:, rows_own].astype(F32), axis=0)
    grad_cols = grad_cols[:, :rows_own]
    to_row = jnp.transpose(grad_cols, (1, 0, 2))
    halves = jnp.sum(
        to_row[:, :, own_width:]
        .reshape(rows_own, KEY_VALUE_HEADS, sharers // 2, 2, HEAD_SIZE)
        .astype(F32),
        axis=2,
    )
    kv_width = KEY_VALUE_HEADS * HEAD_SIZE
    grad_wq = to_row[:, :, :own_width].reshape(rows_own, query_width).astype(F32)
    grad_wk = halves[:, :, 0].reshape(rows_own, kv_width)
    grad_wv = halves[:, :, 1].reshape(rows_own, kv_width)

    attn_gain_sum = (
        jnp.sum(w_query.astype(F32) * grad_wq, axis=1)
        + jnp.sum(key_projection.astype(F32) * grad_wk, axis=1)
        + jnp.sum(value_projection.astype(F32) * grad_wv, axis=1)
    ) / attn_gain.astype(F32)

    return (
        hidden_out[None],
        grad_in[None],
        attn_gain_sum,
        grad_wq,
        grad_wk,
        grad_wv,
        own_gains[cut : cut + small],
        own_gains[cut + small : cut + 2 * small],
        wout_sum,
        own_gains[:cut],
        grad_gate_mat[None],
        grad_up_mat[None],
        grad_down[None],
    )


def solution(mesh):
    rows = P("exp", "ctx", None)
    shard, matrix, expert = P("exp"), P("exp", None), P(("ctx", "exp"), None, None)
    in_specs = (
        rows, rows, rows, shard, matrix, matrix, matrix, shard, shard, matrix, shard,
        expert, expert, expert, rows,
    )
    out_specs = (
        rows, rows, shard, matrix, matrix, matrix, shard, shard, matrix, shard,
        expert, expert, expert,
    )
    return jax.shard_map(
        per_device, mesh=mesh, in_specs=in_specs, out_specs=out_specs, check_vma=False
    )
```

```python
import functools

import jax
import jax.numpy as jnp
from jax import lax
from jax.experimental import pallas as pl
from jax.experimental.pallas import tpu as pltpu
from jax.sharding import PartitionSpec as P


KEY_VALUE_HEADS = 4
HEAD_SIZE = 128
TOPK = 8

EPSILON = 1e-06
THETA = 1000000.0

BF = jnp.bfloat16
F32 = jnp.float32


def rms_scale(tensor):
    return lax.rsqrt(jnp.mean(tensor * tensor, axis=-1, keepdims=True) + EPSILON)


def norm_backward(cotangent, tensor, factor, weight):
    scaled = cotangent * weight
    unit_form = tensor * factor
    return factor * (scaled - unit_form * jnp.mean(scaled * unit_form, axis=-1, keepdims=True))


def rope_tables(positions):
    halfway = HEAD_SIZE // 2
    frequency = THETA ** (-(jnp.arange(halfway, dtype=F32) * (2.0 / HEAD_SIZE)))
    angles = positions.astype(F32)[:, None] * frequency[None, :]
    cosine = jnp.concatenate([jnp.cos(angles), jnp.cos(angles)], axis=-1)
    sine = jnp.concatenate([jnp.sin(angles), jnp.sin(angles)], axis=-1)
    return cosine, sine


def rotate(tensor, cosine, sine):
    halfway = tensor.shape[-1] // 2
    turned = jnp.concatenate([-tensor[..., halfway:], tensor[..., :halfway]], axis=-1)
    return tensor * cosine + turned * sine


def rotation_backward(cotangent, cosine, sine):
    halfway = cotangent.shape[-1] // 2
    sine_part = cotangent * sine
    turned = jnp.concatenate([sine_part[..., halfway:], -sine_part[..., :halfway]], axis=-1)
    return cotangent * cosine + turned


def dot(a, b, dims):
    return lax.dot_general(a, b, (dims, ((), ())), preferred_element_type=F32)


def after(value, *earlier):
    return lax.optimization_barrier((value,) + earlier)[0]


def round_up(number, multiple):
    return -(-number // multiple) * multiple


MESH = pl.DeviceIdType.MESH


def line_sum_steps(n_ctx, chunks, part, finish, line, lag=2):
    (from_left, from_right, to_right, to_left, right_send, right_recv, left_send, left_recv) = line
    ctx, last = lax.axis_index("ctx"), n_ctx - 1

    def copy_right(k):
        return pltpu.make_async_remote_copy(
            src_ref=to_right.at[k], dst_ref=from_left.at[k],
            send_sem=right_send.at[k], recv_sem=right_recv.at[k],
            device_id={"ctx": ctx + 1}, device_id_type=MESH,
        )

    def copy_left(k):
        return pltpu.make_async_remote_copy(
            src_ref=to_left.at[k], dst_ref=from_right.at[k],
            send_sem=left_send.at[k], recv_sem=left_recv.at[k],
            device_id={"ctx": ctx - 1}, device_id_type=MESH,
        )

    def step(time, carry):
        k_right = time - lag * ctx
        k_left = time - lag * (last - ctx)
        k_done = time - lag * jnp.maximum(ctx, last - ctx)

        @pl.when((k_right >= 0) & (k_right < chunks))
        def _():
            @pl.when(ctx == 0)
            def _():
                to_right[k_right] = part(k_right).astype(BF)

            @pl.when(ctx > 0)
            def _():
                copy_right(k_right).wait_recv()
                to_right[k_right] = (part(k_right) + from_left[k_right].astype(F32)).astype(BF)

            @pl.when(ctx < last)
            def _():
                copy_right(k_right).start()

        @pl.when((k_left >= 0) & (k_left < chunks))
        def _():
            @pl.when(ctx == last)
            def _():
                to_left[k_left] = part(k_left).astype(BF)

            @pl.when(ctx < last)
            def _():
                copy_left(k_left).wait_recv()
                to_left[k_left] = (part(k_left) + from_right[k_left].astype(F32)).astype(BF)

            @pl.when(ctx > 0)
            def _():
                copy_left(k_left).start()

        @pl.when((k_done >= 0) & (k_done < chunks))
        def _():
            @pl.when(ctx == last)
            def _():
                finish(k_done, to_right[k_done].astype(F32))

            @pl.when(ctx < last)
            def _():
                finish(k_done, to_right[k_done].astype(F32) + from_right[k_done].astype(F32))

        return carry

    lax.fori_loop(0, chunks + lag * last, step, 0)

    def drain(k, carry):
        @pl.when(ctx < last)
        def _():
            copy_right(k).wait_send()

        @pl.when(ctx > 0)
        def _():
            copy_left(k).wait_send()

        return carry

    lax.fori_loop(0, chunks, drain, 0)


def greet(n_line, others):
    barrier = pltpu.get_barrier_semaphore()
    for other in others:
        pl.semaphore_signal(barrier, inc=1, device_id=other, device_id_type=MESH)
    if n_line == 1:
        pl.semaphore_wait(barrier, len(others))
        return
    ctx, last = lax.axis_index("ctx"), n_line - 1

    @pl.when(ctx > 0)
    def _():
        pl.semaphore_signal(barrier, inc=1, device_id={"ctx": ctx - 1}, device_id_type=MESH)

    @pl.when(ctx < last)
    def _():
        pl.semaphore_signal(barrier, inc=1, device_id={"ctx": ctx + 1}, device_id_type=MESH)

    at_end = (ctx == 0) | (ctx == last)

    @pl.when(at_end)
    def _():
        pl.semaphore_wait(barrier, len(others) + 1)

    @pl.when(jnp.logical_not(at_end))
    def _():
        pl.semaphore_wait(barrier, len(others) + 2)


def line_buffers(chunks, rows, width):
    slots = pltpu.VMEM((chunks, rows, width), BF)
    sems = pltpu.SemaphoreType.DMA((chunks,))
    return [slots] * 4 + [sems] * 4


def line_sum_kernel(n_ctx, chunks, x_ref, out_ref, *line):
    greet(n_ctx, [])

    def finish(k, value):
        out_ref[k] = value

    line_sum_steps(n_ctx, chunks, lambda k: x_ref[k].astype(F32), finish, line)


def line_sum(x, n_ctx, chunks=16):
    total, width = x.shape
    rows = total // chunks
    out = pl.pallas_call(
        functools.partial(line_sum_kernel, n_ctx, chunks),
        out_shape=jax.ShapeDtypeStruct((chunks, rows, width), F32),
        in_specs=[pl.BlockSpec(memory_space=pltpu.VMEM)],
        out_specs=pl.BlockSpec(memory_space=pltpu.VMEM),
        scratch_shapes=line_buffers(chunks, rows, width),
        compiler_params=pltpu.CompilerParams(
            collective_id=2, has_side_effects=True, vmem_limit_bytes=40 * 1024 * 1024
        ),
    )(x.reshape(chunks, rows, width))
    return out.reshape(total, width)


def column_sum_kernel(n_ctx, n_exp, subs, x_ref, out_ref, whole, plane_send, plane_recv, own_sem, *line):
    exp = lax.axis_index("exp")
    chunks = n_exp * subs
    greet(n_ctx, [{"exp": lax.rem(exp + hop, n_exp)} for hop in range(1, n_exp)])

    def copy_plane(k):
        hop, sub = k // subs, lax.rem(k, subs)
        return pltpu.make_async_remote_copy(
            src_ref=whole.at[k], dst_ref=out_ref.at[exp, sub],
            send_sem=plane_send.at[k], recv_sem=plane_recv.at[k],
            device_id={"exp": lax.rem(exp + hop, n_exp)}, device_id_type=MESH,
        )

    def copy_own(k):
        return pltpu.make_async_copy(whole.at[k], out_ref.at[exp, k], own_sem.at[k])

    def part(k):
        owner = lax.rem(exp + k // subs, n_exp)
        return x_ref[owner * subs + lax.rem(k, subs)].astype(F32)

    def finish(k, value):
        whole[k] = value.astype(BF)

        @pl.when(k < subs)
        def _():
            copy_own(k).start()

        @pl.when(k >= subs)
        def _():
            copy_plane(k).start()

    line_sum_steps(n_ctx, chunks, part, finish, line)

    def drain(k, carry):
        @pl.when(k < subs)
        def _():
            copy_own(k).wait()

        @pl.when(k >= subs)
        def _():
            copy_plane(k).wait()

        return carry

    lax.fori_loop(0, chunks, drain, 0)


def column_sum(x, n_ctx, n_exp, subs=4):
    total, width = x.shape
    rows = total // n_exp // subs
    chunks = n_exp * subs
    sems = pltpu.SemaphoreType.DMA((chunks,))
    out = pl.pallas_call(
        functools.partial(column_sum_kernel, n_ctx, n_exp, subs),
        out_shape=jax.ShapeDtypeStruct((n_exp, subs, rows, width), BF),
        in_specs=[pl.BlockSpec(memory_space=pltpu.VMEM)],
        out_specs=pl.BlockSpec(memory_space=pltpu.VMEM),
        scratch_shapes=[
            pltpu.VMEM((chunks, rows, width), BF), sems, sems, pltpu.SemaphoreType.DMA((subs,)),
        ] + line_buffers(chunks, rows, width),
        compiler_params=pltpu.CompilerParams(
            collective_id=1, has_side_effects=True, vmem_limit_bytes=48 * 1024 * 1024
        ),
    )(x.reshape(chunks, rows, width))
    return out.reshape(n_exp, subs * rows, width)


def gather_kernel(n_line, x_ref, out_ref, *sems):
    (z_send, x_send, y_send, d_send, p_send, z_recv, x_recv, y_recv, d_recv, p_recv, own_sem) = sems
    exp = lax.axis_index("exp")
    ctx = lax.axis_index("ctx") if n_line > 1 else 0
    last = n_line - 1

    def flip(bit):
        return exp + bit - 2 * bit * lax.rem(exp // bit, 2)

    over_core, over_x, over_y = flip(1), flip(2), flip(4)
    over_both = over_x + over_y - exp
    greet(n_line, [{"exp": other} for other in (over_core, over_x, over_y)])

    def send(src, place, half, send_sem, recv_sem, device):
        return pltpu.make_async_remote_copy(
            src_ref=src, dst_ref=out_ref.at[place[0], place[1], half],
            send_sem=send_sem, recv_sem=recv_sem, device_id=device, device_id_type=MESH,
        )

    def held(block, line, half):
        return out_ref.at[block, line, half]

    def to_z(src, line, half, way):
        step = 2 * way - 1
        return send(
            src, (exp, line), half, z_send.at[way, line, half], z_recv.at[line, half],
            {"ctx": ctx + step},
        )

    def to_x(src, line, half):
        return send(src, (exp, line), half, x_send.at[line, half], x_recv.at[line, half], {"exp": over_x})

    def to_y(src, line, half):
        return send(src, (exp, line), half, y_send.at[line, half], y_recv.at[line, half], {"exp": over_y})

    def across(line, half):
        block, device = ((over_x, over_y), (over_y, over_x))[half]
        return send(
            held(block, line, half), (block, line), half, d_send.at[line, half],
            d_recv.at[line, half], {"exp": device},
        )

    blocks = (exp, over_x, over_y, over_both)

    def to_core(src, which, line, half):
        return send(
            src, (blocks[which], line), half, p_send.at[which, line, half],
            p_recv.at[which, line, half], {"exp": over_core},
        )

    def when(cond, body):
        if cond is True:
            body()
        else:
            pl.when(cond)(body)

    def own(half):
        return pltpu.make_async_copy(x_ref.at[half], held(exp, ctx, half), own_sem.at[half])

    def place(distance, way):
        line = ctx - (2 * way - 1) * distance
        return line, (True if distance == 0 else (line >= 0) & (line <= last))

    def along(distance, way):
        line, there = place(distance, way)

        def body():
            for half in (0, 1):
                src = x_ref.at[half] if distance == 0 else held(exp, line, half)
                if distance:
                    to_z(src, line, half, way).wait_recv()
                if n_line > 1:
                    for onward in (0, 1) if distance == 0 else (way,):
                        @pl.when((ctx > 0) if onward == 0 else (ctx < last))
                        def _():
                            to_z(src, line, half, onward).start()
            for half in (0, 1):
                src = [x_ref.at[h] if distance == 0 else held(exp, line, h) for h in (0, 1)]
                to_x(src[half], line, half).start()
                to_y(src[1 - half], line, 1 - half).start()
            for half in (0, 1):
                to_core(src[half], 0, line, half).start()

        when(there, body)

    def plane(distance, way):
        line, there = place(distance, way)

        def body():
            to_x(held(over_x, line, 0), line, 0).wait_recv()
            across(line, 0).start()
            to_y(held(over_y, line, 1), line, 1).wait_recv()
            across(line, 1).start()
            to_core(held(over_x, line, 0), 1, line, 0).start()
            to_core(held(over_y, line, 1), 2, line, 1).start()
            to_x(held(over_x, line, 1), line, 1).wait_recv()
            to_core(held(over_x, line, 1), 1, line, 1).start()
            to_y(held(over_y, line, 0), line, 0).wait_recv()
            to_core(held(over_y, line, 0), 2, line, 0).start()

        when(there, body)

    def corner(distance, way):
        line, there = place(distance, way)

        def body():
            for half in (0, 1):
                across(line, half).wait_recv()
                to_core(held(over_both, line, half), 3, line, half).start()

        when(there, body)

    def finish(distance, way):
        line, there = place(distance, way)

        def body():
            for half in (0, 1):
                src = x_ref.at[half] if distance == 0 else held(exp, line, half)
                for which in range(4):
                    from_core = to_core(src, which, line, half)
                    from_core.wait_recv()
                    from_core.wait_send()
                to_x(src, line, half).wait_send()
                to_y(src, line, half).wait_send()
                across(line, half).wait_send()
                if n_line > 1:
                    for onward in (0, 1) if distance == 0 else (way,):
                        @pl.when((ctx > 0) if onward == 0 else (ctx < last))
                        def _():
                            to_z(src, line, half, onward).wait_send()

        when(there, body)

    def everywhere(stage, distance):
        if 0 <= distance < n_line:
            for way in (1,) if distance == 0 else (1, 0):
                stage(distance, way)

    for half in (0, 1):
        own(half).start()
    for time in range(n_line + 2):
        everywhere(along, time)
        everywhere(plane, time - 1)
        everywhere(corner, time - 2)
    for distance in range(n_line):
        everywhere(finish, distance)
    for half in (0, 1):
        own(half).wait()


def gather_rows(x, n_line, n_exp, collective_id):
    rows, width = x.shape
    if n_exp != 8:
        if n_line > 1:
            x = lax.all_gather(x, "ctx", axis=0, tiled=True)
        return lax.all_gather(x, "exp", axis=0, tiled=False)
    dma = pltpu.SemaphoreType.DMA
    pair, four = dma((n_line, 2)), dma((4, n_line, 2))
    out = pl.pallas_call(
        functools.partial(gather_kernel, n_line),
        out_shape=jax.ShapeDtypeStruct((n_exp, n_line, 2, rows // 2, width), x.dtype),
        in_specs=[pl.BlockSpec(memory_space=pltpu.VMEM)],
        out_specs=pl.BlockSpec(memory_space=pl.ANY),
        scratch_shapes=[
            dma((2, n_line, 2)), pair, pair, pair, four, pair, pair, pair, pair, four, dma((2,)),
        ],
        compiler_params=pltpu.CompilerParams(
            collective_id=collective_id, has_side_effects=True
        ),
    )(x.reshape(2, rows // 2, width))
    return out.reshape(n_exp, n_line * rows, width)


def reduce_kernel(x_ref, out_ref, from_core, sums, arrived, c_send, c_recv, q_send, q_recv):
    exp = lax.axis_index("exp")

    def flip(device, bit):
        return device + bit - 2 * bit * lax.rem(device // bit, 2)

    over_core, over_x, over_y = flip(exp, 1), flip(exp, 2), flip(exp, 4)
    owners = (flip(over_x, 4), over_x, over_y, exp)
    greet(1, [{"exp": other} for other in (over_core,) + owners[:3]])
    rows = 16

    def to_core(t):
        return pltpu.make_async_remote_copy(
            src_ref=x_ref.at[flip(owners[t], 1)], dst_ref=from_core.at[t],
            send_sem=c_send.at[t], recv_sem=c_recv.at[t],
            device_id={"exp": over_core}, device_id_type=MESH,
        )

    def to_owner(t):
        return pltpu.make_async_remote_copy(
            src_ref=sums.at[t], dst_ref=arrived.at[t],
            send_sem=q_send.at[t], recv_sem=q_recv.at[t],
            device_id={"exp": owners[t]}, device_id_type=MESH,
        )

    def by_rows(body):
        def step(i, carry):
            body(pl.ds(pl.multiple_of(i * rows, rows), rows))
            return carry

        lax.fori_loop(0, out_ref.shape[0] // rows, step, 0)

    for t in range(4):
        to_core(t).start()
    for t in range(4):
        to_core(t).wait_recv()

        def add(at, t=t):
            value = x_ref[owners[t], at, :].astype(F32) + from_core[t, at, :].astype(F32)
            if t < 3:
                sums[t, at, :] = value.astype(BF)
            else:
                out_ref[at, :] = value

        by_rows(add)
        if t < 3:
            to_owner(t).start()
    for t in (1, 2, 0):
        to_owner(t).wait_recv()

        def gather(at, t=t):
            out_ref[at, :] = out_ref[at, :] + arrived[t, at, :].astype(F32)

        by_rows(gather)
    for t in range(4):
        to_core(t).wait_send()
        if t < 3:
            to_owner(t).wait_send()


def reduce_rows(x, n_exp, collective_id):
    rows, width = x.shape[0] // n_exp, x.shape[1]
    if n_exp != 8:
        return lax.psum_scatter(x, "exp", scatter_dimension=0, tiled=True).astype(F32)
    dma = pltpu.SemaphoreType.DMA
    return pl.pallas_call(
        reduce_kernel,
        out_shape=jax.ShapeDtypeStruct((rows, width), F32),
        in_specs=[pl.BlockSpec(memory_space=pltpu.VMEM)],
        out_specs=pl.BlockSpec(memory_space=pltpu.VMEM),
        scratch_shapes=[
            pltpu.VMEM((4, rows, width), BF), pltpu.VMEM((3, rows, width), BF),
            pltpu.VMEM((3, rows, width), BF), dma((4,)), dma((4,)), dma((3,)), dma((3,)),
        ],
        compiler_params=pltpu.CompilerParams(
            collective_id=collective_id, has_side_effects=True, vmem_limit_bytes=32 * 1024 * 1024
        ),
    )(x.reshape(n_exp, rows, width))


def spread_kernel(
    n_exp, sharers, query_ref, halves_ref, gains_ref, out_ref, gains_out_ref,
    q_send, q_recv, h_send, h_recv, g_send, g_recv, own_sems,
):
    exp = lax.axis_index("exp")
    own_width = query_ref.shape[1] // n_exp
    greet(1, [{"exp": lax.rem(exp + hop, n_exp)} for hop in range(1, n_exp)])

    def pieces(owner):
        columns = pl.ds(pl.multiple_of(owner * own_width, own_width), own_width)
        return (
            (query_ref.at[:, columns], out_ref.at[exp, :, pl.ds(0, own_width)]),
            (
                halves_ref.at[owner // sharers, lax.rem(owner, 2)],
                out_ref.at[exp, :, pl.ds(own_width, HEAD_SIZE)],
            ),
            (gains_ref, gains_out_ref.at[exp]),
        )

    copies = []
    for hop in range(1, n_exp):
        owner = lax.rem(exp + hop, n_exp)
        for (src, dst), send, recv in zip(
            pieces(owner), (q_send, h_send, g_send), (q_recv, h_recv, g_recv)
        ):
            copies.append(
                pltpu.make_async_remote_copy(
                    src_ref=src, dst_ref=dst, send_sem=send.at[hop], recv_sem=recv.at[hop],
                    device_id={"exp": owner}, device_id_type=MESH,
                )
            )
    for i, (src, dst) in enumerate(pieces(exp)):
        copies.append(pltpu.make_async_copy(src, dst, own_sems.at[i]))
    for copy in copies:
        copy.start()
    for copy in copies:
        copy.wait()


def spread_columns(query, halves, gains, n_exp, sharers):
    rows, width = query.shape
    dma = pltpu.SemaphoreType.DMA((n_exp,))
    vmem = pl.BlockSpec(memory_space=pltpu.VMEM)
    return pl.pallas_call(
        functools.partial(spread_kernel, n_exp, sharers),
        out_shape=(
            jax.ShapeDtypeStruct((n_exp, rows, width // n_exp + HEAD_SIZE), BF),
            jax.ShapeDtypeStruct((n_exp,) + gains.shape, BF),
        ),
        in_specs=[vmem] * 3,
        out_specs=(vmem, vmem),
        scratch_shapes=[dma] * 6 + [pltpu.SemaphoreType.DMA((3,))],
        compiler_params=pltpu.CompilerParams(
            collective_id=6, has_side_effects=True, vmem_limit_bytes=24 * 1024 * 1024
        ),
    )(query, halves, gains)


def per_device(
    hidden_in,
    expert_ids,
    gate_weights,
    attn_gain,
    w_query,
    key_projection,
    value_projection,
    query_gain,
    key_norm_gain,
    w_output,
    mlp_gain,
    w_gate,
    w_up,
    w_down,
    grad_out,
):
    length, width = hidden_in.shape[1:]
    n_ctx, n_exp = lax.axis_size("ctx"), lax.axis_size("exp")
    n_all = n_ctx * n_exp
    ctx_index = lax.axis_index("ctx")
    rows_own, query_width = w_query.shape
    heads_own = query_width // HEAD_SIZE // n_exp
    own_width = heads_own * HEAD_SIZE
    sharers = n_exp // KEY_VALUE_HEADS
    tokens = n_exp * length
    holds_keys = lax.rem(lax.axis_index("exp"), 2) == 0
    pairs = [(i, i ^ 1) for i in range(n_exp)]
    factor = HEAD_SIZE ** (-0.5)
    w_gate, w_up, w_down = w_gate[0], w_up[0], w_down[0]

    def heads_of(kv):
        return kv.reshape(rows_own, KEY_VALUE_HEADS, 1, HEAD_SIZE)

    halves = jnp.concatenate([heads_of(key_projection), heads_of(value_projection)], axis=2)
    halves = jnp.transpose(halves, (1, 2, 0, 3))
    packed_width = own_width + HEAD_SIZE
    gains = jnp.concatenate([attn_gain, mlp_gain, query_gain, key_norm_gain])
    gain_rows = round_up(gains.shape[0], 16 * HEAD_SIZE) // HEAD_SIZE
    gains = jnp.pad(gains, (0, gain_rows * HEAD_SIZE - gains.shape[0]))
    hidden_all = gather_rows(hidden_in[0], 1, n_exp, 7)
    hidden_all = hidden_all.reshape(tokens, width)
    weight_cols, gains = spread_columns(
        after(w_query, hidden_all), halves, gains.reshape(gain_rows, HEAD_SIZE),
        n_exp, sharers,
    )
    weight_cols = weight_cols.reshape(n_exp * rows_own, packed_width)
    gains = gains.reshape(n_exp, gain_rows * HEAD_SIZE).astype(F32)
    cut = attn_gain.shape[0]
    small = query_gain.shape[0]
    first_gain = gains[:, :cut].reshape(-1)
    second_gain = gains[:, cut : 2 * cut].reshape(-1)
    q_gain = gains[:, 2 * cut : 2 * cut + small].reshape(-1)
    k_gain = gains[:, 2 * cut + small : 2 * cut + 2 * small].reshape(-1)

    hits = expert_ids[0][:, :, None] == jnp.arange(n_all, dtype=jnp.int32)[None, None, :]
    dense_gates = jnp.sum(jnp.where(hits, gate_weights[0][:, :, None], 0.0), axis=1)
    high = lax.reduce_precision(dense_gates, 8, 7)
    middle = lax.reduce_precision(dense_gates - high, 8, 7)
    gate_parts = jnp.concatenate([high, middle, dense_gates - high - middle], axis=1).astype(BF)
    gate_parts = jnp.pad(gate_parts, ((0, 0), (0, round_up(3 * n_all, HEAD_SIZE) - 3 * n_all)))
    grad_column = lax.all_gather(
        jnp.concatenate([grad_out[0], gate_parts], axis=1), "ctx",
        axis=0, tiled=True,
    )
    gate_parts = grad_column[:, width : width + 3 * n_all].reshape(n_ctx * length, 3, n_all)
    gate_parts = lax.dynamic_slice(
        gate_parts, (0, 0, ctx_index * n_exp), (n_ctx * length, 3, n_exp)
    )
    gate_parts = jnp.transpose(gate_parts, (2, 1, 0))
    span = n_ctx * length
    slots = round_up(n_ctx * max(2, length * TOPK * 4 // (3 * n_all)), 8)
    below = (
        jnp.arange(span, dtype=jnp.int32)[:, None] < jnp.arange(span, dtype=jnp.int32)[None, :]
    ).astype(BF)

    def in_slots(chosen):
        rank = dot(chosen.astype(BF), below, ((1,), (0,))).astype(jnp.int32)
        return chosen[:, None, :] & (
            rank[:, None, :] == jnp.arange(slots, dtype=jnp.int32)[None, :, None]
        )

    pick = in_slots(gate_parts[:, 0] > 0.0).astype(BF).reshape(n_exp * slots, span)

    def exchange(rows):
        rows = rows.astype(BF).reshape(n_exp, slots, width)
        rows = lax.all_to_all(rows, "exp", split_axis=0, concat_axis=0, tiled=True)
        return rows.reshape(n_exp * slots, width)

    packed_rows = dot(pick, grad_column[:, :width], ((1,), (0,))).astype(BF)
    gate_parts = jnp.pad(gate_parts, ((0, 0), (0, 5), (0, width - span)))
    sent = jnp.concatenate(
        [packed_rows.reshape(n_exp, slots, width), gate_parts], axis=1,
    )
    received = lax.all_to_all(sent, "exp", split_axis=0, concat_axis=0, tiled=True)
    own_gates = jnp.sum(received[:, slots : slots + 3, :span].astype(F32), axis=1)
    taken = in_slots(own_gates > 0.0)
    take = taken.astype(BF)
    slot_gates = jnp.sum(jnp.where(taken, own_gates[:, None, :], 0.0), axis=2)
    slot_grads = slot_gates[:, :, None] * received[:, :slots].astype(F32)
    slot_grads = slot_grads.astype(BF).reshape(n_exp * slots, width)
    slot_gates = slot_gates.reshape(n_exp * slots, 1)

    positions = ctx_index * length + jnp.arange(length, dtype=jnp.int32)
    cosine, sine = rope_tables(positions)
    cos_q, sin_q = cosine[None, :, None, :], sine[None, :, None, :]
    cos_k, sin_k = cosine[None], sine[None]
    wide_all = hidden_all.astype(F32)
    normed = (wide_all * rms_scale(wide_all) * first_gain).astype(BF)
    projected = dot(normed, weight_cols, ((1,), (0,)))
    queries = after(projected[:, :own_width], sent).reshape(n_exp, length, heads_own, HEAD_SIZE)
    own_raw = projected[:, own_width:].reshape(n_exp, length, HEAD_SIZE)
    query_scale, key_scale = rms_scale(queries), rms_scale(own_raw)
    query_rot = rotate(queries * query_scale * q_gain, cos_q, sin_q).astype(BF)
    key_rot = rotate(own_raw * key_scale * k_gain, cos_k, sin_k).astype(BF)
    own_half = jnp.where(holds_keys, key_rot, own_raw.astype(BF)).reshape(tokens, HEAD_SIZE)
    own_half = lax.all_gather(own_half, "ctx", axis=0, tiled=True)
    other_half = lax.ppermute(own_half, "exp", pairs)

    def by_sequence(half):
        half = half.reshape(n_ctx, n_exp, length, HEAD_SIZE)
        return jnp.transpose(half, (1, 0, 2, 3)).reshape(n_exp, n_ctx * length, HEAD_SIZE)

    keys_all = by_sequence(jnp.where(holds_keys, own_half, other_half))
    values_all = by_sequence(jnp.where(holds_keys, other_half, own_half))

    query_rows = jnp.transpose(query_rot, (0, 2, 1, 3)).reshape(n_exp, heads_own * length, HEAD_SIZE)
    key_pos = jnp.arange(n_ctx * length, dtype=jnp.int32)
    causal = key_pos[None, :] <= jnp.tile(positions, heads_own)[:, None]

    def batched(a, b, a_dim, b_dim):
        return lax.dot_general(
            a, b, (((a_dim,), (b_dim,)), ((0,), (0,))), preferred_element_type=F32
        )

    expos = jnp.where(causal, jnp.exp(batched(query_rows, keys_all, 2, 2) * factor), 0.0)
    totals = jnp.sum(expos, axis=-1, keepdims=True)
    attn_heads = (batched(expos.astype(BF), values_all, 2, 1) / totals).astype(BF)
    attn_rows = jnp.transpose(
        attn_heads.reshape(n_exp, heads_own, length, HEAD_SIZE), (0, 2, 1, 3)
    ).reshape(tokens, own_width)
    branch_part = dot(attn_rows, w_output, ((1,), (0,))).astype(BF)
    branch = reduce_rows(branch_part, n_exp, 5)
    wide_in = hidden_in[0].astype(F32)
    mid = wide_in + branch
    second_scale = rms_scale(mid)
    mlp_in = (mid * second_scale * second_gain).astype(BF)

    mlp_all = gather_rows(after(mlp_in, take), n_ctx, n_exp, 3)
    arrived = lax.dot_general(
        take, mlp_all, (((2,), (1,)), ((0,), (0,))), preferred_element_type=F32
    ).astype(BF).reshape(n_exp * slots, width)
    gate_pre = dot(arrived, w_gate, ((1,), (0,)))
    up_pre = dot(arrived, w_up, ((1,), (0,)))
    sigmoid_gate = jax.nn.sigmoid(gate_pre)
    silu_gate = gate_pre * sigmoid_gate
    inner = (silu_gate * up_pre).astype(BF)
    grad_inner = dot(slot_grads, w_down, ((1,), (1,)))
    grad_gate_pre = (
        grad_inner * up_pre * sigmoid_gate * (1.0 + gate_pre * (1.0 - sigmoid_gate))
    ).astype(BF)
    grad_up_pre = (grad_inner * silu_gate).astype(BF)
    split = width // 2

    def give_back(at):
        rows = dot(grad_gate_pre, w_gate[at], ((1,), (1,))) + dot(grad_up_pre, w_up[at], ((1,), (1,)))
        return rows.astype(BF).reshape(n_exp, slots, split)

    def back_sum(rows):
        part = dot(pick, rows.reshape(n_exp * slots, split), ((0,), (0,))).astype(BF)
        return lax.psum_scatter(part, "ctx", scatter_dimension=0, tiled=True)

    first = lax.all_to_all(give_back(slice(0, split)), "exp", split_axis=0, concat_axis=0, tiled=True)
    second = after(give_back(slice(split, width)), first)
    second = lax.all_to_all(second, "exp", split_axis=0, concat_axis=0, tiled=True)
    grad_mlp = jnp.concatenate([back_sum(first), back_sum(second)], axis=1).astype(F32)

    gradient_wide = grad_out[0].astype(F32)
    mlp_gain_part = jnp.sum(grad_mlp * mid * second_scale, axis=0)
    grad_mid = gradient_wide + norm_backward(grad_mlp, mid, second_scale, second_gain)
    branch_all = gather_rows(grad_mid.astype(BF), 1, n_exp, 4)
    branch_all = branch_all.reshape(tokens, width)

    expert_out = slot_gates * dot(inner, w_down, ((1,), (0,)))
    out_back = exchange(after(expert_out.astype(BF), branch_all))
    mixed_part = dot(pick, out_back, ((0,), (0,))).astype(BF)
    mixed = lax.psum_scatter(mixed_part, "ctx", scatter_dimension=0, tiled=True)
    hidden_out = (mid + mixed.astype(F32)).astype(BF)
    grad_down = dot(inner, slot_grads, ((0,), (0,)))
    grad_gate_mat = dot(arrived, grad_gate_pre, ((0,), (0,)))
    grad_up_mat = dot(arrived, grad_up_pre, ((0,), (0,)))

    grad_wout = dot(attn_rows, branch_all, ((0,), (0,))).astype(BF)
    wout_sum = line_sum(grad_wout, n_ctx)
    attn_grad = dot(after(branch_all, wout_sum), w_output, ((1,), (1,))).astype(BF)
    grad_heads = jnp.transpose(
        after(attn_grad, mixed_part).reshape(n_exp, length, heads_own, HEAD_SIZE), (0, 2, 1, 3)
    ).reshape(n_exp, heads_own * length, HEAD_SIZE)
    deltas = jnp.sum(grad_heads.astype(F32) * attn_heads.astype(F32), axis=-1, keepdims=True)
    probs = jnp.where(causal, jnp.exp(batched(query_rows, keys_all, 2, 2) * factor), 0.0) / totals
    grad_scores = (
        probs * (batched(grad_heads, values_all, 2, 2) - deltas) * factor
    ).astype(BF)
    value_part = batched(probs.astype(BF), grad_heads, 1, 1)
    key_part = batched(grad_scores, query_rows, 1, 1)

    def by_position(part):
        part = part.reshape(n_exp, n_ctx, length, HEAD_SIZE)
        return jnp.transpose(part, (1, 0, 2, 3))

    key_part, value_part = by_position(key_part), by_position(value_part)
    partner = jnp.where(holds_keys, value_part, key_part).astype(BF)
    partner = lax.ppermute(partner, "exp", pairs)
    own_part = jnp.where(holds_keys, key_part, value_part) + partner.astype(F32)
    own_part = own_part.astype(BF).reshape(n_ctx, tokens, HEAD_SIZE)
    own_part = lax.all_to_all(own_part, "ctx", split_axis=0, concat_axis=0, tiled=True)
    own_sums = jnp.sum(own_part.astype(F32), axis=0).reshape(n_exp, length, HEAD_SIZE)
    grad_query_rot = batched(grad_scores, keys_all, 2, 1)
    grad_query_unit = rotation_backward(
        jnp.transpose(
            grad_query_rot.reshape(n_exp, heads_own, length, HEAD_SIZE), (0, 2, 1, 3)
        ), cos_q, sin_q,
    )
    q_gain_part = jnp.sum(grad_query_unit * queries * query_scale, axis=(0, 1, 2))
    grad_query_rows = norm_backward(grad_query_unit, queries, query_scale, q_gain).astype(BF)
    grad_query_rows = grad_query_rows.reshape(tokens, own_width)
    grad_key_unit = rotation_backward(own_sums, cos_k, sin_k)
    k_gain_part = jnp.sum(grad_key_unit * own_raw * key_scale, axis=(0, 1))
    k_gain_part = jnp.where(holds_keys, k_gain_part, 0.0)
    grad_own = jnp.where(
        holds_keys, norm_backward(grad_key_unit, own_raw, key_scale, k_gain), own_sums
    ).astype(BF)
    grad_heads_in = jnp.concatenate(
        [grad_query_rows, grad_own.reshape(tokens, HEAD_SIZE)], axis=1
    )
    normed_part = dot(grad_heads_in, weight_cols, ((1,), (1,))).astype(BF)
    grad_normed = lax.psum_scatter(normed_part, "exp", scatter_dimension=0, tiled=True)
    grad_normed = grad_normed.astype(F32)
    first_scale = rms_scale(wide_in)
    grad_in = grad_mid + norm_backward(grad_normed, wide_in, first_scale, first_gain)

    grad_cols = dot(normed, grad_heads_in, ((0,), (0,))).astype(BF)
    gain_parts = jnp.concatenate(
        [
            mlp_gain_part.reshape(n_exp, cut),
            q_gain_part.reshape(n_exp, small),
            k_gain_part.reshape(n_exp, small),
        ],
        axis=1,
    )
    gain_parts = jnp.pad(gain_parts, ((0, 0), (0, packed_width - cut - 2 * small)))[:, None, :]
    gain_parts = jnp.pad(gain_parts, ((0, 0), (0, 31), (0, 0))).astype(BF)
    grad_cols = jnp.concatenate(
        [grad_cols.reshape(n_exp, rows_own, packed_width), gain_parts], axis=1
    )
    grad_cols = column_sum(grad_cols.reshape(n_exp * (rows_own + 32), packed_width), n_ctx, n_exp)
    own_gains = jnp.sum(grad_cols[:, rows_own].astype(F32), axis=0)
    grad_cols = grad_cols[:, :rows_own]
    to_row = jnp.transpose(grad_cols, (1, 0, 2))
    halves = jnp.sum(
        to_row[:, :, own_width:]
        .reshape(rows_own, KEY_VALUE_HEADS, sharers // 2, 2, HEAD_SIZE)
        .astype(F32),
        axis=2,
    )
    kv_width = KEY_VALUE_HEADS * HEAD_SIZE
    grad_wq = to_row[:, :, :own_width].reshape(rows_own, query_width).astype(F32)
    grad_wk = halves[:, :, 0].reshape(rows_own, kv_width)
    grad_wv = halves[:, :, 1].reshape(rows_own, kv_width)

    attn_gain_sum = (
        jnp.sum(w_query.astype(F32) * grad_wq, axis=1)
        + jnp.sum(key_projection.astype(F32) * grad_wk, axis=1)
        + jnp.sum(value_projection.astype(F32) * grad_wv, axis=1)
    ) / attn_gain.astype(F32)

    return (
        hidden_out[None],
        grad_in[None],
        attn_gain_sum,
        grad_wq,
        grad_wk,
        grad_wv,
        own_gains[cut : cut + small],
        own_gains[cut + small : cut + 2 * small],
        wout_sum,
        own_gains[:cut],
        grad_gate_mat[None],
        grad_up_mat[None],
        grad_down[None],
    )


def solution(mesh):
    rows = P("exp", "ctx", None)
    shard, matrix, expert = P("exp"), P("exp", None), P(("ctx", "exp"), None, None)
    in_specs = (
        rows, rows, rows, shard, matrix, matrix, matrix, shard, shard, matrix, shard,
        expert, expert, expert, rows,
    )
    out_specs = (
        rows, rows, shard, matrix, matrix, matrix, shard, shard, matrix, shard,
        expert, expert, expert,
    )
    return jax.shard_map(
        per_device, mesh=mesh, in_specs=in_specs, out_specs=out_specs, check_vma=False
    )
```

```python
import functools

import jax
import jax.numpy as jnp
from jax import lax
from jax.experimental import pallas as pl
from jax.experimental.pallas import tpu as pltpu
from jax.sharding import PartitionSpec as P


KEY_VALUE_HEADS = 4
HEAD_SIZE = 128
TOPK = 8

EPSILON = 1e-06
THETA = 1000000.0

BF = jnp.bfloat16
F32 = jnp.float32


def rms_scale(tensor):
    return lax.rsqrt(jnp.mean(tensor * tensor, axis=-1, keepdims=True) + EPSILON)


def norm_backward(cotangent, tensor, factor, weight):
    scaled = cotangent * weight
    unit_form = tensor * factor
    return factor * (scaled - unit_form * jnp.mean(scaled * unit_form, axis=-1, keepdims=True))


def rope_tables(positions):
    halfway = HEAD_SIZE // 2
    frequency = THETA ** (-(jnp.arange(halfway, dtype=F32) * (2.0 / HEAD_SIZE)))
    angles = positions.astype(F32)[:, None] * frequency[None, :]
    cosine = jnp.concatenate([jnp.cos(angles), jnp.cos(angles)], axis=-1)
    sine = jnp.concatenate([jnp.sin(angles), jnp.sin(angles)], axis=-1)
    return cosine, sine


def rotate(tensor, cosine, sine):
    halfway = tensor.shape[-1] // 2
    turned = jnp.concatenate([-tensor[..., halfway:], tensor[..., :halfway]], axis=-1)
    return tensor * cosine + turned * sine


def rotation_backward(cotangent, cosine, sine):
    halfway = cotangent.shape[-1] // 2
    sine_part = cotangent * sine
    turned = jnp.concatenate([sine_part[..., halfway:], -sine_part[..., :halfway]], axis=-1)
    return cotangent * cosine + turned


def dot(a, b, dims):
    return lax.dot_general(a, b, (dims, ((), ())), preferred_element_type=F32)


def after(value, *earlier):
    return lax.optimization_barrier((value,) + earlier)[0]


def round_up(number, multiple):
    return -(-number // multiple) * multiple


MESH = pl.DeviceIdType.MESH


def line_sum_steps(n_ctx, chunks, part, finish, line, lag=2):
    (from_left, from_right, to_right, to_left, right_send, right_recv, left_send, left_recv) = line
    ctx, last = lax.axis_index("ctx"), n_ctx - 1

    def copy_right(k):
        return pltpu.make_async_remote_copy(
            src_ref=to_right.at[k], dst_ref=from_left.at[k],
            send_sem=right_send.at[k], recv_sem=right_recv.at[k],
            device_id={"ctx": ctx + 1}, device_id_type=MESH,
        )

    def copy_left(k):
        return pltpu.make_async_remote_copy(
            src_ref=to_left.at[k], dst_ref=from_right.at[k],
            send_sem=left_send.at[k], recv_sem=left_recv.at[k],
            device_id={"ctx": ctx - 1}, device_id_type=MESH,
        )

    def step(time, carry):
        k_right = time - lag * ctx
        k_left = time - lag * (last - ctx)
        k_done = time - lag * jnp.maximum(ctx, last - ctx)

        @pl.when((k_right >= 0) & (k_right < chunks))
        def _():
            @pl.when(ctx == 0)
            def _():
                to_right[k_right] = part(k_right).astype(BF)

            @pl.when(ctx > 0)
            def _():
                copy_right(k_right).wait_recv()
                to_right[k_right] = (part(k_right) + from_left[k_right].astype(F32)).astype(BF)

            @pl.when(ctx < last)
            def _():
                copy_right(k_right).start()

        @pl.when((k_left >= 0) & (k_left < chunks))
        def _():
            @pl.when(ctx == last)
            def _():
                to_left[k_left] = part(k_left).astype(BF)

            @pl.when(ctx < last)
            def _():
                copy_left(k_left).wait_recv()
                to_left[k_left] = (part(k_left) + from_right[k_left].astype(F32)).astype(BF)

            @pl.when(ctx > 0)
            def _():
                copy_left(k_left).start()

        @pl.when((k_done >= 0) & (k_done < chunks))
        def _():
            @pl.when(ctx == last)
            def _():
                finish(k_done, to_right[k_done].astype(F32))

            @pl.when(ctx < last)
            def _():
                finish(k_done, to_right[k_done].astype(F32) + from_right[k_done].astype(F32))

        return carry

    lax.fori_loop(0, chunks + lag * last, step, 0)

    def drain(k, carry):
        @pl.when(ctx < last)
        def _():
            copy_right(k).wait_send()

        @pl.when(ctx > 0)
        def _():
            copy_left(k).wait_send()

        return carry

    lax.fori_loop(0, chunks, drain, 0)


def greet(n_line, others):
    barrier = pltpu.get_barrier_semaphore()
    for other in others:
        pl.semaphore_signal(barrier, inc=1, device_id=other, device_id_type=MESH)
    if n_line == 1:
        pl.semaphore_wait(barrier, len(others))
        return
    ctx, last = lax.axis_index("ctx"), n_line - 1

    @pl.when(ctx > 0)
    def _():
        pl.semaphore_signal(barrier, inc=1, device_id={"ctx": ctx - 1}, device_id_type=MESH)

    @pl.when(ctx < last)
    def _():
        pl.semaphore_signal(barrier, inc=1, device_id={"ctx": ctx + 1}, device_id_type=MESH)

    at_end = (ctx == 0) | (ctx == last)

    @pl.when(at_end)
    def _():
        pl.semaphore_wait(barrier, len(others) + 1)

    @pl.when(jnp.logical_not(at_end))
    def _():
        pl.semaphore_wait(barrier, len(others) + 2)


def line_buffers(chunks, rows, width):
    slots = pltpu.VMEM((chunks, rows, width), BF)
    sems = pltpu.SemaphoreType.DMA((chunks,))
    return [slots] * 4 + [sems] * 4


def line_sum_kernel(n_ctx, chunks, x_ref, out_ref, *line):
    greet(n_ctx, [])

    def finish(k, value):
        out_ref[k] = value

    line_sum_steps(n_ctx, chunks, lambda k: x_ref[k].astype(F32), finish, line)


def line_sum(x, n_ctx, chunks=16):
    total, width = x.shape
    rows = total // chunks
    out = pl.pallas_call(
        functools.partial(line_sum_kernel, n_ctx, chunks),
        out_shape=jax.ShapeDtypeStruct((chunks, rows, width), F32),
        in_specs=[pl.BlockSpec(memory_space=pltpu.VMEM)],
        out_specs=pl.BlockSpec(memory_space=pltpu.VMEM),
        scratch_shapes=line_buffers(chunks, rows, width),
        compiler_params=pltpu.CompilerParams(
            collective_id=2, has_side_effects=True, vmem_limit_bytes=40 * 1024 * 1024
        ),
    )(x.reshape(chunks, rows, width))
    return out.reshape(total, width)


def column_sum_kernel(n_ctx, n_exp, subs, x_ref, out_ref, whole, plane_send, plane_recv, own_sem, *line):
    exp = lax.axis_index("exp")
    chunks = n_exp * subs
    greet(n_ctx, [{"exp": lax.rem(exp + hop, n_exp)} for hop in range(1, n_exp)])

    def copy_plane(k):
        hop, sub = k // subs, lax.rem(k, subs)
        return pltpu.make_async_remote_copy(
            src_ref=whole.at[k], dst_ref=out_ref.at[exp, sub],
            send_sem=plane_send.at[k], recv_sem=plane_recv.at[k],
            device_id={"exp": lax.rem(exp + hop, n_exp)}, device_id_type=MESH,
        )

    def copy_own(k):
        return pltpu.make_async_copy(whole.at[k], out_ref.at[exp, k], own_sem.at[k])

    def part(k):
        owner = lax.rem(exp + k // subs, n_exp)
        return x_ref[owner * subs + lax.rem(k, subs)].astype(F32)

    def finish(k, value):
        whole[k] = value.astype(BF)

        @pl.when(k < subs)
        def _():
            copy_own(k).start()

        @pl.when(k >= subs)
        def _():
            copy_plane(k).start()

    line_sum_steps(n_ctx, chunks, part, finish, line)

    def drain(k, carry):
        @pl.when(k < subs)
        def _():
            copy_own(k).wait()

        @pl.when(k >= subs)
        def _():
            copy_plane(k).wait()

        return carry

    lax.fori_loop(0, chunks, drain, 0)


def column_sum(x, n_ctx, n_exp, subs=4):
    total, width = x.shape
    rows = total // n_exp // subs
    chunks = n_exp * subs
    sems = pltpu.SemaphoreType.DMA((chunks,))
    out = pl.pallas_call(
        functools.partial(column_sum_kernel, n_ctx, n_exp, subs),
        out_shape=jax.ShapeDtypeStruct((n_exp, subs, rows, width), BF),
        in_specs=[pl.BlockSpec(memory_space=pltpu.VMEM)],
        out_specs=pl.BlockSpec(memory_space=pltpu.VMEM),
        scratch_shapes=[
            pltpu.VMEM((chunks, rows, width), BF), sems, sems, pltpu.SemaphoreType.DMA((subs,)),
        ] + line_buffers(chunks, rows, width),
        compiler_params=pltpu.CompilerParams(
            collective_id=1, has_side_effects=True, vmem_limit_bytes=48 * 1024 * 1024
        ),
    )(x.reshape(chunks, rows, width))
    return out.reshape(n_exp, subs * rows, width)


def gather_kernel(n_line, x_ref, out_ref, *sems):
    (z_send, x_send, y_send, d_send, p_send, z_recv, x_recv, y_recv, d_recv, p_recv, own_sem) = sems
    exp = lax.axis_index("exp")
    ctx = lax.axis_index("ctx") if n_line > 1 else 0
    last = n_line - 1

    def flip(bit):
        return exp + bit - 2 * bit * lax.rem(exp // bit, 2)

    over_core, over_x, over_y = flip(1), flip(2), flip(4)
    over_both = over_x + over_y - exp
    greet(n_line, [{"exp": other} for other in (over_core, over_x, over_y)])

    def send(src, place, half, send_sem, recv_sem, device):
        return pltpu.make_async_remote_copy(
            src_ref=src, dst_ref=out_ref.at[place[0], place[1], half],
            send_sem=send_sem, recv_sem=recv_sem, device_id=device, device_id_type=MESH,
        )

    def held(block, line, half):
        return out_ref.at[block, line, half]

    def to_z(src, line, half, way):
        step = 2 * way - 1
        return send(
            src, (exp, line), half, z_send.at[way, line, half], z_recv.at[line, half],
            {"ctx": ctx + step},
        )

    def to_x(src, line, half):
        return send(src, (exp, line), half, x_send.at[line, half], x_recv.at[line, half], {"exp": over_x})

    def to_y(src, line, half):
        return send(src, (exp, line), half, y_send.at[line, half], y_recv.at[line, half], {"exp": over_y})

    def across(line, half):
        block, device = ((over_x, over_y), (over_y, over_x))[half]
        return send(
            held(block, line, half), (block, line), half, d_send.at[line, half],
            d_recv.at[line, half], {"exp": device},
        )

    blocks = (exp, over_x, over_y, over_both)

    def to_core(src, which, line, half):
        return send(
            src, (blocks[which], line), half, p_send.at[which, line, half],
            p_recv.at[which, line, half], {"exp": over_core},
        )

    def when(cond, body):
        if cond is True:
            body()
        else:
            pl.when(cond)(body)

    def own(half):
        return pltpu.make_async_copy(x_ref.at[half], held(exp, ctx, half), own_sem.at[half])

    def place(distance, way):
        line = ctx - (2 * way - 1) * distance
        return line, (True if distance == 0 else (line >= 0) & (line <= last))

    def along(distance, way):
        line, there = place(distance, way)

        def body():
            for half in (0, 1):
                src = x_ref.at[half] if distance == 0 else held(exp, line, half)
                if distance:
                    to_z(src, line, half, way).wait_recv()
                if n_line > 1:
                    for onward in (0, 1) if distance == 0 else (way,):
                        @pl.when((ctx > 0) if onward == 0 else (ctx < last))
                        def _():
                            to_z(src, line, half, onward).start()
            for half in (0, 1):
                src = [x_ref.at[h] if distance == 0 else held(exp, line, h) for h in (0, 1)]
                to_x(src[half], line, half).start()
                to_y(src[1 - half], line, 1 - half).start()
            for half in (0, 1):
                to_core(src[half], 0, line, half).start()

        when(there, body)

    def plane(distance, way):
        line, there = place(distance, way)

        def body():
            to_x(held(over_x, line, 0), line, 0).wait_recv()
            across(line, 0).start()
            to_y(held(over_y, line, 1), line, 1).wait_recv()
            across(line, 1).start()
            to_core(held(over_x, line, 0), 1, line, 0).start()
            to_core(held(over_y, line, 1), 2, line, 1).start()
            to_x(held(over_x, line, 1), line, 1).wait_recv()
            to_core(held(over_x, line, 1), 1, line, 1).start()
            to_y(held(over_y, line, 0), line, 0).wait_recv()
            to_core(held(over_y, line, 0), 2, line, 0).start()

        when(there, body)

    def corner(distance, way):
        line, there = place(distance, way)

        def body():
            for half in (0, 1):
                across(line, half).wait_recv()
                to_core(held(over_both, line, half), 3, line, half).start()

        when(there, body)

    def finish(distance, way):
        line, there = place(distance, way)

        def body():
            for half in (0, 1):
                src = x_ref.at[half] if distance == 0 else held(exp, line, half)
                for which in range(4):
                    from_core = to_core(src, which, line, half)
                    from_core.wait_recv()
                    from_core.wait_send()
                to_x(src, line, half).wait_send()
                to_y(src, line, half).wait_send()
                across(line, half).wait_send()
                if n_line > 1:
                    for onward in (0, 1) if distance == 0 else (way,):
                        @pl.when((ctx > 0) if onward == 0 else (ctx < last))
                        def _():
                            to_z(src, line, half, onward).wait_send()

        when(there, body)

    def everywhere(stage, distance):
        if 0 <= distance < n_line:
            for way in (1,) if distance == 0 else (1, 0):
                stage(distance, way)

    for half in (0, 1):
        own(half).start()
    for time in range(n_line + 2):
        everywhere(along, time)
        everywhere(plane, time - 1)
        everywhere(corner, time - 2)
    for distance in range(n_line):
        everywhere(finish, distance)
    for half in (0, 1):
        own(half).wait()


def gather_rows(x, n_line, n_exp, collective_id):
    rows, width = x.shape
    if n_exp != 8:
        if n_line > 1:
            x = lax.all_gather(x, "ctx", axis=0, tiled=True)
        return lax.all_gather(x, "exp", axis=0, tiled=False)
    dma = pltpu.SemaphoreType.DMA
    pair, four = dma((n_line, 2)), dma((4, n_line, 2))
    out = pl.pallas_call(
        functools.partial(gather_kernel, n_line),
        out_shape=jax.ShapeDtypeStruct((n_exp, n_line, 2, rows // 2, width), x.dtype),
        in_specs=[pl.BlockSpec(memory_space=pltpu.VMEM)],
        out_specs=pl.BlockSpec(memory_space=pl.ANY),
        scratch_shapes=[
            dma((2, n_line, 2)), pair, pair, pair, four, pair, pair, pair, pair, four, dma((2,)),
        ],
        compiler_params=pltpu.CompilerParams(
            collective_id=collective_id, has_side_effects=True
        ),
    )(x.reshape(2, rows // 2, width))
    return out.reshape(n_exp, n_line * rows, width)


def reduce_kernel(x_ref, out_ref, from_core, sums, arrived, c_send, c_recv, q_send, q_recv):
    exp = lax.axis_index("exp")

    def flip(device, bit):
        return device + bit - 2 * bit * lax.rem(device // bit, 2)

    over_core, over_x, over_y = flip(exp, 1), flip(exp, 2), flip(exp, 4)
    owners = (flip(over_x, 4), over_x, over_y, exp)
    greet(1, [{"exp": other} for other in (over_core,) + owners[:3]])
    rows = 16

    def to_core(t):
        return pltpu.make_async_remote_copy(
            src_ref=x_ref.at[flip(owners[t], 1)], dst_ref=from_core.at[t],
            send_sem=c_send.at[t], recv_sem=c_recv.at[t],
            device_id={"exp": over_core}, device_id_type=MESH,
        )

    def to_owner(t):
        return pltpu.make_async_remote_copy(
            src_ref=sums.at[t], dst_ref=arrived.at[t],
            send_sem=q_send.at[t], recv_sem=q_recv.at[t],
            device_id={"exp": owners[t]}, device_id_type=MESH,
        )

    def by_rows(body):
        def step(i, carry):
            body(pl.ds(pl.multiple_of(i * rows, rows), rows))
            return carry

        lax.fori_loop(0, out_ref.shape[0] // rows, step, 0)

    for t in range(4):
        to_core(t).start()
    for t in range(4):
        to_core(t).wait_recv()

        def add(at, t=t):
            value = x_ref[owners[t], at, :].astype(F32) + from_core[t, at, :].astype(F32)
            if t < 3:
                sums[t, at, :] = value.astype(BF)
            else:
                out_ref[at, :] = value

        by_rows(add)
        if t < 3:
            to_owner(t).start()
    for t in (1, 2, 0):
        to_owner(t).wait_recv()

        def gather(at, t=t):
            out_ref[at, :] = out_ref[at, :] + arrived[t, at, :].astype(F32)

        by_rows(gather)
    for t in range(4):
        to_core(t).wait_send()
        if t < 3:
            to_owner(t).wait_send()


def reduce_rows(x, n_exp, collective_id):
    rows, width = x.shape[0] // n_exp, x.shape[1]
    if n_exp != 8:
        return lax.psum_scatter(x, "exp", scatter_dimension=0, tiled=True).astype(F32)
    dma = pltpu.SemaphoreType.DMA
    return pl.pallas_call(
        reduce_kernel,
        out_shape=jax.ShapeDtypeStruct((rows, width), F32),
        in_specs=[pl.BlockSpec(memory_space=pltpu.VMEM)],
        out_specs=pl.BlockSpec(memory_space=pltpu.VMEM),
        scratch_shapes=[
            pltpu.VMEM((4, rows, width), BF), pltpu.VMEM((3, rows, width), BF),
            pltpu.VMEM((3, rows, width), BF), dma((4,)), dma((4,)), dma((3,)), dma((3,)),
        ],
        compiler_params=pltpu.CompilerParams(
            collective_id=collective_id, has_side_effects=True, vmem_limit_bytes=32 * 1024 * 1024
        ),
    )(x.reshape(n_exp, rows, width))


def spread_kernel(
    n_exp, sharers, query_ref, halves_ref, gains_ref, out_ref, gains_out_ref,
    q_send, q_recv, h_send, h_recv, g_send, g_recv, own_sems,
):
    exp = lax.axis_index("exp")
    own_width = query_ref.shape[1] // n_exp
    greet(1, [{"exp": lax.rem(exp + hop, n_exp)} for hop in range(1, n_exp)])

    def pieces(owner):
        columns = pl.ds(pl.multiple_of(owner * own_width, own_width), own_width)
        return (
            (query_ref.at[:, columns], out_ref.at[exp, :, pl.ds(0, own_width)]),
            (
                halves_ref.at[owner // sharers, lax.rem(owner, 2)],
                out_ref.at[exp, :, pl.ds(own_width, HEAD_SIZE)],
            ),
            (gains_ref, gains_out_ref.at[exp]),
        )

    copies = []
    for hop in range(1, n_exp):
        owner = lax.rem(exp + hop, n_exp)
        for (src, dst), send, recv in zip(
            pieces(owner), (q_send, h_send, g_send), (q_recv, h_recv, g_recv)
        ):
            copies.append(
                pltpu.make_async_remote_copy(
                    src_ref=src, dst_ref=dst, send_sem=send.at[hop], recv_sem=recv.at[hop],
                    device_id={"exp": owner}, device_id_type=MESH,
                )
            )
    for i, (src, dst) in enumerate(pieces(exp)):
        copies.append(pltpu.make_async_copy(src, dst, own_sems.at[i]))
    for copy in copies:
        copy.start()
    for copy in copies:
        copy.wait()


def spread_columns(query, halves, gains, n_exp, sharers):
    rows, width = query.shape
    dma = pltpu.SemaphoreType.DMA((n_exp,))
    vmem = pl.BlockSpec(memory_space=pltpu.VMEM)
    return pl.pallas_call(
        functools.partial(spread_kernel, n_exp, sharers),
        out_shape=(
            jax.ShapeDtypeStruct((n_exp, rows, width // n_exp + HEAD_SIZE), BF),
            jax.ShapeDtypeStruct((n_exp,) + gains.shape, BF),
        ),
        in_specs=[vmem] * 3,
        out_specs=(vmem, vmem),
        scratch_shapes=[dma] * 6 + [pltpu.SemaphoreType.DMA((3,))],
        compiler_params=pltpu.CompilerParams(
            collective_id=6, has_side_effects=True, vmem_limit_bytes=24 * 1024 * 1024
        ),
    )(query, halves, gains)


def per_device(
    hidden_in,
    expert_ids,
    gate_weights,
    attn_gain,
    w_query,
    key_projection,
    value_projection,
    query_gain,
    key_norm_gain,
    w_output,
    mlp_gain,
    w_gate,
    w_up,
    w_down,
    grad_out,
):
    length, width = hidden_in.shape[1:]
    n_ctx, n_exp = lax.axis_size("ctx"), lax.axis_size("exp")
    n_all = n_ctx * n_exp
    ctx_index = lax.axis_index("ctx")
    rows_own, query_width = w_query.shape
    heads_own = query_width // HEAD_SIZE // n_exp
    own_width = heads_own * HEAD_SIZE
    sharers = n_exp // KEY_VALUE_HEADS
    tokens = n_exp * length
    holds_keys = lax.rem(lax.axis_index("exp"), 2) == 0
    pairs = [(i, i ^ 1) for i in range(n_exp)]
    factor = HEAD_SIZE ** (-0.5)
    w_gate, w_up, w_down = w_gate[0], w_up[0], w_down[0]

    def heads_of(kv):
        return kv.reshape(rows_own, KEY_VALUE_HEADS, 1, HEAD_SIZE)

    halves = jnp.concatenate([heads_of(key_projection), heads_of(value_projection)], axis=2)
    halves = jnp.transpose(halves, (1, 2, 0, 3))
    packed_width = own_width + HEAD_SIZE
    gains = jnp.concatenate([attn_gain, mlp_gain, query_gain, key_norm_gain])
    gain_rows = round_up(gains.shape[0], 16 * HEAD_SIZE) // HEAD_SIZE
    gains = jnp.pad(gains, (0, gain_rows * HEAD_SIZE - gains.shape[0]))
    hidden_all = gather_rows(hidden_in[0], 1, n_exp, 7)
    hidden_all = hidden_all.reshape(tokens, width)
    weight_cols, gains = spread_columns(
        after(w_query, hidden_all), halves, gains.reshape(gain_rows, HEAD_SIZE),
        n_exp, sharers,
    )
    weight_cols = weight_cols.reshape(n_exp * rows_own, packed_width)
    gains = gains.reshape(n_exp, gain_rows * HEAD_SIZE).astype(F32)
    cut = attn_gain.shape[0]
    small = query_gain.shape[0]
    first_gain = gains[:, :cut].reshape(-1)
    second_gain = gains[:, cut : 2 * cut].reshape(-1)
    q_gain = gains[:, 2 * cut : 2 * cut + small].reshape(-1)
    k_gain = gains[:, 2 * cut + small : 2 * cut + 2 * small].reshape(-1)

    hits = expert_ids[0][:, :, None] == jnp.arange(n_all, dtype=jnp.int32)[None, None, :]
    dense_gates = jnp.sum(jnp.where(hits, gate_weights[0][:, :, None], 0.0), axis=1)
    high = lax.reduce_precision(dense_gates, 8, 7)
    middle = lax.reduce_precision(dense_gates - high, 8, 7)
    gate_parts = jnp.concatenate([high, middle, dense_gates - high - middle], axis=1).astype(BF)
    gate_parts = jnp.pad(gate_parts, ((0, 0), (0, round_up(3 * n_all, HEAD_SIZE) - 3 * n_all)))
    grad_column = lax.all_gather(
        jnp.concatenate([grad_out[0], gate_parts], axis=1), "ctx",
        axis=0, tiled=True,
    )
    gate_parts = grad_column[:, width : width + 3 * n_all].reshape(n_ctx * length, 3, n_all)
    gate_parts = lax.dynamic_slice(
        gate_parts, (0, 0, ctx_index * n_exp), (n_ctx * length, 3, n_exp)
    )
    gate_parts = jnp.transpose(gate_parts, (2, 1, 0))
    span = n_ctx * length
    slots = round_up(n_ctx * max(2, length * TOPK * 4 // (3 * n_all)), 8)
    below = (
        jnp.arange(span, dtype=jnp.int32)[:, None] < jnp.arange(span, dtype=jnp.int32)[None, :]
    ).astype(BF)

    def in_slots(chosen):
        rank = dot(chosen.astype(BF), below, ((1,), (0,))).astype(jnp.int32)
        return chosen[:, None, :] & (
            rank[:, None, :] == jnp.arange(slots, dtype=jnp.int32)[None, :, None]
        )

    pick = in_slots(gate_parts[:, 0] > 0.0).astype(BF).reshape(n_exp * slots, span)

    def exchange(rows):
        rows = rows.astype(BF).reshape(n_exp, slots, width)
        rows = lax.all_to_all(rows, "exp", split_axis=0, concat_axis=0, tiled=True)
        return rows.reshape(n_exp * slots, width)

    packed_rows = dot(pick, grad_column[:, :width], ((1,), (0,))).astype(BF)
    split = width // 2
    packed_rows = packed_rows.reshape(n_exp, slots, width)
    gate_parts = jnp.pad(gate_parts, ((0, 0), (0, 5), (0, split - span)))
    sent = jnp.concatenate([packed_rows[:, :, :split], gate_parts], axis=1)
    received = lax.all_to_all(sent, "exp", split_axis=0, concat_axis=0, tiled=True)
    received_rest = lax.all_to_all(
        packed_rows[:, :, split:], "exp",
        split_axis=0, concat_axis=0, tiled=True,
    )
    own_gates = jnp.sum(received[:, slots : slots + 3, :span].astype(F32), axis=1)
    taken = in_slots(own_gates > 0.0)
    take = taken.astype(BF)
    slot_gates = jnp.sum(jnp.where(taken, own_gates[:, None, :], 0.0), axis=2)

    def weigh(rows):
        rows = slot_gates[:, :, None] * rows.astype(F32)
        return rows.astype(BF).reshape(n_exp * slots, split)

    slot_grads = weigh(received[:, :slots])
    slot_grads_rest = weigh(received_rest)
    slot_gates = slot_gates.reshape(n_exp * slots, 1)

    positions = ctx_index * length + jnp.arange(length, dtype=jnp.int32)
    cosine, sine = rope_tables(positions)
    cos_q, sin_q = cosine[None, :, None, :], sine[None, :, None, :]
    cos_k, sin_k = cosine[None], sine[None]
    wide_all = hidden_all.astype(F32)
    normed = (wide_all * rms_scale(wide_all) * first_gain).astype(BF)
    projected = dot(normed, weight_cols, ((1,), (0,)))
    queries = after(projected[:, :own_width], sent).reshape(n_exp, length, heads_own, HEAD_SIZE)
    own_raw = projected[:, own_width:].reshape(n_exp, length, HEAD_SIZE)
    query_scale, key_scale = rms_scale(queries), rms_scale(own_raw)
    query_rot = rotate(queries * query_scale * q_gain, cos_q, sin_q).astype(BF)
    key_rot = rotate(own_raw * key_scale * k_gain, cos_k, sin_k).astype(BF)
    own_half = jnp.where(holds_keys, key_rot, own_raw.astype(BF)).reshape(tokens, HEAD_SIZE)
    own_half = lax.all_gather(own_half, "ctx", axis=0, tiled=True)
    other_half = lax.ppermute(own_half, "exp", pairs)

    def by_sequence(half):
        half = half.reshape(n_ctx, n_exp, length, HEAD_SIZE)
        return jnp.transpose(half, (1, 0, 2, 3)).reshape(n_exp, n_ctx * length, HEAD_SIZE)

    keys_all = by_sequence(jnp.where(holds_keys, own_half, other_half))
    values_all = by_sequence(jnp.where(holds_keys, other_half, own_half))

    query_rows = jnp.transpose(query_rot, (0, 2, 1, 3)).reshape(n_exp, heads_own * length, HEAD_SIZE)
    key_pos = jnp.arange(n_ctx * length, dtype=jnp.int32)
    causal = key_pos[None, :] <= jnp.tile(positions, heads_own)[:, None]

    def batched(a, b, a_dim, b_dim):
        return lax.dot_general(
            a, b, (((a_dim,), (b_dim,)), ((0,), (0,))), preferred_element_type=F32
        )

    expos = jnp.where(causal, jnp.exp(batched(query_rows, keys_all, 2, 2) * factor), 0.0)
    totals = jnp.sum(expos, axis=-1, keepdims=True)
    attn_heads = (batched(expos.astype(BF), values_all, 2, 1) / totals).astype(BF)
    attn_rows = jnp.transpose(
        attn_heads.reshape(n_exp, heads_own, length, HEAD_SIZE), (0, 2, 1, 3)
    ).reshape(tokens, own_width)
    branch_part = dot(attn_rows, w_output, ((1,), (0,))).astype(BF)
    branch = reduce_rows(branch_part, n_exp, 5)
    wide_in = hidden_in[0].astype(F32)
    mid = wide_in + branch
    second_scale = rms_scale(mid)
    mlp_in = (mid * second_scale * second_gain).astype(BF)

    mlp_all = gather_rows(after(mlp_in, take), n_ctx, n_exp, 3)
    arrived = lax.dot_general(
        take, mlp_all, (((2,), (1,)), ((0,), (0,))), preferred_element_type=F32
    ).astype(BF).reshape(n_exp * slots, width)
    gate_pre = dot(arrived, w_gate, ((1,), (0,)))
    up_pre = dot(arrived, w_up, ((1,), (0,)))
    sigmoid_gate = jax.nn.sigmoid(gate_pre)
    silu_gate = gate_pre * sigmoid_gate
    inner = (silu_gate * up_pre).astype(BF)
    grad_inner = dot(slot_grads, w_down[:, :split], ((1,), (1,))) + dot(
        slot_grads_rest, w_down[:, split:], ((1,), (1,))
    )
    grad_gate_pre = (
        grad_inner * up_pre * sigmoid_gate * (1.0 + gate_pre * (1.0 - sigmoid_gate))
    ).astype(BF)
    grad_up_pre = (grad_inner * silu_gate).astype(BF)

    def give_back(at):
        rows = dot(grad_gate_pre, w_gate[at], ((1,), (1,))) + dot(grad_up_pre, w_up[at], ((1,), (1,)))
        return rows.astype(BF).reshape(n_exp, slots, split)

    def back_sum(rows):
        part = dot(pick, rows.reshape(n_exp * slots, split), ((0,), (0,))).astype(BF)
        return lax.psum_scatter(part, "ctx", scatter_dimension=0, tiled=True)

    first = lax.all_to_all(give_back(slice(0, split)), "exp", split_axis=0, concat_axis=0, tiled=True)
    second = after(give_back(slice(split, width)), first)
    second = lax.all_to_all(second, "exp", split_axis=0, concat_axis=0, tiled=True)
    grad_mlp = jnp.concatenate([back_sum(first), back_sum(second)], axis=1).astype(F32)

    gradient_wide = grad_out[0].astype(F32)
    mlp_gain_part = jnp.sum(grad_mlp * mid * second_scale, axis=0)
    grad_mid = gradient_wide + norm_backward(grad_mlp, mid, second_scale, second_gain)
    branch_all = gather_rows(grad_mid.astype(BF), 1, n_exp, 4)
    branch_all = branch_all.reshape(tokens, width)

    expert_out = slot_gates * dot(inner, w_down, ((1,), (0,)))
    out_back = exchange(after(expert_out.astype(BF), branch_all))
    mixed_part = dot(pick, out_back, ((0,), (0,))).astype(BF)
    mixed = lax.psum_scatter(mixed_part, "ctx", scatter_dimension=0, tiled=True)
    hidden_out = (mid + mixed.astype(F32)).astype(BF)
    grad_down = dot(inner, jnp.concatenate([slot_grads, slot_grads_rest], axis=1), ((0,), (0,)))
    grad_gate_mat = dot(arrived, grad_gate_pre, ((0,), (0,)))
    grad_up_mat = dot(arrived, grad_up_pre, ((0,), (0,)))

    grad_wout = dot(attn_rows, branch_all, ((0,), (0,))).astype(BF)
    wout_sum = line_sum(grad_wout, n_ctx)
    attn_grad = dot(after(branch_all, wout_sum), w_output, ((1,), (1,))).astype(BF)
    grad_heads = jnp.transpose(
        after(attn_grad, mixed_part).reshape(n_exp, length, heads_own, HEAD_SIZE), (0, 2, 1, 3)
    ).reshape(n_exp, heads_own * length, HEAD_SIZE)
    deltas = jnp.sum(grad_heads.astype(F32) * attn_heads.astype(F32), axis=-1, keepdims=True)
    probs = jnp.where(causal, jnp.exp(batched(query_rows, keys_all, 2, 2) * factor), 0.0) / totals
    grad_scores = (
        probs * (batched(grad_heads, values_all, 2, 2) - deltas) * factor
    ).astype(BF)
    value_part = batched(probs.astype(BF), grad_heads, 1, 1)
    key_part = batched(grad_scores, query_rows, 1, 1)

    def by_position(part):
        part = part.reshape(n_exp, n_ctx, length, HEAD_SIZE)
        return jnp.transpose(part, (1, 0, 2, 3))

    key_part, value_part = by_position(key_part), by_position(value_part)
    partner = jnp.where(holds_keys, value_part, key_part).astype(BF)
    partner = lax.ppermute(partner, "exp", pairs)
    own_part = jnp.where(holds_keys, key_part, value_part) + partner.astype(F32)
    own_part = own_part.astype(BF).reshape(n_ctx, tokens, HEAD_SIZE)
    own_part = lax.all_to_all(own_part, "ctx", split_axis=0, concat_axis=0, tiled=True)
    own_sums = jnp.sum(own_part.astype(F32), axis=0).reshape(n_exp, length, HEAD_SIZE)
    grad_query_rot = batched(grad_scores, keys_all, 2, 1)
    grad_query_unit = rotation_backward(
        jnp.transpose(
            grad_query_rot.reshape(n_exp, heads_own, length, HEAD_SIZE), (0, 2, 1, 3)
        ), cos_q, sin_q,
    )
    q_gain_part = jnp.sum(grad_query_unit * queries * query_scale, axis=(0, 1, 2))
    grad_query_rows = norm_backward(grad_query_unit, queries, query_scale, q_gain).astype(BF)
    grad_query_rows = grad_query_rows.reshape(tokens, own_width)
    grad_key_unit = rotation_backward(own_sums, cos_k, sin_k)
    k_gain_part = jnp.sum(grad_key_unit * own_raw * key_scale, axis=(0, 1))
    k_gain_part = jnp.where(holds_keys, k_gain_part, 0.0)
    grad_own = jnp.where(
        holds_keys, norm_backward(grad_key_unit, own_raw, key_scale, k_gain), own_sums
    ).astype(BF)
    grad_heads_in = jnp.concatenate(
        [grad_query_rows, grad_own.reshape(tokens, HEAD_SIZE)], axis=1
    )
    normed_part = dot(grad_heads_in, weight_cols, ((1,), (1,))).astype(BF)
    grad_normed = lax.psum_scatter(normed_part, "exp", scatter_dimension=0, tiled=True)
    grad_normed = grad_normed.astype(F32)
    first_scale = rms_scale(wide_in)
    grad_in = grad_mid + norm_backward(grad_normed, wide_in, first_scale, first_gain)

    grad_cols = dot(normed, grad_heads_in, ((0,), (0,))).astype(BF)
    gain_parts = jnp.concatenate(
        [
            mlp_gain_part.reshape(n_exp, cut),
            q_gain_part.reshape(n_exp, small),
            k_gain_part.reshape(n_exp, small),
        ],
        axis=1,
    )
    gain_parts = jnp.pad(gain_parts, ((0, 0), (0, packed_width - cut - 2 * small)))[:, None, :]
    gain_parts = jnp.pad(gain_parts, ((0, 0), (0, 31), (0, 0))).astype(BF)
    grad_cols = jnp.concatenate(
        [grad_cols.reshape(n_exp, rows_own, packed_width), gain_parts], axis=1
    )
    grad_cols = column_sum(grad_cols.reshape(n_exp * (rows_own + 32), packed_width), n_ctx, n_exp)
    own_gains = jnp.sum(grad_cols[:, rows_own].astype(F32), axis=0)
    grad_cols = grad_cols[:, :rows_own]
    to_row = jnp.transpose(grad_cols, (1, 0, 2))
    halves = jnp.sum(
        to_row[:, :, own_width:]
        .reshape(rows_own, KEY_VALUE_HEADS, sharers // 2, 2, HEAD_SIZE)
        .astype(F32),
        axis=2,
    )
    kv_width = KEY_VALUE_HEADS * HEAD_SIZE
    grad_wq = to_row[:, :, :own_width].reshape(rows_own, query_width).astype(F32)
    grad_wk = halves[:, :, 0].reshape(rows_own, kv_width)
    grad_wv = halves[:, :, 1].reshape(rows_own, kv_width)

    attn_gain_sum = (
        jnp.sum(w_query.astype(F32) * grad_wq, axis=1)
        + jnp.sum(key_projection.astype(F32) * grad_wk, axis=1)
        + jnp.sum(value_projection.astype(F32) * grad_wv, axis=1)
    ) / attn_gain.astype(F32)

    return (
        hidden_out[None],
        grad_in[None],
        attn_gain_sum,
        grad_wq,
        grad_wk,
        grad_wv,
        own_gains[cut : cut + small],
        own_gains[cut + small : cut + 2 * small],
        wout_sum,
        own_gains[:cut],
        grad_gate_mat[None],
        grad_up_mat[None],
        grad_down[None],
    )


def solution(mesh):
    rows = P("exp", "ctx", None)
    shard, matrix, expert = P("exp"), P("exp", None), P(("ctx", "exp"), None, None)
    in_specs = (
        rows, rows, rows, shard, matrix, matrix, matrix, shard, shard, matrix, shard,
        expert, expert, expert, rows,
    )
    out_specs = (
        rows, rows, shard, matrix, matrix, matrix, shard, shard, matrix, shard,
        expert, expert, expert,
    )
    return jax.shard_map(
        per_device, mesh=mesh, in_specs=in_specs, out_specs=out_specs, check_vma=False
    )
```

```python
import functools

import jax
import jax.numpy as jnp
from jax import lax
from jax.experimental import pallas as pl
from jax.experimental.pallas import tpu as pltpu
from jax.sharding import PartitionSpec as P


KEY_VALUE_HEADS = 4
HEAD_SIZE = 128
TOPK = 8

EPSILON = 1e-06
THETA = 1000000.0

BF = jnp.bfloat16
F32 = jnp.float32


def rms_scale(tensor):
    return lax.rsqrt(jnp.mean(tensor * tensor, axis=-1, keepdims=True) + EPSILON)


def norm_backward(cotangent, tensor, factor, weight):
    scaled = cotangent * weight
    unit_form = tensor * factor
    return factor * (scaled - unit_form * jnp.mean(scaled * unit_form, axis=-1, keepdims=True))


def rope_tables(positions):
    halfway = HEAD_SIZE // 2
    frequency = THETA ** (-(jnp.arange(halfway, dtype=F32) * (2.0 / HEAD_SIZE)))
    angles = positions.astype(F32)[:, None] * frequency[None, :]
    cosine = jnp.concatenate([jnp.cos(angles), jnp.cos(angles)], axis=-1)
    sine = jnp.concatenate([jnp.sin(angles), jnp.sin(angles)], axis=-1)
    return cosine, sine


def rotate(tensor, cosine, sine):
    halfway = tensor.shape[-1] // 2
    turned = jnp.concatenate([-tensor[..., halfway:], tensor[..., :halfway]], axis=-1)
    return tensor * cosine + turned * sine


def rotation_backward(cotangent, cosine, sine):
    halfway = cotangent.shape[-1] // 2
    sine_part = cotangent * sine
    turned = jnp.concatenate([sine_part[..., halfway:], -sine_part[..., :halfway]], axis=-1)
    return cotangent * cosine + turned


def dot(a, b, dims):
    return lax.dot_general(a, b, (dims, ((), ())), preferred_element_type=F32)


def after(value, *earlier):
    return lax.optimization_barrier((value,) + earlier)[0]


def round_up(number, multiple):
    return -(-number // multiple) * multiple


MESH = pl.DeviceIdType.MESH


def line_sum_steps(n_ctx, chunks, part, finish, line, lag=2):
    (from_left, from_right, to_right, to_left, right_send, right_recv, left_send, left_recv) = line
    ctx, last = lax.axis_index("ctx"), n_ctx - 1

    def copy_right(k):
        return pltpu.make_async_remote_copy(
            src_ref=to_right.at[k], dst_ref=from_left.at[k],
            send_sem=right_send.at[k], recv_sem=right_recv.at[k],
            device_id={"ctx": jnp.minimum(ctx + 1, last)}, device_id_type=MESH,
        )

    def copy_left(k):
        return pltpu.make_async_remote_copy(
            src_ref=to_left.at[k], dst_ref=from_right.at[k],
            send_sem=left_send.at[k], recv_sem=left_recv.at[k],
            device_id={"ctx": jnp.maximum(ctx - 1, 0)}, device_id_type=MESH,
        )

    def step(time, carry):
        k_right = time - lag * ctx
        k_left = time - lag * (last - ctx)
        k_done = time - lag * jnp.maximum(ctx, last - ctx)

        @pl.when((k_right >= 0) & (k_right < chunks))
        def _():
            @pl.when(ctx == 0)
            def _():
                to_right[k_right] = part(k_right).astype(BF)

            @pl.when(ctx > 0)
            def _():
                copy_right(k_right).wait_recv()
                to_right[k_right] = (part(k_right) + from_left[k_right].astype(F32)).astype(BF)

            @pl.when(ctx < last)
            def _():
                copy_right(k_right).start()

        @pl.when((k_left >= 0) & (k_left < chunks))
        def _():
            @pl.when(ctx == last)
            def _():
                to_left[k_left] = part(k_left).astype(BF)

            @pl.when(ctx < last)
            def _():
                copy_left(k_left).wait_recv()
                to_left[k_left] = (part(k_left) + from_right[k_left].astype(F32)).astype(BF)

            @pl.when(ctx > 0)
            def _():
                copy_left(k_left).start()

        @pl.when((k_done >= 0) & (k_done < chunks))
        def _():
            @pl.when(ctx == last)
            def _():
                finish(k_done, to_right[k_done].astype(F32))

            @pl.when(ctx < last)
            def _():
                finish(k_done, to_right[k_done].astype(F32) + from_right[k_done].astype(F32))

        return carry

    lax.fori_loop(0, chunks + lag * last, step, 0)

    def drain(k, carry):
        @pl.when(ctx < last)
        def _():
            copy_right(k).wait_send()

        @pl.when(ctx > 0)
        def _():
            copy_left(k).wait_send()

        return carry

    lax.fori_loop(0, chunks, drain, 0)


def greet(n_line, others):
    barrier = pltpu.get_barrier_semaphore()
    for other in others:
        pl.semaphore_signal(barrier, inc=1, device_id=other, device_id_type=MESH)
    if n_line == 1:
        pl.semaphore_wait(barrier, len(others))
        return
    ctx, last = lax.axis_index("ctx"), n_line - 1

    @pl.when(ctx > 0)
    def _():
        pl.semaphore_signal(barrier, inc=1, device_id={"ctx": ctx - 1}, device_id_type=MESH)

    @pl.when(ctx < last)
    def _():
        pl.semaphore_signal(barrier, inc=1, device_id={"ctx": ctx + 1}, device_id_type=MESH)

    at_end = (ctx == 0) | (ctx == last)

    @pl.when(at_end)
    def _():
        pl.semaphore_wait(barrier, len(others) + 1)

    @pl.when(jnp.logical_not(at_end))
    def _():
        pl.semaphore_wait(barrier, len(others) + 2)


def line_buffers(chunks, rows, width):
    slots = pltpu.VMEM((chunks, rows, width), BF)
    sems = pltpu.SemaphoreType.DMA((chunks,))
    return [slots] * 4 + [sems] * 4


def line_sum_kernel(n_ctx, chunks, x_ref, out_ref, *line):
    greet(n_ctx, [])

    def finish(k, value):
        out_ref[k] = value

    line_sum_steps(n_ctx, chunks, lambda k: x_ref[k].astype(F32), finish, line)


def line_sum(x, n_ctx, chunks=16):
    total, width = x.shape
    rows = total // chunks
    out = pl.pallas_call(
        functools.partial(line_sum_kernel, n_ctx, chunks),
        out_shape=jax.ShapeDtypeStruct((chunks, rows, width), F32),
        in_specs=[pl.BlockSpec(memory_space=pltpu.VMEM)],
        out_specs=pl.BlockSpec(memory_space=pltpu.VMEM),
        scratch_shapes=line_buffers(chunks, rows, width),
        compiler_params=pltpu.CompilerParams(
            collective_id=2, has_side_effects=True, vmem_limit_bytes=40 * 1024 * 1024
        ),
    )(x.reshape(chunks, rows, width))
    return out.reshape(total, width)


def column_sum_kernel(n_ctx, n_exp, subs, x_ref, out_ref, whole, plane_send, plane_recv, own_sem, *line):
    exp = lax.axis_index("exp")
    chunks = n_exp * subs
    greet(n_ctx, [{"exp": lax.rem(exp + hop, n_exp)} for hop in range(1, n_exp)])

    def copy_plane(k):
        hop, sub = k // subs, lax.rem(k, subs)
        return pltpu.make_async_remote_copy(
            src_ref=whole.at[k], dst_ref=out_ref.at[exp, sub],
            send_sem=plane_send.at[k], recv_sem=plane_recv.at[k],
            device_id={"exp": lax.rem(exp + hop, n_exp)}, device_id_type=MESH,
        )

    def copy_own(k):
        return pltpu.make_async_copy(whole.at[k], out_ref.at[exp, k], own_sem.at[k])

    def part(k):
        owner = lax.rem(exp + k // subs, n_exp)
        return x_ref[owner * subs + lax.rem(k, subs)].astype(F32)

    def finish(k, value):
        whole[k] = value.astype(BF)

        @pl.when(k < subs)
        def _():
            copy_own(k).start()

        @pl.when(k >= subs)
        def _():
            copy_plane(k).start()

    line_sum_steps(n_ctx, chunks, part, finish, line)

    def drain(k, carry):
        @pl.when(k < subs)
        def _():
            copy_own(k).wait()

        @pl.when(k >= subs)
        def _():
            copy_plane(k).wait()

        return carry

    lax.fori_loop(0, chunks, drain, 0)


def column_sum(x, n_ctx, n_exp, subs=4):
    total, width = x.shape
    rows = total // n_exp // subs
    chunks = n_exp * subs
    sems = pltpu.SemaphoreType.DMA((chunks,))
    out = pl.pallas_call(
        functools.partial(column_sum_kernel, n_ctx, n_exp, subs),
        out_shape=jax.ShapeDtypeStruct((n_exp, subs, rows, width), BF),
        in_specs=[pl.BlockSpec(memory_space=pltpu.VMEM)],
        out_specs=pl.BlockSpec(memory_space=pltpu.VMEM),
        scratch_shapes=[
            pltpu.VMEM((chunks, rows, width), BF), sems, sems, pltpu.SemaphoreType.DMA((subs,)),
        ] + line_buffers(chunks, rows, width),
        compiler_params=pltpu.CompilerParams(
            collective_id=1, has_side_effects=True, vmem_limit_bytes=48 * 1024 * 1024
        ),
    )(x.reshape(chunks, rows, width))
    return out.reshape(n_exp, subs * rows, width)


def gather_kernel(n_line, x_ref, out_ref, *sems):
    (z_send, x_send, y_send, d_send, p_send, z_recv, x_recv, y_recv, d_recv, p_recv, own_sem) = sems
    exp = lax.axis_index("exp")
    ctx = lax.axis_index("ctx") if n_line > 1 else 0
    last = n_line - 1

    def flip(bit):
        return exp + bit - 2 * bit * lax.rem(exp // bit, 2)

    over_core, over_x, over_y = flip(1), flip(2), flip(4)
    over_both = over_x + over_y - exp
    greet(n_line, [{"exp": other} for other in (over_core, over_x, over_y)])

    def send(src, place, half, send_sem, recv_sem, device):
        return pltpu.make_async_remote_copy(
            src_ref=src, dst_ref=out_ref.at[place[0], place[1], half],
            send_sem=send_sem, recv_sem=recv_sem, device_id=device, device_id_type=MESH,
        )

    def held(block, line, half):
        return out_ref.at[block, line, half]

    def to_z(src, line, half, way):
        step = 2 * way - 1
        return send(
            src, (exp, line), half, z_send.at[way, line, half], z_recv.at[line, half],
            {"ctx": jnp.clip(ctx + step, 0, last)},
        )

    def to_x(src, line, half):
        return send(src, (exp, line), half, x_send.at[line, half], x_recv.at[line, half], {"exp": over_x})

    def to_y(src, line, half):
        return send(src, (exp, line), half, y_send.at[line, half], y_recv.at[line, half], {"exp": over_y})

    def across(line, half):
        block, device = ((over_x, over_y), (over_y, over_x))[half]
        return send(
            held(block, line, half), (block, line), half, d_send.at[line, half],
            d_recv.at[line, half], {"exp": device},
        )

    blocks = (exp, over_x, over_y, over_both)

    def to_core(src, which, line, half):
        return send(
            src, (blocks[which], line), half, p_send.at[which, line, half],
            p_recv.at[which, line, half], {"exp": over_core},
        )

    def when(cond, body):
        if cond is True:
            body()
        else:
            pl.when(cond)(body)

    def own(half):
        return pltpu.make_async_copy(x_ref.at[half], held(exp, ctx, half), own_sem.at[half])

    def place(distance, way):
        line = ctx - (2 * way - 1) * distance
        return line, (True if distance == 0 else (line >= 0) & (line <= last))

    def along(distance, way):
        line, there = place(distance, way)

        def body():
            for half in (0, 1):
                src = x_ref.at[half] if distance == 0 else held(exp, line, half)
                if distance:
                    to_z(src, line, half, way).wait_recv()
                if n_line > 1:
                    for onward in (0, 1) if distance == 0 else (way,):
                        @pl.when((ctx > 0) if onward == 0 else (ctx < last))
                        def _():
                            to_z(src, line, half, onward).start()
            for half in (0, 1):
                src = [x_ref.at[h] if distance == 0 else held(exp, line, h) for h in (0, 1)]
                to_x(src[half], line, half).start()
                to_y(src[1 - half], line, 1 - half).start()
            for half in (0, 1):
                to_core(src[half], 0, line, half).start()

        when(there, body)

    def plane(distance, way):
        line, there = place(distance, way)

        def body():
            to_x(held(over_x, line, 0), line, 0).wait_recv()
            across(line, 0).start()
            to_y(held(over_y, line, 1), line, 1).wait_recv()
            across(line, 1).start()
            to_core(held(over_x, line, 0), 1, line, 0).start()
            to_core(held(over_y, line, 1), 2, line, 1).start()
            to_x(held(over_x, line, 1), line, 1).wait_recv()
            to_core(held(over_x, line, 1), 1, line, 1).start()
            to_y(held(over_y, line, 0), line, 0).wait_recv()
            to_core(held(over_y, line, 0), 2, line, 0).start()

        when(there, body)

    def corner(distance, way):
        line, there = place(distance, way)

        def body():
            for half in (0, 1):
                across(line, half).wait_recv()
                to_core(held(over_both, line, half), 3, line, half).start()

        when(there, body)

    def finish(distance, way):
        line, there = place(distance, way)

        def body():
            for half in (0, 1):
                src = x_ref.at[half] if distance == 0 else held(exp, line, half)
                for which in range(4):
                    from_core = to_core(src, which, line, half)
                    from_core.wait_recv()
                    from_core.wait_send()
                to_x(src, line, half).wait_send()
                to_y(src, line, half).wait_send()
                across(line, half).wait_send()
                if n_line > 1:
                    for onward in (0, 1) if distance == 0 else (way,):
                        @pl.when((ctx > 0) if onward == 0 else (ctx < last))
                        def _():
                            to_z(src, line, half, onward).wait_send()

        when(there, body)

    def everywhere(stage, distance):
        if 0 <= distance < n_line:
            for way in (1,) if distance == 0 else (1, 0):
                stage(distance, way)

    for half in (0, 1):
        own(half).start()
    for time in range(n_line + 2):
        everywhere(along, time)
        everywhere(plane, time - 1)
        everywhere(corner, time - 2)
    for distance in range(n_line):
        everywhere(finish, distance)
    for half in (0, 1):
        own(half).wait()


def gather_rows(x, n_line, n_exp, collective_id):
    rows, width = x.shape
    if n_exp != 8:
        if n_line > 1:
            x = lax.all_gather(x, "ctx", axis=0, tiled=True)
        return lax.all_gather(x, "exp", axis=0, tiled=False)
    dma = pltpu.SemaphoreType.DMA
    pair, four = dma((n_line, 2)), dma((4, n_line, 2))
    out = pl.pallas_call(
        functools.partial(gather_kernel, n_line),
        out_shape=jax.ShapeDtypeStruct((n_exp, n_line, 2, rows // 2, width), x.dtype),
        in_specs=[pl.BlockSpec(memory_space=pltpu.VMEM)],
        out_specs=pl.BlockSpec(memory_space=pl.ANY),
        scratch_shapes=[
            dma((2, n_line, 2)), pair, pair, pair, four, pair, pair, pair, pair, four, dma((2,)),
        ],
        compiler_params=pltpu.CompilerParams(
            collective_id=collective_id, has_side_effects=True
        ),
    )(x.reshape(2, rows // 2, width))
    return out.reshape(n_exp, n_line * rows, width)


def reduce_kernel(x_ref, out_ref, from_core, sums, arrived, c_send, c_recv, q_send, q_recv):
    exp = lax.axis_index("exp")

    def flip(device, bit):
        return device + bit - 2 * bit * lax.rem(device // bit, 2)

    over_core, over_x, over_y = flip(exp, 1), flip(exp, 2), flip(exp, 4)
    owners = (flip(over_x, 4), over_x, over_y, exp)
    greet(1, [{"exp": other} for other in (over_core,) + owners[:3]])
    rows = 16

    def to_core(t):
        return pltpu.make_async_remote_copy(
            src_ref=x_ref.at[flip(owners[t], 1)], dst_ref=from_core.at[t],
            send_sem=c_send.at[t], recv_sem=c_recv.at[t],
            device_id={"exp": over_core}, device_id_type=MESH,
        )

    def to_owner(t):
        return pltpu.make_async_remote_copy(
            src_ref=sums.at[t], dst_ref=arrived.at[t],
            send_sem=q_send.at[t], recv_sem=q_recv.at[t],
            device_id={"exp": owners[t]}, device_id_type=MESH,
        )

    def by_rows(body):
        def step(i, carry):
            body(pl.ds(pl.multiple_of(i * rows, rows), rows))
            return carry

        lax.fori_loop(0, out_ref.shape[0] // rows, step, 0)

    for t in range(4):
        to_core(t).start()
    for t in range(4):
        to_core(t).wait_recv()

        def add(at, t=t):
            value = x_ref[owners[t], at, :].astype(F32) + from_core[t, at, :].astype(F32)
            if t < 3:
                sums[t, at, :] = value.astype(BF)
            else:
                out_ref[at, :] = value

        by_rows(add)
        if t < 3:
            to_owner(t).start()
    for t in (1, 2, 0):
        to_owner(t).wait_recv()

        def gather(at, t=t):
            out_ref[at, :] = out_ref[at, :] + arrived[t, at, :].astype(F32)

        by_rows(gather)
    for t in range(4):
        to_core(t).wait_send()
        if t < 3:
            to_owner(t).wait_send()


def reduce_rows(x, n_exp, collective_id):
    rows, width = x.shape[0] // n_exp, x.shape[1]
    if n_exp != 8:
        return lax.psum_scatter(x, "exp", scatter_dimension=0, tiled=True).astype(F32)
    dma = pltpu.SemaphoreType.DMA
    return pl.pallas_call(
        reduce_kernel,
        out_shape=jax.ShapeDtypeStruct((rows, width), F32),
        in_specs=[pl.BlockSpec(memory_space=pltpu.VMEM)],
        out_specs=pl.BlockSpec(memory_space=pltpu.VMEM),
        scratch_shapes=[
            pltpu.VMEM((4, rows, width), BF), pltpu.VMEM((3, rows, width), BF),
            pltpu.VMEM((3, rows, width), BF), dma((4,)), dma((4,)), dma((3,)), dma((3,)),
        ],
        compiler_params=pltpu.CompilerParams(
            collective_id=collective_id, has_side_effects=True, vmem_limit_bytes=32 * 1024 * 1024
        ),
    )(x.reshape(n_exp, rows, width))


def spread_kernel(
    n_exp, sharers, query_ref, halves_ref, gains_ref, out_ref, gains_out_ref,
    q_send, q_recv, h_send, h_recv, g_send, g_recv, own_sems,
):
    exp = lax.axis_index("exp")
    own_width = query_ref.shape[1] // n_exp
    greet(1, [{"exp": lax.rem(exp + hop, n_exp)} for hop in range(1, n_exp)])

    def pieces(owner):
        columns = pl.ds(pl.multiple_of(owner * own_width, own_width), own_width)
        return (
            (query_ref.at[:, columns], out_ref.at[exp, :, pl.ds(0, own_width)]),
            (
                halves_ref.at[owner // sharers, lax.rem(owner, 2)],
                out_ref.at[exp, :, pl.ds(own_width, HEAD_SIZE)],
            ),
            (gains_ref, gains_out_ref.at[exp]),
        )

    copies = []
    for hop in range(1, n_exp):
        owner = lax.rem(exp + hop, n_exp)
        for (src, dst), send, recv in zip(
            pieces(owner), (q_send, h_send, g_send), (q_recv, h_recv, g_recv)
        ):
            copies.append(
                pltpu.make_async_remote_copy(
                    src_ref=src, dst_ref=dst, send_sem=send.at[hop], recv_sem=recv.at[hop],
                    device_id={"exp": owner}, device_id_type=MESH,
                )
            )
    for i, (src, dst) in enumerate(pieces(exp)):
        copies.append(pltpu.make_async_copy(src, dst, own_sems.at[i]))
    for copy in copies:
        copy.start()
    for copy in copies:
        copy.wait()


def spread_columns(query, halves, gains, n_exp, sharers):
    rows, width = query.shape
    dma = pltpu.SemaphoreType.DMA((n_exp,))
    vmem = pl.BlockSpec(memory_space=pltpu.VMEM)
    return pl.pallas_call(
        functools.partial(spread_kernel, n_exp, sharers),
        out_shape=(
            jax.ShapeDtypeStruct((n_exp, rows, width // n_exp + HEAD_SIZE), BF),
            jax.ShapeDtypeStruct((n_exp,) + gains.shape, BF),
        ),
        in_specs=[vmem] * 3,
        out_specs=(vmem, vmem),
        scratch_shapes=[dma] * 6 + [pltpu.SemaphoreType.DMA((3,))],
        compiler_params=pltpu.CompilerParams(
            collective_id=6, has_side_effects=True, vmem_limit_bytes=24 * 1024 * 1024
        ),
    )(query, halves, gains)


def per_device(
    hidden_in,
    expert_ids,
    gate_weights,
    attn_gain,
    w_query,
    key_projection,
    value_projection,
    query_gain,
    key_norm_gain,
    w_output,
    mlp_gain,
    w_gate,
    w_up,
    w_down,
    grad_out,
):
    length, width = hidden_in.shape[1:]
    n_ctx, n_exp = lax.axis_size("ctx"), lax.axis_size("exp")
    n_all = n_ctx * n_exp
    ctx_index = lax.axis_index("ctx")
    rows_own, query_width = w_query.shape
    heads_own = query_width // HEAD_SIZE // n_exp
    own_width = heads_own * HEAD_SIZE
    sharers = n_exp // KEY_VALUE_HEADS
    tokens = n_exp * length
    holds_keys = lax.rem(lax.axis_index("exp"), 2) == 0
    pairs = [(i, i ^ 1) for i in range(n_exp)]
    factor = HEAD_SIZE ** (-0.5)
    w_gate, w_up, w_down = w_gate[0], w_up[0], w_down[0]

    def heads_of(kv):
        return kv.reshape(rows_own, KEY_VALUE_HEADS, 1, HEAD_SIZE)

    halves = jnp.concatenate([heads_of(key_projection), heads_of(value_projection)], axis=2)
    halves = jnp.transpose(halves, (1, 2, 0, 3))
    packed_width = own_width + HEAD_SIZE
    gains = jnp.concatenate([attn_gain, mlp_gain, query_gain, key_norm_gain])
    gain_rows = round_up(gains.shape[0], 16 * HEAD_SIZE) // HEAD_SIZE
    gains = jnp.pad(gains, (0, gain_rows * HEAD_SIZE - gains.shape[0]))
    hidden_all = gather_rows(hidden_in[0], 1, n_exp, 7)
    hidden_all = hidden_all.reshape(tokens, width)
    weight_cols, gains = spread_columns(
        after(w_query, hidden_all), halves, gains.reshape(gain_rows, HEAD_SIZE),
        n_exp, sharers,
    )
    weight_cols = weight_cols.reshape(n_exp * rows_own, packed_width)
    gains = gains.reshape(n_exp, gain_rows * HEAD_SIZE).astype(F32)
    cut = attn_gain.shape[0]
    small = query_gain.shape[0]
    first_gain = gains[:, :cut].reshape(-1)
    second_gain = gains[:, cut : 2 * cut].reshape(-1)
    q_gain = gains[:, 2 * cut : 2 * cut + small].reshape(-1)
    k_gain = gains[:, 2 * cut + small : 2 * cut + 2 * small].reshape(-1)

    hits = expert_ids[0][:, :, None] == jnp.arange(n_all, dtype=jnp.int32)[None, None, :]
    dense_gates = jnp.sum(jnp.where(hits, gate_weights[0][:, :, None], 0.0), axis=1)
    high = lax.reduce_precision(dense_gates, 8, 7)
    middle = lax.reduce_precision(dense_gates - high, 8, 7)
    gate_parts = jnp.concatenate([high, middle, dense_gates - high - middle], axis=1).astype(BF)
    gate_parts = jnp.pad(gate_parts, ((0, 0), (0, round_up(3 * n_all, HEAD_SIZE) - 3 * n_all)))
    grad_column = lax.all_gather(
        jnp.concatenate([grad_out[0], gate_parts], axis=1), "ctx",
        axis=0, tiled=True,
    )
    gate_parts = grad_column[:, width : width + 3 * n_all].reshape(n_ctx * length, 3, n_all)
    gate_parts = lax.dynamic_slice(
        gate_parts, (0, 0, ctx_index * n_exp), (n_ctx * length, 3, n_exp)
    )
    gate_parts = jnp.transpose(gate_parts, (2, 1, 0))
    span = n_ctx * length
    slots = round_up(n_ctx * max(2, length * TOPK * 4 // (3 * n_all)), 8)
    below = (
        jnp.arange(span, dtype=jnp.int32)[:, None] < jnp.arange(span, dtype=jnp.int32)[None, :]
    ).astype(BF)

    def in_slots(chosen):
        rank = dot(chosen.astype(BF), below, ((1,), (0,))).astype(jnp.int32)
        return chosen[:, None, :] & (
            rank[:, None, :] == jnp.arange(slots, dtype=jnp.int32)[None, :, None]
        )

    pick = in_slots(gate_parts[:, 0] > 0.0).astype(BF).reshape(n_exp * slots, span)

    def exchange(rows):
        rows = rows.astype(BF).reshape(n_exp, slots, width)
        rows = lax.all_to_all(rows, "exp", split_axis=0, concat_axis=0, tiled=True)
        return rows.reshape(n_exp * slots, width)

    packed_rows = dot(pick, grad_column[:, :width], ((1,), (0,))).astype(BF)
    split = width // 2
    packed_rows = packed_rows.reshape(n_exp, slots, width)
    gate_parts = jnp.pad(gate_parts, ((0, 0), (0, 5), (0, split - span)))
    sent = jnp.concatenate([packed_rows[:, :, :split], gate_parts], axis=1)
    received = lax.all_to_all(sent, "exp", split_axis=0, concat_axis=0, tiled=True)
    received_rest = lax.all_to_all(
        packed_rows[:, :, split:], "exp",
        split_axis=0, concat_axis=0, tiled=True,
    )
    own_gates = jnp.sum(received[:, slots : slots + 3, :span].astype(F32), axis=1)
    taken = in_slots(own_gates > 0.0)
    take = taken.astype(BF)
    slot_gates = jnp.sum(jnp.where(taken, own_gates[:, None, :], 0.0), axis=2)

    def weigh(rows):
        rows = slot_gates[:, :, None] * rows.astype(F32)
        return rows.astype(BF).reshape(n_exp * slots, split)

    slot_grads = weigh(received[:, :slots])
    slot_grads_rest = weigh(received_rest)
    slot_gates = slot_gates.reshape(n_exp * slots, 1)

    positions = ctx_index * length + jnp.arange(length, dtype=jnp.int32)
    cosine, sine = rope_tables(positions)
    cos_q, sin_q = cosine[None, :, None, :], sine[None, :, None, :]
    cos_k, sin_k = cosine[None], sine[None]
    wide_all = hidden_all.astype(F32)
    normed = (wide_all * rms_scale(wide_all) * first_gain).astype(BF)
    projected = dot(normed, weight_cols, ((1,), (0,)))
    queries = after(projected[:, :own_width], sent).reshape(n_exp, length, heads_own, HEAD_SIZE)
    own_raw = projected[:, own_width:].reshape(n_exp, length, HEAD_SIZE)
    query_scale, key_scale = rms_scale(queries), rms_scale(own_raw)
    query_rot = rotate(queries * query_scale * q_gain, cos_q, sin_q).astype(BF)
    key_rot = rotate(own_raw * key_scale * k_gain, cos_k, sin_k).astype(BF)
    own_half = jnp.where(holds_keys, key_rot, own_raw.astype(BF)).reshape(tokens, HEAD_SIZE)
    own_half = lax.all_gather(own_half, "ctx", axis=0, tiled=True)
    other_half = lax.ppermute(own_half, "exp", pairs)

    def by_sequence(half):
        half = half.reshape(n_ctx, n_exp, length, HEAD_SIZE)
        return jnp.transpose(half, (1, 0, 2, 3)).reshape(n_exp, n_ctx * length, HEAD_SIZE)

    keys_all = by_sequence(jnp.where(holds_keys, own_half, other_half))
    values_all = by_sequence(jnp.where(holds_keys, other_half, own_half))

    query_rows = jnp.transpose(query_rot, (0, 2, 1, 3)).reshape(n_exp, heads_own * length, HEAD_SIZE)
    key_pos = jnp.arange(n_ctx * length, dtype=jnp.int32)
    causal = key_pos[None, :] <= jnp.tile(positions, heads_own)[:, None]

    def batched(a, b, a_dim, b_dim):
        return lax.dot_general(
            a, b, (((a_dim,), (b_dim,)), ((0,), (0,))), preferred_element_type=F32
        )

    expos = jnp.where(causal, jnp.exp(batched(query_rows, keys_all, 2, 2) * factor), 0.0)
    totals = jnp.sum(expos, axis=-1, keepdims=True)
    attn_heads = (batched(expos.astype(BF), values_all, 2, 1) / totals).astype(BF)
    attn_rows = jnp.transpose(
        attn_heads.reshape(n_exp, heads_own, length, HEAD_SIZE), (0, 2, 1, 3)
    ).reshape(tokens, own_width)
    branch_part = dot(attn_rows, w_output, ((1,), (0,))).astype(BF)
    branch = reduce_rows(branch_part, n_exp, 5)
    wide_in = hidden_in[0].astype(F32)
    mid = wide_in + branch
    second_scale = rms_scale(mid)
    mlp_in = (mid * second_scale * second_gain).astype(BF)

    mlp_all = gather_rows(after(mlp_in, take), n_ctx, n_exp, 3)
    arrived = lax.dot_general(
        take, mlp_all, (((2,), (1,)), ((0,), (0,))), preferred_element_type=F32
    ).astype(BF).reshape(n_exp * slots, width)
    gate_pre = dot(arrived, w_gate, ((1,), (0,)))
    up_pre = dot(arrived, w_up, ((1,), (0,)))
    sigmoid_gate = jax.nn.sigmoid(gate_pre)
    silu_gate = gate_pre * sigmoid_gate
    inner = (silu_gate * up_pre).astype(BF)
    grad_inner = dot(slot_grads, w_down[:, :split], ((1,), (1,))) + dot(
        slot_grads_rest, w_down[:, split:], ((1,), (1,))
    )
    grad_gate_pre = (
        grad_inner * up_pre * sigmoid_gate * (1.0 + gate_pre * (1.0 - sigmoid_gate))
    ).astype(BF)
    grad_up_pre = (grad_inner * silu_gate).astype(BF)

    def give_back(at):
        rows = dot(grad_gate_pre, w_gate[at], ((1,), (1,))) + dot(grad_up_pre, w_up[at], ((1,), (1,)))
        return rows.astype(BF).reshape(n_exp, slots, split)

    def back_sum(rows):
        part = dot(pick, rows.reshape(n_exp * slots, split), ((0,), (0,))).astype(BF)
        return lax.psum_scatter(part, "ctx", scatter_dimension=0, tiled=True)

    first = lax.all_to_all(give_back(slice(0, split)), "exp", split_axis=0, concat_axis=0, tiled=True)
    second = after(give_back(slice(split, width)), first)
    second = lax.all_to_all(second, "exp", split_axis=0, concat_axis=0, tiled=True)
    grad_mlp = jnp.concatenate([back_sum(first), back_sum(second)], axis=1).astype(F32)

    gradient_wide = grad_out[0].astype(F32)
    mlp_gain_part = jnp.sum(grad_mlp * mid * second_scale, axis=0)
    grad_mid = gradient_wide + norm_backward(grad_mlp, mid, second_scale, second_gain)
    branch_all = gather_rows(grad_mid.astype(BF), 1, n_exp, 4)
    branch_all = branch_all.reshape(tokens, width)

    expert_out = slot_gates * dot(inner, w_down, ((1,), (0,)))
    out_back = exchange(after(expert_out.astype(BF), branch_all))
    mixed_part = dot(pick, out_back, ((0,), (0,))).astype(BF)
    mixed = lax.psum_scatter(mixed_part, "ctx", scatter_dimension=0, tiled=True)
    hidden_out = (mid + mixed.astype(F32)).astype(BF)
    grad_down = dot(inner, jnp.concatenate([slot_grads, slot_grads_rest], axis=1), ((0,), (0,)))
    grad_gate_mat = dot(arrived, grad_gate_pre, ((0,), (0,)))
    grad_up_mat = dot(arrived, grad_up_pre, ((0,), (0,)))

    grad_wout = dot(attn_rows, branch_all, ((0,), (0,))).astype(BF)
    wout_sum = line_sum(grad_wout, n_ctx)
    attn_grad = dot(after(branch_all, wout_sum), w_output, ((1,), (1,))).astype(BF)
    grad_heads = jnp.transpose(
        after(attn_grad, mixed_part).reshape(n_exp, length, heads_own, HEAD_SIZE), (0, 2, 1, 3)
    ).reshape(n_exp, heads_own * length, HEAD_SIZE)
    deltas = jnp.sum(grad_heads.astype(F32) * attn_heads.astype(F32), axis=-1, keepdims=True)
    probs = jnp.where(causal, jnp.exp(batched(query_rows, keys_all, 2, 2) * factor), 0.0) / totals
    grad_scores = (
        probs * (batched(grad_heads, values_all, 2, 2) - deltas) * factor
    ).astype(BF)
    value_part = batched(probs.astype(BF), grad_heads, 1, 1)
    key_part = batched(grad_scores, query_rows, 1, 1)

    def by_position(part):
        part = part.reshape(n_exp, n_ctx, length, HEAD_SIZE)
        return jnp.transpose(part, (1, 0, 2, 3))

    key_part, value_part = by_position(key_part), by_position(value_part)
    partner = jnp.where(holds_keys, value_part, key_part).astype(BF)
    partner = lax.ppermute(partner, "exp", pairs)
    own_part = jnp.where(holds_keys, key_part, value_part) + partner.astype(F32)
    own_part = own_part.astype(BF).reshape(n_ctx, tokens, HEAD_SIZE)
    own_part = lax.all_to_all(own_part, "ctx", split_axis=0, concat_axis=0, tiled=True)
    own_sums = jnp.sum(own_part.astype(F32), axis=0).reshape(n_exp, length, HEAD_SIZE)
    grad_query_rot = batched(grad_scores, keys_all, 2, 1)
    grad_query_unit = rotation_backward(
        jnp.transpose(
            grad_query_rot.reshape(n_exp, heads_own, length, HEAD_SIZE), (0, 2, 1, 3)
        ), cos_q, sin_q,
    )
    q_gain_part = jnp.sum(grad_query_unit * queries * query_scale, axis=(0, 1, 2))
    grad_query_rows = norm_backward(grad_query_unit, queries, query_scale, q_gain).astype(BF)
    grad_query_rows = grad_query_rows.reshape(tokens, own_width)
    grad_key_unit = rotation_backward(own_sums, cos_k, sin_k)
    k_gain_part = jnp.sum(grad_key_unit * own_raw * key_scale, axis=(0, 1))
    k_gain_part = jnp.where(holds_keys, k_gain_part, 0.0)
    grad_own = jnp.where(
        holds_keys, norm_backward(grad_key_unit, own_raw, key_scale, k_gain), own_sums
    ).astype(BF)
    grad_heads_in = jnp.concatenate(
        [grad_query_rows, grad_own.reshape(tokens, HEAD_SIZE)], axis=1
    )
    normed_part = dot(grad_heads_in, weight_cols, ((1,), (1,))).astype(BF)
    grad_normed = lax.psum_scatter(normed_part, "exp", scatter_dimension=0, tiled=True)
    grad_normed = grad_normed.astype(F32)
    first_scale = rms_scale(wide_in)
    grad_in = grad_mid + norm_backward(grad_normed, wide_in, first_scale, first_gain)

    grad_cols = dot(normed, grad_heads_in, ((0,), (0,))).astype(BF)
    gain_parts = jnp.concatenate(
        [
            mlp_gain_part.reshape(n_exp, cut),
            q_gain_part.reshape(n_exp, small),
            k_gain_part.reshape(n_exp, small),
        ],
        axis=1,
    )
    gain_parts = jnp.pad(gain_parts, ((0, 0), (0, packed_width - cut - 2 * small)))[:, None, :]
    gain_parts = jnp.pad(gain_parts, ((0, 0), (0, 31), (0, 0))).astype(BF)
    grad_cols = jnp.concatenate(
        [grad_cols.reshape(n_exp, rows_own, packed_width), gain_parts], axis=1
    )
    grad_cols = column_sum(grad_cols.reshape(n_exp * (rows_own + 32), packed_width), n_ctx, n_exp)
    own_gains = jnp.sum(grad_cols[:, rows_own].astype(F32), axis=0)
    grad_cols = grad_cols[:, :rows_own]
    to_row = jnp.transpose(grad_cols, (1, 0, 2))
    halves = jnp.sum(
        to_row[:, :, own_width:]
        .reshape(rows_own, KEY_VALUE_HEADS, sharers // 2, 2, HEAD_SIZE)
        .astype(F32),
        axis=2,
    )
    kv_width = KEY_VALUE_HEADS * HEAD_SIZE
    grad_wq = to_row[:, :, :own_width].reshape(rows_own, query_width).astype(F32)
    grad_wk = halves[:, :, 0].reshape(rows_own, kv_width)
    grad_wv = halves[:, :, 1].reshape(rows_own, kv_width)

    attn_gain_sum = (
        jnp.sum(w_query.astype(F32) * grad_wq, axis=1)
        + jnp.sum(key_projection.astype(F32) * grad_wk, axis=1)
        + jnp.sum(value_projection.astype(F32) * grad_wv, axis=1)
    ) / attn_gain.astype(F32)

    return (
        hidden_out[None],
        grad_in[None],
        attn_gain_sum,
        grad_wq,
        grad_wk,
        grad_wv,
        own_gains[cut : cut + small],
        own_gains[cut + small : cut + 2 * small],
        wout_sum,
        own_gains[:cut],
        grad_gate_mat[None],
        grad_up_mat[None],
        grad_down[None],
    )


def solution(mesh):
    rows = P("exp", "ctx", None)
    shard, matrix, expert = P("exp"), P("exp", None), P(("ctx", "exp"), None, None)
    in_specs = (
        rows, rows, rows, shard, matrix, matrix, matrix, shard, shard, matrix, shard,
        expert, expert, expert, rows,
    )
    out_specs = (
        rows, rows, shard, matrix, matrix, matrix, shard, shard, matrix, shard,
        expert, expert, expert,
    )
    return jax.shard_map(
        per_device, mesh=mesh, in_specs=in_specs, out_specs=out_specs, check_vma=False
    )
```
